128 devices in a mesh: ep: 32 (over y, z, core), dp: 4 (over x).
Axes of the slice: x: 4, y: 4, z: 4, core: 2. Of those that a mesh axis runs over, the one named last changes fastest.
Arguments:
- tokens: bfloat16 [24576, 2880], P(('ep', 'dp')), may hold values from -64 to 64
- out_grad: bfloat16 [24576, 2880], P(('ep', 'dp')), may hold values from -6 to 6
- indices: int32 [24576, 4], P(('ep', 'dp')), may hold values from 0 to 127, as said below
- expert_rows: bfloat16 [4, 128, 32, 9, 2880], P('dp', 'ep'), may hold values from -0.111328125 to 0.111328125
- router_weight: bfloat16 [2880, 128], replicated, may hold values from -1 to 1
- router_bias: float32 [128], replicated, may hold values from -3 to 3
- balance_scale: float32 [1], replicated, may hold values from 64 to 256
Outputs:
- token_grad: bfloat16 [24576, 2880], P(('ep', 'dp'))
- weight_grad: float32 [2880, 128], P('dp', 'ep')
- balance_loss: float32 [1], replicated
The draws below stay inside these ranges and needn't reach their ends.
Inputs may be any that keep to these rules, and one draw needn't show every extreme that they name: `indices`: each row names 4 different experts. Within the 192 rows of one device no expert is named by more than 9 rows, and some expert is named by exactly 9 rows. Within the rows of one device the 4 experts of one ep index (experts j * 4 to j * 4 + 3) are named by at most 27 rows together, and those of some ep index by exactly 27. Every expert is named by some row of every device.
All inputs are finite; a program needn't handle non-finite values.
Results may differ from the reference program's by a relative error of at most 0.0014.
The reference program's roundings to bfloat16 on the way (of `picked` and `logit_grad`) count: a program that leaves them out, or rounds other values in their place, can miss the bound.
Values may be sent and summed in bfloat16 or wider, within the bound.
A program may use at most 128 MiB of HBM per device.

```python
import math
import jax
import jax.numpy as jnp
from jax import lax

D = 2880
K = 4
EXP_DEV = 4
TOK_DEV = 192
E = 128
CAP = 9
TOKENS = 24576
N_EP = 32
N_DP = 4


def router_table(key):
    sub_key = jax.random.fold_in(key, 11)
    scale = D ** (-0.5)
    return jnp.clip(jax.random.normal(sub_key, (D, E), jnp.float32) * scale, -6.0 * scale, 6.0 * scale)


def draw_router_weight(key, part):
    return router_table(key).astype(jnp.bfloat16)


def block_offsets(key, table_rows):
    pick_key = jax.random.fold_in(key, 29)
    picks = jax.random.randint(pick_key, (N_EP * N_DP, 8), 0, E)
    columns = jnp.take(table_rows.T, picks.reshape(-1), axis=0).reshape(N_EP * N_DP, 8, D)
    per_block = 4.0 * jnp.sum(columns, axis=1)
    return jnp.repeat(per_block, TOK_DEV, axis=0)


def draw_tokens(key, part):
    sub_key = jax.random.fold_in(key, 23)
    table_rows = router_table(key)
    shifted = block_offsets(key, table_rows)
    result = jnp.clip(jax.random.normal(sub_key, (TOKENS, D), jnp.float32), -6.0, 6.0) + shifted
    return jnp.clip(result, -64.0, 64.0).astype(jnp.bfloat16)


def route_block(block_key, common_key):
    key_shift, key_rows, key_cols = jax.random.split(block_key, 3)
    key_heavy, key_inner = jax.random.split(common_key, 2)
    third = CAP // 3
    group_order = jax.random.permutation(key_heavy, N_EP)
    heavy = (group_order % 2 == 0)[:, None]
    shift = jax.random.randint(key_shift, (N_EP, 1), 0, third + 1)
    heavy_loads = jnp.concatenate([jnp.full((N_EP, 2), CAP, jnp.int32), 2 * third - shift, third + shift], axis=1)
    light_loads = jnp.concatenate([jnp.full((N_EP, 1), CAP, jnp.int32), 2 * third - shift, third + shift, jnp.full((N_EP, 1), third, jnp.int32)], axis=1)
    pattern = jnp.where(heavy, heavy_loads, light_loads).astype(jnp.int32)
    inner_scores = jax.random.randint(key_inner, (N_EP, EXP_DEV), 0, 1 << 20) * EXP_DEV + jnp.arange(EXP_DEV, dtype=jnp.int32)[None, :]
    inner_order = jnp.argsort(inner_scores, axis=1)
    loads = jnp.take_along_axis(pattern, inner_order, axis=1).reshape(E)
    bounds = jnp.cumsum(loads)
    positions = jnp.arange(TOK_DEV * K, dtype=jnp.int32)
    labels = jnp.searchsorted(bounds, positions, side='right').astype(jnp.int32)
    grid = labels.reshape(K, TOK_DEV).T
    row_order = jax.random.permutation(key_rows, TOK_DEV)
    grid = jnp.take(grid, row_order, axis=0)
    col_scores = jax.random.randint(key_cols, (TOK_DEV, K), 0, 1 << 20) * K + jnp.arange(K, dtype=jnp.int32)[None, :]
    col_order = jnp.argsort(col_scores, axis=1)
    return jnp.take_along_axis(grid, col_order, axis=1).astype(jnp.int32)


def draw_indices(key, part):
    base_key = jax.random.fold_in(key, 37)
    common_key = jax.random.fold_in(key, 41)
    block_ids = jnp.arange(N_EP * N_DP, dtype=jnp.int32)
    blocks = jax.vmap(lambda block_id: route_block(jax.random.fold_in(base_key, block_id), common_key))(block_ids)
    return blocks.reshape(TOKENS, K).astype(jnp.int32)


def block_levels(key, extent, shards, least, largest):
    factor_of, own = 1.0, jax.random.fold_in(key, 6)
    for position, parts in shards:
        draws = jnp.exp(jax.random.uniform(jax.random.fold_in(own, position), (parts,), jnp.float32, least / len(shards), largest / len(shards)))
        factor_of = factor_of * jnp.repeat(draws, extent[position] // parts).reshape([-1 if axis == position else 1 for axis in range(len(extent))])
    return factor_of


def gaussian(stream_key, extent, scale, bound, pieces=(), kind=jnp.bfloat16):
    entries = jax.random.normal(stream_key, extent, jnp.float32) * scale
    if len(pieces) > 0:
        entries = block_levels(stream_key, extent, pieces, -0.22, 0.18) * entries
    return jnp.clip(entries, min=-bound, max=bound).astype(kind)


def setup_inputs(seed: int = 0) -> dict:
    splits = jax.random.split(jax.random.key(seed), 8)
    return {
        "tokens": draw_tokens(jax.random.fold_in(splits[7], 71), 0),
        "out_grad": gaussian(splits[1], (TOKENS, D), 1.0, 6.0, ((0, 128),)),
        "indices": draw_indices(jax.random.fold_in(splits[7], 71), 0),
        "expert_rows": gaussian(splits[3], (N_DP, E, N_EP, CAP, D), (D ** -0.5), 0.111328125, ((0, 4), (1, 32))),
        "router_weight": draw_router_weight(jax.random.fold_in(splits[7], 71), 0),
        "router_bias": gaussian(splits[5], (E,), 0.5, 3.0, (), jnp.float32),
        "balance_scale": jnp.clip(jnp.exp(jax.random.uniform(splits[6], (1,), jnp.float32, math.log(64.0), math.log(256.0))), 64.0, 256.0),
    }


def reference(tokens, out_grad, indices, expert_rows, router_weight, router_bias, balance_scale):
    logits = jnp.dot(tokens, router_weight, preferred_element_type=jnp.float32) + router_bias
    probability = jax.nn.softmax(logits, axis=-1)
    expert_ids = jnp.arange(E, dtype=jnp.int32)
    onehot = (indices[:, :, None] == expert_ids[None, None, :]).astype(jnp.float32)
    counts = lax.optimization_barrier(jnp.sum(onehot, axis=(0, 1)))
    prob_mean = lax.optimization_barrier(jnp.sum(probability, axis=0)) / TOKENS
    share_of = counts / (TOKENS * K)
    balance_loss = (E * jnp.sum(share_of * prob_mean)).reshape(1)

    def block_dots(block_id):
        ep_index = block_id // N_DP
        dp_index = block_id % N_DP
        cotangent = lax.dynamic_slice_in_dim(out_grad, block_id * TOK_DEV, TOK_DEV, 0)
        chosen_ids = lax.dynamic_slice_in_dim(indices, block_id * TOK_DEV, TOK_DEV, 0)
        group_rows = lax.dynamic_index_in_dim(expert_rows, dp_index, 0, keepdims=False)
        table_rows = lax.dynamic_index_in_dim(group_rows, ep_index, 1, keepdims=False)
        named_by = lax.optimization_barrier(jnp.sum((chosen_ids[:, :, None] == expert_ids[None, None, :]).astype(jnp.int32), axis=1))
        before = jnp.cumsum(named_by, axis=0) - named_by
        slot_index = jnp.take_along_axis(before, chosen_ids, axis=1)
        row_index = (chosen_ids * CAP + slot_index).astype(jnp.int32)
        picked = table_rows.reshape(E * CAP, D)[row_index]
        return jnp.einsum('td,tkd->tk', cotangent.astype(jnp.float32), picked.astype(jnp.float32))
    pair_dots = lax.map(block_dots, jnp.arange(N_EP * N_DP, dtype=jnp.int32)).reshape(TOKENS, K)
    chosen_logits = jnp.take_along_axis(logits, indices, axis=1)
    mix_weight = jax.nn.softmax(chosen_logits, axis=-1)
    sel_grad = mix_weight * (pair_dots - lax.optimization_barrier(jnp.sum(mix_weight * pair_dots, axis=1, keepdims=True)))
    balance_push = balance_scale[0] * E * share_of
    spread = probability * (balance_push[None, :] - lax.optimization_barrier(jnp.sum(probability * balance_push[None, :], axis=1, keepdims=True)))
    logit_grad = (spread + lax.optimization_barrier(jnp.sum(onehot * sel_grad[:, :, None], axis=1))).astype(jnp.bfloat16)
    token_grad = jnp.dot(logit_grad, router_weight.T, preferred_element_type=jnp.float32).astype(jnp.bfloat16)
    weight_grad = jnp.dot(tokens.T, logit_grad, preferred_element_type=jnp.float32) / math.sqrt(TOKENS)
    return (token_grad, weight_grad, balance_loss)
```

```python
import math

import jax
import jax.numpy as jnp
from jax import lax
from jax.experimental import pallas as pl
from jax.experimental.pallas import tpu as pltpu
from jax.sharding import Mesh
from jax.sharding import PartitionSpec as P

AXES = ("ep_0", "ep_1", "ep_2", "dp")
EP = AXES[:3]
MESH = pl.DeviceIdType.MESH
F32, BF16, I32 = jnp.float32, jnp.bfloat16, jnp.int32

D, E, T, K, CAP = 2880, 128, 192, 4, 9
DPAD = 2944
SPLIT = 1536
WIDTH = (SPLIT, DPAD - SPLIT)
PER = 27
ROWS = 112
ES = 4 * CAP
KQ = ES * 8
PIECES = (((0, 768), (768, 768)), ((0, 768), (768, 640)))
N = 2
BLK = 896
TOTAL = 24576


def dot(a, b, dims=((1,), (0,)), **kw):
    return lax.dot_general(a, b, (dims, ((), ())), preferred_element_type=F32, **kw)


def iota(shape, dim):
    return lax.broadcasted_iota(I32, shape, dim)


def kernel(
    tok_h, og_h, idx_h, ex_h, w_h, b_h, bs_s,
    tg_o, wt_o, loss_o,
    tokraw, tokp, ogfull, og0, og1, idxv, ev3, ev, wv, bv,
    snd0, snd1, tr0, tr1, ex0, ex1, tokr,
    cntsnd, cntr, cc_v, meta, metar, rowsel, acc, gbuf, pds, pdr,
    psb, psr1, psr2, psb2, xcs, xcr, xps, xpr,
    lt, pt, mixv, lgs, lgr, rss, rsr,
    loc, og_s, og_r, ex2_s, ex2_r, fw_s, ex1_s, own_s, exr,
    c1_s, c1_r, c2_s, c2_r, me_s, me_r, p1_s, p1_r, p2_s, p2_r,
    xc_s, xc_r, xp_s, xp_r, tk_s, tk_r, pd_s, pd_r, lg_s, lg_r, rs_s, rs_r,
):
    y, z, c, x = (lax.axis_index(a) for a in AXES)
    og, snd, tr, ex = (og0, og1), (snd0, snd1), (tr0, tr1), (ex0, ex1)
    m4 = lambda v: lax.rem(v + 4, 4)
    po = (z, y)
    pe = (y, z)
    other = 1 - c

    def at(dy=0, dz=0, cc=None, dx=0):
        return (m4(y + dy), m4(z + dz), c if cc is None else cc, m4(x + dx))

    og_dev = (lambda s: at(dz=s), lambda s: at(dy=s))
    ex_dev = (lambda s, cc: at(dy=s, cc=cc), lambda s, cc: at(dz=s, cc=cc))

    def remote(src, dst, ss, rs, dev):
        return pltpu.make_async_remote_copy(src_ref=src, dst_ref=dst, send_sem=ss, recv_sem=rs, device_id=dev, device_id_type=MESH)

    sent = []

    def send(*a):
        r = remote(*a)
        r.start()
        sent.append(r)

    def got(ref, sem):
        remote(ref, ref, sem, sem, at(dx=1)).wait_recv()

    loads = [
        pltpu.make_async_copy(idx_h, idxv, loc.at[0]),
        pltpu.make_async_copy(og_h, ogfull, loc.at[1]),
        pltpu.make_async_copy(tok_h, tokraw, loc.at[2]),
        pltpu.make_async_copy(w_h, wv, loc.at[3]),
        pltpu.make_async_copy(b_h, bv, loc.at[4]),
    ] + [pltpu.make_async_copy(ex_h.at[:, q * 8 : q * 8 + 8, :], ev3.at[q], loc.at[5 + q]) for q in range(4)]
    for l in loads:
        l.start()
    peers = [at(dy=a, dz=b) for a in range(4) for b in range(4) if a or b]
    peers += [at(dy=a, cc=other) for a in (1, 2, 3)] + [at(dz=a, cc=other) for a in (1, 2, 3)]
    peers += [at(cc=other)] + [at(dx=a, cc=k) for a in (1, 2, 3) for k in (c, other)]
    barrier = pltpu.get_barrier_semaphore()
    for p in peers:
        pl.semaphore_signal(barrier, inc=1, device_id=p, device_id_type=MESH)

    loads[0].wait()
    idx = idxv[...]
    ie = iota((E, T), 0)
    named = jnp.zeros((E, T), F32)
    for k in range(K):
        named += jnp.where(idx[k : k + 1, :] == ie, 1.0, 0.0)
    nb = named.astype(BF16)
    upper = jnp.where(iota((T, T), 0) < iota((T, T), 1), 1.0, 0.0).astype(BF16)
    ones_tt = jnp.ones((T, T), BF16)
    r_e, c_e = iota((E, E), 0), iota((E, E), 1)
    same_ep = jnp.where((r_e // 4 == c_e // 4) & (c_e < r_e), 1.0, 0.0).astype(BF16)
    ahead = dot(same_ep, nb).astype(BF16)
    rowpos = dot(nb, upper) + dot(ahead, ones_tt)
    cntsnd[...] = dot(jnp.ones((8, T), BF16), nb, ((1,), (1,)))
    meta[...] = jnp.full((8, 256), -1e6, F32)
    for k in range(K):
        ik = idx[k : k + 1, :]
        off = jnp.sum(jnp.where(ik == ie, rowpos, 0.0), axis=0, keepdims=True)
        ey, ez, ec = ik // 32, (ik // 8) % 4, (ik // 4) % 2
        for h, (ea, eb) in enumerate(((ey, ez), (ez, ey))):
            code = (eb * 1024 + (ea * 2 + ec) * ROWS + po[h] * PER).astype(F32) + off
            meta[4 * h + k : 4 * h + k + 1, 0:T] = code

    loads[1].wait()
    own_og = [pl.ds(pl.multiple_of(po[h] * T, T), T) for h in range(2)]
    og0[own_og[0], :] = ogfull[:, 0:SPLIT]
    og1[own_og[1], WIDTH[1] - 128 : WIDTH[1]] = jnp.zeros((T, 128), BF16)
    og1[own_og[1], 0 : D - SPLIT] = ogfull[:, SPLIT:D]
    pl.semaphore_wait(barrier, len(peers))

    zc = z * 2 + c
    cntr[y, zc] = cntsnd[...]
    zpeers = [(b, k) for b in (1, 2, 3) for k in (0, 1)] + [(0, 1)]
    zdev = lambda b, k: at(dz=b, cc=lax.rem(c + k, 2))
    for n, (b, k) in enumerate(zpeers):
        send(cntsnd, cntr.at[y, zc], c1_s.at[n], c1_r.at[zc], zdev(b, k))
    for h in range(2):
        for s in (1, 2, 3):
            send(meta, metar.at[h, po[h]], me_s.at[h, s - 1], me_r.at[h, po[h]], og_dev[h](s))

    def og_rows(pos, second):
        return pl.ds(pl.multiple_of(pos * T + second * 96, 32), 96)

    def og_send(h, d, m):
        where = og_rows(po[h], d ^ m)
        send(og[h].at[where, :], og[h].at[where, :], og_s.at[h, d, m], og_r.at[h, d, m], og_dev[h](1 - 2 * d))

    for h in range(2):
        for d in range(2):
            og_send(h, d, 0)

    for b, k in zpeers:
        src = m4(z + b) * 2 + lax.rem(c + k, 2)
        got(cntr.at[y, src], c1_r.at[src])
    for s in (1, 2, 3):
        send(cntr.at[y], cntr.at[y], c2_s.at[s - 1], c2_r.at[y], at(dy=s))
    for h in range(2):
        for d in range(2):
            og_send(h, d, 1)

    loads[2].wait()
    tokp[:, DPAD - 128 : DPAD] = jnp.zeros((T, 128), BF16)
    tokp[:, 0:D] = tokraw[...]

    def block(pos):
        return pl.ds(pl.multiple_of((pos * 720) // 128 * 128, 128), BLK)

    xc = x * 2 + c
    xpeers = [(a, k) for a in (1, 2, 3) for k in (0, 1)] + [(0, 1)]
    xdev = lambda a, k: at(dx=a, cc=lax.rem(c + k, 2))
    tokr[xc] = tokp[:, block(x)]
    for n, (a, k) in enumerate(xpeers):
        send(tokp.at[:, block(m4(x + a))], tokr.at[xc], tk_s.at[n], tk_r.at[xc], xdev(a, k))

    loads[3].wait()
    loads[4].wait()
    logits = jnp.transpose(dot(tokp[:, 0:D], wv[...]) + bv[...])
    lt[...] = logits
    ex_l = jnp.exp(logits - jnp.max(logits, axis=0, keepdims=True))
    prob = ex_l / jnp.sum(ex_l, axis=0, keepdims=True)
    pt[...] = prob
    picked = [jnp.sum(jnp.where(idx[k : k + 1, :] == ie, logits, 0.0), axis=0, keepdims=True) for k in range(K)]
    top = jnp.maximum(jnp.maximum(picked[0], picked[1]), jnp.maximum(picked[2], picked[3]))
    picked = [jnp.exp(p - top) for p in picked]
    total = picked[0] + picked[1] + picked[2] + picked[3]
    for k in range(K):
        mixv[k : k + 1, :] = picked[k] / total
    diag = r_e == c_e
    pcol = jnp.sum(prob, axis=1, keepdims=True)
    prow = jnp.sum(jnp.where(diag, pcol, 0.0), axis=0, keepdims=True)
    psb[...] = jnp.broadcast_to(prow, (8, E))
    for n, (b, k) in enumerate(zpeers):
        send(psb, psr1.at[zc], p1_s.at[n], p1_r.at[zc], zdev(b, k))
    psr1[zc] = psb[...]

    for q in range(4):
        loads[5 + q].wait()
    ev[:, DPAD - 128 : DPAD] = jnp.zeros((4 * KQ, 128), BF16)

    def flatten(n, _):
        q, p = n // (ES // 2), lax.rem(n, ES // 2)
        pair = jnp.concatenate([ev3[q, 2 * p], ev3[q, 2 * p + 1]], axis=0)
        ev[pl.ds(pl.multiple_of(n * 16, 16), 16), 0:D] = pair
        return 0

    lax.fori_loop(0, 4 * ES // 2, flatten, 0)

    def og_from(d, h):
        return m4(po[h] - (1 - 2 * d))

    for h in range(2):
        for d in range(2):
            where = og_rows(og_from(d, h), d)
            got(og[h].at[where, :], og_r.at[h, d, 0])
            send(og[h].at[where, :], og[h].at[where, :], og_s.at[h, d, 2], og_r.at[h, d, 2], og_dev[h](1 - 2 * d))

    for s in (1, 2, 3):
        got(cntr.at[m4(y + s)], c2_r.at[m4(y + s)])
    counts = cntr[...]
    plane = jnp.sum(counts.reshape(32, 8, E), axis=0)
    xcs[...] = plane
    xcr[x] = plane
    for a in (1, 2, 3):
        send(xcs, xcr.at[x], xc_s.at[a - 1], xc_r.at[x], at(dx=a))
    first = (y * 8 + z * 2 + c) * 4
    cb = counts.reshape(256, E).astype(BF16)
    for k in range(K):
        mine = jnp.where((r_e >= first) & (r_e <= first + k), 1.0, 0.0).astype(BF16)
        cc_v[k] = dot(cb, mine).astype(BF16)

    def gather(h, delta):
        q = m4(pe[h] + delta)
        row = iota((2 * ROWS, E), 0)
        core = jnp.where(row >= ROWS, 1, 0)
        rr = row - core * ROWS
        i = jnp.where(rr >= PER, 1, 0) + jnp.where(rr >= 2 * PER, 1, 0) + jnp.where(rr >= 3 * PER, 1, 0)
        r = rr - i * PER
        dev = (q * 8 + i * 2 + core) if h == 0 else (i * 8 + q * 2 + core)
        pick = (jnp.broadcast_to(dev[:, 0:1] * 8, (2 * ROWS, 256)) == iota((2 * ROWS, 256), 1))
        pick = jnp.where(pick, 1.0, 0.0).astype(BF16)
        t = [dot(pick, cc_v[k]).astype(I32) for k in range(K)]
        e_in = jnp.where(r >= t[0], 1, 0) + jnp.where(r >= t[1], 1, 0) + jnp.where(r >= t[2], 1, 0)
        base = jnp.where(r >= t[2], t[2], jnp.where(r >= t[1], t[1], jnp.where(r >= t[0], t[0], 0)))
        es = e_in * CAP + r - base
        target = (es * 8 + i * 2 + core) if h == 0 else (i * KQ + es * 8 + q * 2 + core)
        target = jnp.where((r < t[3]) & (rr < 4 * PER), target, -1)
        depth = KQ if h == 0 else 4 * KQ
        sel = jnp.broadcast_to(target[:, 0:1], (2 * ROWS, depth)) == iota((2 * ROWS, depth), 1)
        sel = jnp.where(sel, 1.0, 0.0).astype(BF16)
        rows = pl.ds(pl.multiple_of(q * KQ, KQ), KQ) if h == 0 else pl.ds(0, 4 * KQ)
        for lo, w in PIECES[h]:
            snd[h][delta, :, lo : lo + w] = dot(sel, ev[rows, h * SPLIT + lo : h * SPLIT + lo + w]).astype(BF16)

    def core_rows(cc):
        return pl.ds(pl.multiple_of(cc * ROWS, 16), ROWS)

    def cols(h, n):
        return pl.ds(PIECES[h][n][0], PIECES[h][n][1])

    for h in range(2):
        gather(h, 2)
        for d in range(2):
            for n in range(N):
                send(
                    snd[h].at[2, core_rows(d), cols(h, n)], tr[h].at[d, :, cols(h, n)],
                    ex2_s.at[h, d, n], ex2_r.at[h, d, n], ex_dev[h](1 - 2 * d, c),
                )

    def gather_rest(o, _):
        delta = jnp.where(o == 0, 1, jnp.where(o == 1, 3, 0))
        gather(0, delta)
        gather(1, delta)
        return 0

    lax.fori_loop(0, 3, gather_rest, 0)

    def ex1_send(slot):
        cc = c if slot == 0 else other
        for n in range(N):
            for h in range(2):
                for d in range(2):
                    send(
                        snd[h].at[1 + 2 * d, core_rows(cc), cols(h, n)], ex[h].at[pe[h] * 2 + c, :, cols(h, n)],
                        ex1_s.at[h, d, slot, n], exr.at[h, pe[h] * 2 + c, n], ex_dev[h](1 - 2 * d, cc),
                    )

    ex1_send(0)
    for h in range(2):
        for n in range(N):
            send(
                snd[h].at[0, core_rows(other), cols(h, n)], ex[h].at[pe[h] * 2 + c, :, cols(h, n)],
                own_s.at[h, n], exr.at[h, pe[h] * 2 + c, n], at(cc=other),
            )
        ex[h][pe[h] * 2 + c] = snd[h][0, core_rows(c), :]

    for h in range(2):
        for s in (1, 2, 3):
            got(metar.at[h, m4(po[h] + s)], me_r.at[h, m4(po[h] + s)])
        metar[h, po[h]] = meta[...]
        for i in range(4):
            rowsel[h, :, i * T : (i + 1) * T] = metar[h, i, 4 * h : 4 * h + 4, 0:T] - (pe[1 - h] * 1024).astype(F32)
        for d in range(2):
            got(og[h].at[og_rows(og_from(d, h), 1 - d), :], og_r.at[h, d, 1])
            got(og[h].at[og_rows(m4(po[h] + 2), d), :], og_r.at[h, d, 2])
    acc[...] = jnp.zeros_like(acc)

    def absorb(h, src, here):
        for n in range(N):
            if not here:
                got(ex[h].at[src, :, cols(h, n)], exr.at[h, src, n])
            lo, w = PIECES[h][n]
            part = dot(ex[h][src, :, lo : lo + w], og[h][:, lo : lo + w], ((1,), (1,)))
            if n == 0:
                gbuf[...] = part
            else:
                gbuf[...] += part
        rid = (iota((ROWS, 128), 0) + src * ROWS).astype(F32)
        for lb in range(6):
            lanes = slice(lb * 128, lb * 128 + 128)
            g = gbuf[:, lanes]
            for k in range(K):
                hit = jnp.where(rid == rowsel[h, k : k + 1, lanes], g, 0.0)
                acc[h, k, :, lanes] += jnp.sum(hit.reshape(ROWS // 8, 8, 128), axis=0)

    for h in range(2):
        absorb(h, pe[h] * 2 + c, True)

    for n in range(N):
        for h in range(2):
            for d in range(2):
                got(tr[h].at[d, :, cols(h, n)], ex2_r.at[h, d, n])
                src = m4(pe[h] - (1 - 2 * d)) * 2 + c
                send(
                    tr[h].at[d, :, cols(h, n)], ex[h].at[src, :, cols(h, n)],
                    fw_s.at[h, d, n], exr.at[h, src, n], ex_dev[h](1 - 2 * d, d),
                )
    ex1_send(1)

    for b, k in zpeers:
        src = m4(z + b) * 2 + lax.rem(c + k, 2)
        got(psr1.at[src], p1_r.at[src])
    psb2[...] = jnp.sum(psr1[...], axis=0)
    psr2[y] = psb2[...]
    for s in (1, 2, 3):
        send(psb2, psr2.at[y], p2_s.at[s - 1], p2_r.at[y], at(dy=s))

    for a in (1, 2, 3):
        got(xcr.at[m4(x + a)], xc_r.at[m4(x + a)])
    cnt_row = jnp.sum(xcr[...], axis=0)[0:1, :]
    cnt_col = jnp.sum(jnp.where(diag, cnt_row, 0.0), axis=1, keepdims=True)
    push = bs_s[0] * E * (cnt_col / (TOTAL * K))
    prob = pt[...]
    lt[...] = prob * (push - jnp.sum(prob * push, axis=0, keepdims=True))

    def arrivals(o, _):
        g, o2 = (o + 1) // 2, lax.rem(o + 1, 2)
        step = jnp.where(g == 0, 0, jnp.where(g == 2, 2, 1 + 2 * o2))
        core = jnp.where(g == 1, c, jnp.where(g == 2, o2, other))
        for h in range(2):
            absorb(h, m4(pe[h] + step) * 2 + core, False)
        return 0

    lax.fori_loop(0, 7, arrivals, 0)

    for h in range(2):
        for i in range(4):
            pds[h, i] = jnp.zeros((8, 256), F32)
            for k in range(K):
                pds[h, i, k : k + 1, 0:T] = jnp.sum(acc[h, k, :, i * T : (i + 1) * T], axis=0, keepdims=True)
        for s in (1, 2, 3):
            send(pds.at[h, m4(po[h] + s)], pdr.at[h, po[h]], pd_s.at[h, s - 1], pd_r.at[h, po[h]], og_dev[h](s))
        pdr[h, po[h]] = pds[h, po[h]]
    for s in (1, 2, 3):
        got(psr2.at[m4(y + s)], p2_r.at[m4(y + s)])
    xps[...] = jnp.sum(psr2[...], axis=0)
    xpr[x] = xps[...]
    for a in (1, 2, 3):
        send(xps, xpr.at[x], xp_s.at[a - 1], xp_r.at[x], at(dx=a))
    pd = jnp.zeros((8, 256), F32)
    for h in range(2):
        for s in (1, 2, 3):
            got(pdr.at[h, m4(po[h] + s)], pd_r.at[h, m4(po[h] + s)])
        pd += (pdr[h, 0] + pdr[h, 1]) + (pdr[h, 2] + pdr[h, 3])

    dots = [pd[k : k + 1, 0:T] for k in range(K)]
    mix = [mixv[k : k + 1, :] for k in range(K)]
    mean = mix[0] * dots[0] + mix[1] * dots[1] + mix[2] * dots[2] + mix[3] * dots[3]
    lg = lt[...]
    named = jnp.zeros((E, T), F32)
    for k in range(K):
        named += jnp.where(idxv[k : k + 1, :] == ie, mix[k] * (dots[k] - mean), 0.0)
    lg = lg + named
    lgb = lg.astype(BF16)
    for par in range(2):
        rs_, cs_ = iota((64, E), 0), iota((64, E), 1)
        perm = jnp.where(cs_ == (rs_ // 4) * 8 + par * 4 + rs_ % 4, 1.0, 0.0).astype(BF16)
        lgs[par, :, 0:T] = dot(perm, lgb).astype(BF16)
        lgs[par, :, T:256] = jnp.zeros((64, 256 - T), BF16)
    for n, (a, k) in enumerate(xpeers):
        cc = lax.rem(c + k, 2)
        send(lgs.at[cc], lgr.at[xc], lg_s.at[n], lg_r.at[xc], xdev(a, k))
    lgr[xc] = lgs[c]

    lgt = jnp.transpose(lg).astype(BF16)
    tg_o[...] = dot(lgt, wv[...], ((1,), (1,))).astype(BF16)

    for a, k in xpeers:
        src = m4(x + a) * 2 + lax.rem(c + k, 2)
        got(tokr.at[src], tk_r.at[src])
    wsum = dot(lgr[xc][:, 0:T], tokr[xc])
    for a, k in xpeers:
        src = m4(x + a) * 2 + lax.rem(c + k, 2)
        got(lgr.at[src], lg_r.at[src])
        wsum += dot(lgr[src][:, 0:T], tokr[src])
    for n in range(16):
        rss[n] = wsum[4 * n : 4 * n + 4, :]
    chip = y * 4 + z
    n = 0
    for a in range(4):
        for b in range(4):
            if a or b:
                dest = m4(y + a) * 4 + m4(z + b)
                send(rss.at[dest], rsr.at[chip], rs_s.at[n], rs_r.at[chip], at(dy=a, dz=b))
                n += 1
    rsr[chip] = rss[chip]

    for a in (1, 2, 3):
        got(xpr.at[m4(x + a)], xp_r.at[m4(x + a)])
    ps_row = jnp.sum(xpr[...], axis=0)[0:1, :]
    loss_o[0] = E * jnp.sum((cnt_row / (TOTAL * K)) * (ps_row / TOTAL))

    for a in range(4):
        for b in range(4):
            if a or b:
                src = m4(y + a) * 4 + m4(z + b)
                got(rsr.at[src], rs_r.at[src])
    out = jnp.sum(rsr[...], axis=0) * (1.0 / math.sqrt(TOTAL))
    out = jnp.concatenate([out, out], axis=0)
    shift = x * 720 - (x * 720) // 128 * 128
    out = pltpu.roll(out, lax.rem(BLK - shift, BLK), 1)
    wt_o[...] = out[0:4, 0:720]
    for s in sent:
        s.wait_send()


def on_device(tokens, out_grad, indices, expert_rows, router_weight, router_bias, balance_scale):
    rows = jnp.transpose(expert_rows[0], (0, 2, 1, 3)).reshape(ES, 32, D)
    dma = pltpu.SemaphoreType.DMA
    vm = pltpu.VMEM
    scratch = [
        vm((T, D), BF16), vm((T, DPAD), BF16), vm((T, D), BF16), vm((4 * T, WIDTH[0]), BF16), vm((4 * T, WIDTH[1]), BF16),
        vm((K, T), I32), vm((4, ES, 8, D), BF16), vm((4 * KQ, DPAD), BF16), vm((D, E), BF16), vm((1, E), F32),
        vm((4, 2 * ROWS, WIDTH[0]), BF16), vm((4, 2 * ROWS, WIDTH[1]), BF16),
        vm((2, ROWS, WIDTH[0]), BF16), vm((2, ROWS, WIDTH[1]), BF16),
        vm((8, ROWS, WIDTH[0]), BF16), vm((8, ROWS, WIDTH[1]), BF16), vm((8, T, BLK), BF16),
        vm((8, E), F32), vm((4, 8, 8, E), F32), vm((K, 256, E), BF16), vm((8, 256), F32), vm((2, 4, 8, 256), F32),
        vm((2, K, 4 * T), F32), vm((2, K, 8, 4 * T), F32), vm((ROWS, 4 * T), F32), vm((2, 4, 8, 256), F32), vm((2, 4, 8, 256), F32),
        vm((8, E), F32), vm((8, 8, E), F32), vm((4, 8, E), F32), vm((8, E), F32),
        vm((8, E), F32), vm((4, 8, E), F32), vm((8, E), F32), vm((4, 8, E), F32),
        vm((E, T), F32), vm((E, T), F32), vm((K, T), F32), vm((2, 64, 256), BF16), vm((8, 64, 256), BF16),
        vm((16, 4, BLK), F32), vm((16, 4, BLK), F32),
        dma((9,)), dma((2, 2, 3)), dma((2, 2, 3)), dma((2, 2, N)), dma((2, 2, N)), dma((2, 2, N)), dma((2, 2, 2, N)), dma((2, N)), dma((2, 8, N)),
        dma((7,)), dma((8,)), dma((3,)), dma((4,)), dma((2, 3)), dma((2, 4)), dma((7,)), dma((8,)), dma((3,)), dma((4,)),
        dma((3,)), dma((4,)), dma((3,)), dma((4,)), dma((7,)), dma((8,)), dma((2, 3)), dma((2, 4)), dma((7,)), dma((8,)), dma((15,)), dma((16,)),
    ]
    hbm = pl.BlockSpec(memory_space=pl.ANY)
    token_grad, weight_grad, loss = pl.pallas_call(
        kernel,
        out_shape=(
            jax.ShapeDtypeStruct((T, D), BF16),
            jax.ShapeDtypeStruct((4, 720), F32),
            jax.ShapeDtypeStruct((1,), F32),
        ),
        in_specs=[hbm] * 6 + [pl.BlockSpec(memory_space=pltpu.SMEM)],
        out_specs=(
            pl.BlockSpec(memory_space=pltpu.VMEM),
            pl.BlockSpec(memory_space=pltpu.VMEM),
            pl.BlockSpec(memory_space=pltpu.SMEM),
        ),
        scratch_shapes=scratch,
        compiler_params=pltpu.CompilerParams(collective_id=0, has_side_effects=True, vmem_limit_bytes=64000 * 1024),
        name="router",
    )(tokens, out_grad, indices.T, rows, router_weight, router_bias.reshape(1, E), balance_scale)
    return token_grad, weight_grad.T, loss


def solution(mesh):
    torus = Mesh(mesh.devices.reshape(4, 4, 2, mesh.shape["dp"]), AXES)
    return jax.shard_map(
        on_device,
        mesh=torus,
        in_specs=(P(AXES, None), P(AXES, None), P(AXES, None), P("dp", EP, None, None, None), P(), P(), P()),
        out_specs=(P(AXES, None), P("dp", EP), P()),
        check_vma=False,
    )
```

```python
import math

import jax
import jax.numpy as jnp
from jax import lax
from jax.experimental import pallas as pl
from jax.experimental.pallas import tpu as pltpu
from jax.sharding import Mesh
from jax.sharding import PartitionSpec as P

AXES = ("ep_0", "ep_1", "ep_2", "dp")
EP = AXES[:3]
MESH = pl.DeviceIdType.MESH
F32, BF16, I32 = jnp.float32, jnp.bfloat16, jnp.int32

D, E, T, K, CAP = 2880, 128, 192, 4, 9
DPAD = 2944
SPLIT = 1536
WIDTH = (SPLIT, DPAD - SPLIT)
PER = 27
ROWS = 112
ES = 4 * CAP
KQ = ES * 8
PIECES = (((0, 640), (640, 512), (1152, 384)), ((0, 640), (640, 512), (1152, 256)))
N = 3
BLK = 896
OUT = 768
TOTAL = 24576


def dot(a, b, dims=((1,), (0,)), **kw):
    return lax.dot_general(a, b, (dims, ((), ())), preferred_element_type=F32, **kw)


def iota(shape, dim):
    return lax.broadcasted_iota(I32, shape, dim)


def kernel(
    tok_h, og_h, idx_h, ex_h, w_h, b_h, bs_h,
    lg_o, wt_o, loss_o,
    tokraw, tokp, ogfull, og0, og1, idxv, ev3, ev, wv, bv,
    snd0, snd1, tr0, tr1, ex0, ex1, tokr,
    cntsnd, cntr, cc_v, meta, metar, rowsel, acc, gbuf, pds, pdr,
    psb, psr1, psr2, psb2, xcs, xcr, xps, xpr,
    lt, pt, mixv, spb, spr, selb, selr, rss, rsr, bs_s,
    loc, og_s, og_r, ex2_s, ex2_r, fw_s, ex1_s, own_s, exr,
    c1_s, c1_r, c2_s, c2_r, me_s, me_r, p1_s, p1_r, p2_s, p2_r,
    xc_s, xc_r, xp_s, xp_r, tk_s, tk_r, pd_s, pd_r, sp_s, sp_r, lg_s, lg_r, rs_s, rs_r,
):
    y, z, c, x = (lax.axis_index(a) for a in AXES)
    og, snd, tr, ex = (og0, og1), (snd0, snd1), (tr0, tr1), (ex0, ex1)
    m4 = lambda v: lax.rem(v + 4, 4)
    po = (z, y)
    pe = (y, z)
    other = 1 - c

    def at(dy=0, dz=0, cc=None, dx=0):
        return (m4(y + dy), m4(z + dz), c if cc is None else cc, m4(x + dx))

    og_dev = (lambda s: at(dz=s), lambda s: at(dy=s))
    ex_dev = (lambda s, cc: at(dy=s, cc=cc), lambda s, cc: at(dz=s, cc=cc))

    def remote(src, dst, ss, rs, dev):
        return pltpu.make_async_remote_copy(src_ref=src, dst_ref=dst, send_sem=ss, recv_sem=rs, device_id=dev, device_id_type=MESH)

    sent = []

    def send(*a):
        r = remote(*a)
        r.start()
        sent.append(r)

    def got(ref, sem):
        remote(ref, ref, sem, sem, at(dx=1)).wait_recv()

    loads = [
        pltpu.make_async_copy(idx_h, idxv, loc.at[0]),
        pltpu.make_async_copy(og_h, ogfull, loc.at[1]),
        pltpu.make_async_copy(tok_h, tokraw, loc.at[2]),
        pltpu.make_async_copy(w_h, wv, loc.at[3]),
        pltpu.make_async_copy(b_h, bv, loc.at[4]),
    ] + [pltpu.make_async_copy(ex_h.at[:, q * 8 : q * 8 + 8, :], ev3.at[q], loc.at[5 + q]) for q in range(4)]
    loads.append(pltpu.make_async_copy(bs_h, bs_s, loc.at[9]))
    for l in loads:
        l.start()
    peers = [at(dy=a, dz=b) for a in range(4) for b in range(4) if a or b]
    peers += [at(dy=a, cc=other) for a in (1, 2, 3)] + [at(dz=a, cc=other) for a in (1, 2, 3)]
    peers += [at(cc=other)] + [at(dx=a, cc=k) for a in (1, 2, 3) for k in (c, other)]
    barrier = pltpu.get_barrier_semaphore()
    for p in peers:
        pl.semaphore_signal(barrier, inc=1, device_id=p, device_id_type=MESH)

    loads[0].wait()
    idx = idxv[...]
    ie = iota((E, T), 0)
    named = jnp.zeros((E, T), F32)
    for k in range(K):
        named += jnp.where(idx[k : k + 1, :] == ie, 1.0, 0.0)
    nb = named.astype(BF16)
    upper = jnp.where(iota((T, T), 0) < iota((T, T), 1), 1.0, 0.0).astype(BF16)
    ones_tt = jnp.ones((T, T), BF16)
    r_e, c_e = iota((E, E), 0), iota((E, E), 1)
    same_ep = jnp.where((r_e // 4 == c_e // 4) & (c_e < r_e), 1.0, 0.0).astype(BF16)
    ahead = dot(same_ep, nb).astype(BF16)
    rowpos = dot(nb, upper) + dot(ahead, ones_tt)
    cntsnd[...] = dot(jnp.ones((8, T), BF16), nb, ((1,), (1,)))
    meta[...] = jnp.full((8, 256), -1e6, F32)
    for k in range(K):
        ik = idx[k : k + 1, :]
        off = jnp.sum(jnp.where(ik == ie, rowpos, 0.0), axis=0, keepdims=True)
        ey, ez, ec = ik // 32, (ik // 8) % 4, (ik // 4) % 2
        for h, (ea, eb) in enumerate(((ey, ez), (ez, ey))):
            step, same = (ea - pe[h] + 4) % 4, ec == c
            near = jnp.where(step == 1, jnp.where(same, 2, 6), jnp.where(same, 3, 7))
            slot = jnp.where(step == 0, jnp.where(same, 0, 1), jnp.where(step == 2, 4 + ec, near))
            code = (eb * 1024 + slot * ROWS + po[h] * PER).astype(F32) + off
            meta[4 * h + k : 4 * h + k + 1, 0:T] = code

    loads[1].wait()
    own_og = [pl.ds(pl.multiple_of(po[h] * T, T), T) for h in range(2)]
    og0[own_og[0], :] = ogfull[:, 0:SPLIT]
    og1[own_og[1], WIDTH[1] - 128 : WIDTH[1]] = jnp.zeros((T, 128), BF16)
    og1[own_og[1], 0 : D - SPLIT] = ogfull[:, SPLIT:D]
    pl.semaphore_wait(barrier, len(peers))

    zc = z * 2 + c
    cntr[y, zc] = cntsnd[...]
    zpeers = [(b, k) for b in (1, 2, 3) for k in (0, 1)] + [(0, 1)]
    zdev = lambda b, k: at(dz=b, cc=lax.rem(c + k, 2))
    for n, (b, k) in enumerate(zpeers):
        send(cntsnd, cntr.at[y, zc], c1_s.at[n], c1_r.at[zc], zdev(b, k))
    for h in range(2):
        for s in (1, 2, 3):
            send(meta, metar.at[h, po[h]], me_s.at[h, s - 1], me_r.at[h, po[h]], og_dev[h](s))

    def og_rows(pos, second):
        return pl.ds(pl.multiple_of(pos * T + second * 96, 32), 96)

    def og_send(h, d, m):
        where = og_rows(po[h], d ^ m)
        send(og[h].at[where, :], og[h].at[where, :], og_s.at[h, d, m], og_r.at[h, d, m], og_dev[h](1 - 2 * d))

    for h in range(2):
        for d in range(2):
            og_send(h, d, 0)

    for b, k in zpeers:
        src = m4(z + b) * 2 + lax.rem(c + k, 2)
        got(cntr.at[y, src], c1_r.at[src])
    for s in (1, 2, 3):
        send(cntr.at[y], cntr.at[y], c2_s.at[s - 1], c2_r.at[y], at(dy=s))
    for h in range(2):
        for d in range(2):
            og_send(h, d, 1)

    loads[2].wait()
    tokp[:, DPAD - 128 : DPAD] = jnp.zeros((T, 128), BF16)
    tokp[:, 0:D] = tokraw[...]

    def block(pos):
        return pl.ds(pl.multiple_of((pos * 720) // 128 * 128, 128), BLK)

    xc = x * 2 + c
    xpeers = [(a, k) for a in (1, 2, 3) for k in (0, 1)] + [(0, 1)]
    xdev = lambda a, k: at(dx=a, cc=lax.rem(c + k, 2))
    tokr[xc] = tokp[:, block(x)]
    for n, (a, k) in enumerate(xpeers):
        send(tokp.at[:, block(m4(x + a))], tokr.at[xc], tk_s.at[n], tk_r.at[xc], xdev(a, k))

    loads[3].wait()
    loads[4].wait()
    logits = jnp.transpose(dot(tokp[:, 0:D], wv[...]) + bv[...])
    lt[...] = logits
    ex_l = jnp.exp(logits - jnp.max(logits, axis=0, keepdims=True))
    prob = ex_l / jnp.sum(ex_l, axis=0, keepdims=True)
    pt[...] = prob
    picked = [jnp.sum(jnp.where(idx[k : k + 1, :] == ie, logits, 0.0), axis=0, keepdims=True) for k in range(K)]
    top = jnp.maximum(jnp.maximum(picked[0], picked[1]), jnp.maximum(picked[2], picked[3]))
    picked = [jnp.exp(p - top) for p in picked]
    total = picked[0] + picked[1] + picked[2] + picked[3]
    for k in range(K):
        mixv[k : k + 1, :] = picked[k] / total
    diag = r_e == c_e
    pcol = jnp.sum(prob, axis=1, keepdims=True)
    prow = jnp.sum(jnp.where(diag, pcol, 0.0), axis=0, keepdims=True)
    psb[...] = jnp.broadcast_to(prow, (8, E))
    for n, (b, k) in enumerate(zpeers):
        send(psb, psr1.at[zc], p1_s.at[n], p1_r.at[zc], zdev(b, k))
    psr1[zc] = psb[...]

    for q in range(4):
        loads[5 + q].wait()
    ev[:, DPAD - 128 : DPAD] = jnp.zeros((4 * KQ, 128), BF16)

    def flatten(n, _):
        q, p = n // (ES // 2), lax.rem(n, ES // 2)
        pair = jnp.concatenate([ev3[q, 2 * p], ev3[q, 2 * p + 1]], axis=0)
        ev[pl.ds(pl.multiple_of(n * 16, 16), 16), 0:D] = pair
        return 0

    lax.fori_loop(0, 4 * ES // 2, flatten, 0)

    def og_from(d, h):
        return m4(po[h] - (1 - 2 * d))

    for h in range(2):
        for d in range(2):
            where = og_rows(og_from(d, h), d)
            got(og[h].at[where, :], og_r.at[h, d, 0])
            send(og[h].at[where, :], og[h].at[where, :], og_s.at[h, d, 2], og_r.at[h, d, 2], og_dev[h](1 - 2 * d))

    for s in (1, 2, 3):
        got(cntr.at[m4(y + s)], c2_r.at[m4(y + s)])
    counts = cntr[...]
    plane = jnp.sum(counts.reshape(32, 8, E), axis=0)
    xcs[...] = plane
    xcr[x] = plane
    for a in (1, 2, 3):
        send(xcs, xcr.at[x], xc_s.at[a - 1], xc_r.at[x], at(dx=a))
    first = (y * 8 + z * 2 + c) * 4
    cb = counts.reshape(256, E).astype(BF16)
    for k in range(K):
        mine = jnp.where((r_e >= first) & (r_e <= first + k), 1.0, 0.0).astype(BF16)
        cc_v[k] = dot(cb, mine).astype(BF16)

    def gather(h, delta):
        q = m4(pe[h] + delta)
        row = iota((2 * ROWS, E), 0)
        core = jnp.where(row >= ROWS, 1, 0)
        rr = row - core * ROWS
        i = jnp.where(rr >= PER, 1, 0) + jnp.where(rr >= 2 * PER, 1, 0) + jnp.where(rr >= 3 * PER, 1, 0)
        r = rr - i * PER
        dev = (q * 8 + i * 2 + core) if h == 0 else (i * 8 + q * 2 + core)
        pick = (jnp.broadcast_to(dev[:, 0:1] * 8, (2 * ROWS, 256)) == iota((2 * ROWS, 256), 1))
        pick = jnp.where(pick, 1.0, 0.0).astype(BF16)
        t = [dot(pick, cc_v[k]).astype(I32) for k in range(K)]
        e_in = jnp.where(r >= t[0], 1, 0) + jnp.where(r >= t[1], 1, 0) + jnp.where(r >= t[2], 1, 0)
        base = jnp.where(r >= t[2], t[2], jnp.where(r >= t[1], t[1], jnp.where(r >= t[0], t[0], 0)))
        es = e_in * CAP + r - base
        target = (es * 8 + i * 2 + core) if h == 0 else (i * KQ + es * 8 + q * 2 + core)
        target = jnp.where((r < t[3]) & (rr < 4 * PER), target, -1)
        depth = KQ if h == 0 else 4 * KQ
        sel = jnp.broadcast_to(target[:, 0:1], (2 * ROWS, depth)) == iota((2 * ROWS, depth), 1)
        sel = jnp.where(sel, 1.0, 0.0).astype(BF16)
        rows = pl.ds(pl.multiple_of(q * KQ, KQ), KQ) if h == 0 else pl.ds(0, 4 * KQ)
        for lo, w in PIECES[h]:
            snd[h][delta, :, lo : lo + w] = dot(sel, ev[rows, h * SPLIT + lo : h * SPLIT + lo + w]).astype(BF16)

    def core_rows(cc):
        return pl.ds(pl.multiple_of(cc * ROWS, 16), ROWS)

    def cols(h, n):
        return pl.ds(PIECES[h][n][0], PIECES[h][n][1])

    for h in range(2):
        gather(h, 2)
        for d in range(2):
            for n in range(N):
                send(
                    snd[h].at[2, core_rows(d), cols(h, n)], tr[h].at[d, :, cols(h, n)],
                    ex2_s.at[h, d, n], ex2_r.at[h, d, n], ex_dev[h](1 - 2 * d, c),
                )

    def gather_rest(o, _):
        delta = jnp.where(o == 0, 1, jnp.where(o == 1, 3, 0))
        gather(0, delta)
        gather(1, delta)
        return 0

    lax.fori_loop(0, 3, gather_rest, 0)

    def ex1_send(slot):
        cc = c if slot == 0 else other
        for n in range(N):
            for h in range(2):
                for d in range(2):
                    send(
                        snd[h].at[1 + 2 * d, core_rows(cc), cols(h, n)], ex[h].at[3 - d + 4 * slot, :, cols(h, n)],
                        ex1_s.at[h, d, slot, n], exr.at[h, 3 - d + 4 * slot, n], ex_dev[h](1 - 2 * d, cc),
                    )

    ex1_send(0)
    for h in range(2):
        for n in range(N):
            send(
                snd[h].at[0, core_rows(other), cols(h, n)], ex[h].at[1, :, cols(h, n)],
                own_s.at[h, n], exr.at[h, 1, n], at(cc=other),
            )
        ex[h][0] = snd[h][0, core_rows(c), :]

    for h in range(2):
        for s in (1, 2, 3):
            got(metar.at[h, m4(po[h] + s)], me_r.at[h, m4(po[h] + s)])
        metar[h, po[h]] = meta[...]
        for i in range(4):
            rowsel[h, :, i * T : (i + 1) * T] = metar[h, i, 4 * h : 4 * h + 4, 0:T] - (pe[1 - h] * 1024).astype(F32)
        for d in range(2):
            got(og[h].at[og_rows(og_from(d, h), 1 - d), :], og_r.at[h, d, 1])
            got(og[h].at[og_rows(m4(po[h] + 2), d), :], og_r.at[h, d, 2])
    acc[...] = jnp.zeros_like(acc)

    def absorb(pair, mine):
        for n in range(N):
            for h in range(2):
                for slot in (1,) if mine else (0, 1):
                    got(ex[h].at[2 * pair + slot, :, cols(h, n)], exr.at[h, 2 * pair + slot, n])
                lo, w = PIECES[h][n]
                block = ex[h][pl.ds(2 * pair, 2), :, lo : lo + w].reshape(2 * ROWS, w)
                part = dot(block, og[h][:, lo : lo + w], ((1,), (1,)))
                if n == 0:
                    gbuf[h] = part
                else:
                    gbuf[h] += part
        rid = (iota((2 * ROWS, 128), 0) + pair * 2 * ROWS).astype(F32)
        for h in range(2):
            for lb in range(6):
                lanes = slice(lb * 128, lb * 128 + 128)
                g = gbuf[h, :, lanes]
                for k in range(K):
                    hit = jnp.where(rid == rowsel[h, k : k + 1, lanes], g, 0.0)
                    acc[h, k, :, lanes] += jnp.sum(hit.reshape(2 * ROWS // 8, 8, 128), axis=0)

    absorb(0, True)

    for n in range(N):
        for h in range(2):
            for d in range(2):
                got(tr[h].at[d, :, cols(h, n)], ex2_r.at[h, d, n])
                send(
                    tr[h].at[d, :, cols(h, n)], ex[h].at[4 + c, :, cols(h, n)],
                    fw_s.at[h, d, n], exr.at[h, 4 + c, n], ex_dev[h](1 - 2 * d, d),
                )
    ex1_send(1)

    for b, k in zpeers:
        src = m4(z + b) * 2 + lax.rem(c + k, 2)
        got(psr1.at[src], p1_r.at[src])
    psb2[...] = jnp.sum(psr1[...], axis=0)
    psr2[y] = psb2[...]
    for s in (1, 2, 3):
        send(psb2, psr2.at[y], p2_s.at[s - 1], p2_r.at[y], at(dy=s))

    for a in (1, 2, 3):
        got(xcr.at[m4(x + a)], xc_r.at[m4(x + a)])
    cnt_row = jnp.sum(xcr[...], axis=0)[0:1, :]
    cnt_col = jnp.sum(jnp.where(diag, cnt_row, 0.0), axis=1, keepdims=True)
    loads[9].wait()
    push = bs_s[0] * E * (cnt_col / (TOTAL * K))
    prob = pt[...]
    spread = prob * (push - jnp.sum(prob * push, axis=0, keepdims=True))
    lt[...] = spread
    spb[...] = jnp.zeros_like(spb)
    for par in range(2):
        for n in range(16):
            spb[par, 4 * n : 4 * n + 4, 0:T] = spread[8 * n + 4 * par : 8 * n + 4 * par + 4, :]
        for k in range(K):
            ik = idxv[k : k + 1, :]
            spb[par, 64 + k : 65 + k, 0:T] = jnp.where((ik // 4) % 2 == par, ik // 8 * 4 + ik % 4, -1).astype(F32)
    for n, (a, k) in enumerate(xpeers):
        send(spb.at[lax.rem(c + k, 2)], spr.at[xc], sp_s.at[n], sp_r.at[xc], xdev(a, k))
    spr[xc] = spb[c]

    def arrivals(pair, _):
        absorb(pair, False)
        return 0

    lax.fori_loop(1, 4, arrivals, 0)

    for h in range(2):
        for i in range(4):
            pds[h, i] = jnp.zeros((K, 256), F32)
            for k in range(K):
                pds[h, i, k : k + 1, 0:T] = jnp.sum(acc[h, k, :, i * T : (i + 1) * T], axis=0, keepdims=True)
        for s in (1, 2, 3):
            send(pds.at[h, m4(po[h] + s)], pdr.at[h, po[h]], pd_s.at[h, s - 1], pd_r.at[h, po[h]], og_dev[h](s))
        pdr[h, po[h]] = pds[h, po[h]]
    for s in (1, 2, 3):
        got(psr2.at[m4(y + s)], p2_r.at[m4(y + s)])
    xps[...] = jnp.sum(psr2[...], axis=0)
    xpr[x] = xps[...]
    for a in (1, 2, 3):
        send(xps, xpr.at[x], xp_s.at[a - 1], xp_r.at[x], at(dx=a))
    pd = jnp.zeros((K, 256), F32)
    for h in range(2):
        for s in (1, 2, 3):
            got(pdr.at[h, m4(po[h] + s)], pd_r.at[h, m4(po[h] + s)])
        pd += (pdr[h, 0] + pdr[h, 1]) + (pdr[h, 2] + pdr[h, 3])

    dots = [pd[k : k + 1, 0:T] for k in range(K)]
    mix = [mixv[k : k + 1, :] for k in range(K)]
    mean = mix[0] * dots[0] + mix[1] * dots[1] + mix[2] * dots[2] + mix[3] * dots[3]
    for k in range(K):
        selb[k : k + 1, 0:T] = mix[k] * (dots[k] - mean)
    selb[:, T:256] = jnp.zeros((K, 256 - T), F32)
    for n, (a, k) in enumerate(xpeers):
        send(selb, selr.at[xc], lg_s.at[n], lg_r.at[xc], xdev(a, k))

    lg = jnp.zeros((E, T), F32)
    for k in range(K):
        lg += jnp.where(idxv[k : k + 1, :] == ie, selb[k : k + 1, 0:T], 0.0)
    lg_o[...] = jnp.transpose(lt[...] + lg).astype(BF16)
    for a, k in xpeers:
        src = m4(x + a) * 2 + lax.rem(c + k, 2)
        got(tokr.at[src], tk_r.at[src])
        got(spr.at[src], sp_r.at[src])

    ir = iota((64, T), 0).astype(F32)

    def weight_term(src, sel):
        named = jnp.zeros((64, T), F32)
        for k in range(K):
            named += jnp.where(spr[src, 64 + k : 65 + k, 0:T] == ir, sel[k : k + 1, 0:T], 0.0)
        return dot((spr[src, 0:64, 0:T] + named).astype(BF16), tokr[src])

    wsum = weight_term(xc, selb)
    for a, k in reversed(xpeers):
        src = m4(x + a) * 2 + lax.rem(c + k, 2)
        got(selr.at[src], lg_r.at[src])
        wsum += weight_term(src, selr.at[src])
    shift = x * 720 - (x * 720) // 128 * 128
    wsum = pltpu.roll(wsum, lax.rem(BLK - shift, BLK), 1)
    for n in range(16):
        rss[n] = wsum[4 * n : 4 * n + 4, 0:OUT]

    chip = y * 4 + z
    hops = lambda v: min(v[0], 4 - v[0]) + min(v[1], 4 - v[1])
    for n, (a, b) in enumerate(sorted([(a, b) for a in range(4) for b in range(4) if a or b], key=hops, reverse=True)):
        dest = m4(y + a) * 4 + m4(z + b)
        send(rss.at[dest], rsr.at[chip], rs_s.at[n], rs_r.at[chip], at(dy=a, dz=b))
    rsr[chip] = rss[chip]

    for a in (1, 2, 3):
        got(xpr.at[m4(x + a)], xp_r.at[m4(x + a)])
    ps_row = jnp.sum(xpr[...], axis=0)[0:1, :]
    loss_o[0] = E * jnp.sum((cnt_row / (TOTAL * K)) * (ps_row / TOTAL))

    for a in range(4):
        for b in range(4):
            if a or b:
                src = m4(y + a) * 4 + m4(z + b)
                got(rsr.at[src], rs_r.at[src])
    out = jnp.sum(rsr[...], axis=0) * (1.0 / math.sqrt(TOTAL))
    wt_o[...] = out[:, 0:720]
    for s in sent:
        s.wait_send()


def on_device(tokens, out_grad, indices, expert_rows, router_weight, router_bias, balance_scale):
    rows = jnp.transpose(expert_rows[0], (0, 2, 1, 3)).reshape(ES, 32, D)
    dma = pltpu.SemaphoreType.DMA
    vm = pltpu.VMEM
    scratch = [
        vm((T, D), BF16), vm((T, DPAD), BF16), vm((T, D), BF16), vm((4 * T, WIDTH[0]), BF16), vm((4 * T, WIDTH[1]), BF16),
        vm((K, T), I32), vm((4, ES, 8, D), BF16), vm((4 * KQ, DPAD), BF16), vm((D, E), BF16), vm((1, E), F32),
        vm((4, 2 * ROWS, WIDTH[0]), BF16), vm((4, 2 * ROWS, WIDTH[1]), BF16),
        vm((2, ROWS, WIDTH[0]), BF16), vm((2, ROWS, WIDTH[1]), BF16),
        vm((8, ROWS, WIDTH[0]), BF16), vm((8, ROWS, WIDTH[1]), BF16), vm((8, T, BLK), BF16),
        vm((8, E), F32), vm((4, 8, 8, E), F32), vm((K, 256, E), BF16), vm((8, 256), F32), vm((2, 4, 8, 256), F32),
        vm((2, K, 4 * T), F32), vm((2, K, 8, 4 * T), F32), vm((2, 2 * ROWS, 4 * T), F32), vm((2, 4, K, 256), F32), vm((2, 4, K, 256), F32),
        vm((8, E), F32), vm((8, 8, E), F32), vm((4, 8, E), F32), vm((8, E), F32),
        vm((8, E), F32), vm((4, 8, E), F32), vm((8, E), F32), vm((4, 8, E), F32),
        vm((E, T), F32), vm((E, T), F32), vm((K, T), F32), vm((2, 72, 256), F32), vm((8, 72, 256), F32),
        vm((K, 256), F32), vm((8, K, 256), F32), vm((16, 4, OUT), F32), vm((16, 4, OUT), F32), pltpu.SMEM((1,), F32),
        dma((10,)), dma((2, 2, 3)), dma((2, 2, 3)), dma((2, 2, N)), dma((2, 2, N)), dma((2, 2, N)), dma((2, 2, 2, N)), dma((2, N)), dma((2, 8, N)),
        dma((7,)), dma((8,)), dma((3,)), dma((4,)), dma((2, 3)), dma((2, 4)), dma((7,)), dma((8,)), dma((3,)), dma((4,)),
        dma((3,)), dma((4,)), dma((3,)), dma((4,)), dma((7,)), dma((8,)), dma((2, 3)), dma((2, 4)), dma((7,)), dma((8,)), dma((7,)), dma((8,)), dma((15,)), dma((16,)),
    ]
    hbm = pl.BlockSpec(memory_space=pl.ANY)
    logit_grad, weight_grad, loss = pl.pallas_call(
        kernel,
        out_shape=(
            jax.ShapeDtypeStruct((T, E), BF16),
            jax.ShapeDtypeStruct((4, 720), F32),
            jax.ShapeDtypeStruct((1,), F32),
        ),
        in_specs=[hbm] * 7,
        out_specs=(
            pl.BlockSpec(memory_space=pltpu.VMEM),
            pl.BlockSpec(memory_space=pltpu.VMEM),
            pl.BlockSpec(memory_space=pltpu.SMEM),
        ),
        scratch_shapes=scratch,
        compiler_params=pltpu.CompilerParams(collective_id=0, has_side_effects=True, vmem_limit_bytes=64000 * 1024),
        name="router",
    )(tokens, out_grad, indices.T, rows, router_weight, router_bias.reshape(1, E), balance_scale)
    token_grad = dot(logit_grad, router_weight, ((1,), (1,))).astype(BF16)
    return token_grad, weight_grad.T, loss


def solution(mesh):
    torus = Mesh(mesh.devices.reshape(4, 4, 2, mesh.shape["dp"]), AXES)
    return jax.shard_map(
        on_device,
        mesh=torus,
        in_specs=(P(AXES, None), P(AXES, None), P(AXES, None), P("dp", EP, None, None, None), P(), P(), P()),
        out_specs=(P(AXES, None), P("dp", EP), P()),
        check_vma=False,
    )
```

```python
import math

import jax
import jax.numpy as jnp
from jax import lax
from jax.experimental import pallas as pl
from jax.experimental.pallas import tpu as pltpu
from jax.sharding import Mesh
from jax.sharding import PartitionSpec as P

AXES = ("ep_0", "ep_1", "ep_2", "dp")
EP = AXES[:3]
MESH = pl.DeviceIdType.MESH
F32, BF16, I32 = jnp.float32, jnp.bfloat16, jnp.int32

D, E, T, K, CAP = 2880, 128, 192, 4, 9
DPAD = 2944
SPLIT = 1536
WIDTH = (SPLIT, DPAD - SPLIT)
PER = 27
ROWS = 112
MAIN, LAST = 96, 16
ES = 4 * CAP
KQ = ES * 8
PIECES = (((0, 640), (640, 512), (1152, 384)), ((0, 640), (640, 512), (1152, 256)))
N = 3
BLK = 896
OUT = 768
TOTAL = 24576
G_EX, G_OWN, G_OG, G_ME, G_PD = 0, 2, 4, 6, 8
G_C1, G_C2, G_P1, G_P2, G_XC, G_XP, G_TK, G_SP, G_LG, G_RS = range(10, 20)


def dot(a, b, dims=((1,), (0,)), **kw):
    return lax.dot_general(a, b, (dims, ((), ())), preferred_element_type=F32, **kw)


def iota(shape, dim):
    return lax.broadcasted_iota(I32, shape, dim)


def kernel(
    tok_h, og_h, idx_h, ex_h, w_h, b_h, bs_h,
    lg_o, wt_o, loss_o,
    tokraw, tokp, ogfull, og0, og1, idxv, ev3, ev, wv, bv,
    snd0, snd1, tr0, tr1, ex0, ex1, exl0, exl1, tokr,
    cntsnd, cntr, cc_v, meta, metar, rowsel, rowlast, acc, gbuf, pds, pdr,
    psb, psr1, psr2, psb2, xcs, xcr, xps, xpr,
    lt, pt, mixv, spb, spr, selb, selr, rss, rsr, bs_s, lgv, wtv, lossv,
    loc, ss, rr, og_r, ex2_r, exr, last_r, lg_r,
):
    y, z, c, x = (lax.axis_index(a) for a in AXES)
    og, snd, tr, ex, exl = (og0, og1), (snd0, snd1), (tr0, tr1), (ex0, ex1), (exl0, exl1)
    m4 = lambda v: lax.rem(v + 4, 4)
    po = (z, y)
    pe = (y, z)
    other = 1 - c

    def at(dy=0, dz=0, cc=None, dx=0):
        return (m4(y + dy), m4(z + dz), c if cc is None else cc, m4(x + dx))

    og_dev = (lambda s: at(dz=s), lambda s: at(dy=s))
    ex_dev = (lambda s, cc: at(dy=s, cc=cc), lambda s, cc: at(dz=s, cc=cc))

    def remote(src, dst, ss, rs, dev):
        return pltpu.make_async_remote_copy(src_ref=src, dst_ref=dst, send_sem=ss, recv_sem=rs, device_id=dev, device_id_type=MESH)

    def send(src, dst, group, recv, dev):
        remote(src, dst, ss.at[group], recv, dev).start()

    def got(ref, sem):
        remote(ref, ref, sem, sem, at(dx=1)).wait_recv()

    def drain(ref, group):
        remote(ref, ref, ss.at[group], ss.at[group], at(dx=1)).wait_send()

    loads = [
        pltpu.make_async_copy(idx_h, idxv, loc.at[0]),
        pltpu.make_async_copy(og_h, ogfull, loc.at[1]),
        pltpu.make_async_copy(tok_h, tokraw, loc.at[2]),
        pltpu.make_async_copy(w_h, wv, loc.at[3]),
        pltpu.make_async_copy(b_h, bv, loc.at[4]),
    ] + [pltpu.make_async_copy(ex_h.at[:, q * 8 : q * 8 + 8, :], ev3.at[q], loc.at[5 + q]) for q in range(4)]
    loads.append(pltpu.make_async_copy(bs_h, bs_s, loc.at[9]))
    for l in loads:
        l.start()
    peers = [at(dy=a, dz=b) for a in range(4) for b in range(4) if a or b]
    peers += [at(dy=a, cc=other) for a in (1, 2, 3)] + [at(dz=a, cc=other) for a in (1, 2, 3)]
    peers += [at(cc=other)] + [at(dx=a, cc=k) for a in (1, 2, 3) for k in (c, other)]
    barrier = pltpu.get_barrier_semaphore()
    for p in peers:
        pl.semaphore_signal(barrier, inc=1, device_id=p, device_id_type=MESH)

    loads[0].wait()
    idx = idxv[...]
    ie = iota((E, T), 0)
    named = jnp.zeros((E, T), F32)
    for k in range(K):
        named += jnp.where(idx[k : k + 1, :] == ie, 1.0, 0.0)
    nb = named.astype(BF16)
    upper = jnp.where(iota((T, T), 0) < iota((T, T), 1), 1.0, 0.0).astype(BF16)
    ones_tt = jnp.ones((T, T), BF16)
    r_e, c_e = iota((E, E), 0), iota((E, E), 1)
    same_ep = jnp.where((r_e // 4 == c_e // 4) & (c_e < r_e), 1.0, 0.0).astype(BF16)
    ahead = dot(same_ep, nb).astype(BF16)
    rowpos = dot(nb, upper) + dot(ahead, ones_tt)
    cntsnd[...] = dot(jnp.ones((8, T), BF16), nb, ((1,), (1,)))
    meta[...] = jnp.full((8, 256), -1e6, F32)
    for k in range(K):
        ik = idx[k : k + 1, :]
        off = jnp.sum(jnp.where(ik == ie, rowpos, 0.0), axis=0, keepdims=True)
        ey, ez, ec = ik // 32, (ik // 8) % 4, (ik // 4) % 2
        for h, (ea, eb) in enumerate(((ey, ez), (ez, ey))):
            step, same = (ea - pe[h] + 4) % 4, ec == c
            near = jnp.where(step == 1, jnp.where(same, 2, 6), jnp.where(same, 3, 7))
            slot = jnp.where(step == 0, jnp.where(same, 0, 1), jnp.where(step == 2, 4 + ec, near))
            code = (eb * 1024 + slot * 32).astype(F32) + off
            meta[4 * h + k : 4 * h + k + 1, 0:T] = code

    loads[1].wait()
    own_og = [pl.ds(pl.multiple_of(po[h] * T, T), T) for h in range(2)]
    og0[own_og[0], :] = ogfull[:, 0:SPLIT]
    og1[own_og[1], WIDTH[1] - 128 : WIDTH[1]] = jnp.zeros((T, 128), BF16)
    og1[own_og[1], 0 : D - SPLIT] = ogfull[:, SPLIT:D]
    pl.semaphore_wait(barrier, len(peers))

    zc = z * 2 + c
    cntr[y, zc] = cntsnd[...]
    zpeers = [(b, k) for b in (1, 2, 3) for k in (0, 1)] + [(0, 1)]
    zdev = lambda b, k: at(dz=b, cc=lax.rem(c + k, 2))
    for n, (b, k) in enumerate(zpeers):
        send(cntsnd, cntr.at[y, zc], G_C1, rr.at[0], zdev(b, k))
    for h in range(2):
        for s in (1, 2, 3):
            send(meta, metar.at[h, po[h]], G_ME + h, rr.at[2 + h], og_dev[h](s))

    def og_rows(pos, second):
        return pl.ds(pl.multiple_of(pos * T + second * 96, 32), 96)

    def og_send(h, d, m):
        where = og_rows(po[h], d ^ m)
        send(og[h].at[where, :], og[h].at[where, :], G_OG + h, og_r.at[h, 2 if m else d], og_dev[h](1 - 2 * d))

    for h in range(2):
        for d in range(2):
            og_send(h, d, 0)

    got(cntr.at[0, 0:7], rr.at[0])
    for s in (1, 2, 3):
        send(cntr.at[y], cntr.at[y], G_C2, rr.at[1], at(dy=s))
    for h in range(2):
        for d in range(2):
            og_send(h, d, 1)

    loads[2].wait()
    tokp[:, DPAD - 128 : DPAD] = jnp.zeros((T, 128), BF16)
    tokp[:, 0:D] = tokraw[...]

    def block(pos):
        return pl.ds(pl.multiple_of((pos * 720) // 128 * 128, 128), BLK)

    xc = x * 2 + c
    xpeers = [(a, k) for a in (1, 2, 3) for k in (0, 1)] + [(0, 1)]
    xdev = lambda a, k: at(dx=a, cc=lax.rem(c + k, 2))
    tokr[xc] = tokp[:, block(x)]
    for n, (a, k) in enumerate(xpeers):
        send(tokp.at[:, block(m4(x + a))], tokr.at[xc], G_TK, rr.at[4], xdev(a, k))

    loads[3].wait()
    loads[4].wait()
    logits = jnp.transpose(dot(tokp[:, 0:D], wv[...]) + bv[...])
    lt[...] = logits
    ex_l = jnp.exp(logits - jnp.max(logits, axis=0, keepdims=True))
    prob = ex_l / jnp.sum(ex_l, axis=0, keepdims=True)
    pt[...] = prob
    picked = [jnp.sum(jnp.where(idx[k : k + 1, :] == ie, logits, 0.0), axis=0, keepdims=True) for k in range(K)]
    top = jnp.maximum(jnp.maximum(picked[0], picked[1]), jnp.maximum(picked[2], picked[3]))
    picked = [jnp.exp(p - top) for p in picked]
    total = picked[0] + picked[1] + picked[2] + picked[3]
    for k in range(K):
        mixv[k : k + 1, :] = picked[k] / total
    diag = r_e == c_e
    pcol = jnp.sum(prob, axis=1, keepdims=True)
    prow = jnp.sum(jnp.where(diag, pcol, 0.0), axis=0, keepdims=True)
    psb[...] = jnp.broadcast_to(prow, (8, E))
    for n, (b, k) in enumerate(zpeers):
        send(psb, psr1.at[zc], G_P1, rr.at[5], zdev(b, k))
    psr1[zc] = psb[...]

    for q in range(4):
        loads[5 + q].wait()
    ev[:, DPAD - 128 : DPAD] = jnp.zeros((4 * KQ, 128), BF16)

    def flatten(n, _):
        q, p = n // (ES // 2), lax.rem(n, ES // 2)
        pair = jnp.concatenate([ev3[q, 2 * p], ev3[q, 2 * p + 1]], axis=0)
        ev[pl.ds(pl.multiple_of(n * 16, 16), 16), 0:D] = pair
        return 0

    lax.fori_loop(0, 4 * ES // 2, flatten, 0)

    def og_from(d, h):
        return m4(po[h] - (1 - 2 * d))

    for h in range(2):
        for d in range(2):
            where = og_rows(og_from(d, h), d)
            got(og[h].at[where, :], og_r.at[h, d])
            send(og[h].at[where, :], og[h].at[where, :], G_OG + h, og_r.at[h, 2], og_dev[h](1 - 2 * d))

    got(cntr.at[0:3], rr.at[1])
    counts = cntr[...]
    plane = jnp.sum(counts.reshape(32, 8, E), axis=0)
    xcs[...] = plane
    xcr[x] = plane
    for a in (1, 2, 3):
        send(xcs, xcr.at[x], G_XC, rr.at[7], at(dx=a))
    first = (y * 8 + z * 2 + c) * 4
    cb = counts.reshape(256, E).astype(BF16)
    for k in range(K):
        mine = jnp.where((r_e >= first) & (r_e <= first + k), 1.0, 0.0).astype(BF16)
        cc_v[k] = dot(cb, mine).astype(BF16)

    def gather(h, delta):
        q = m4(pe[h] + delta)
        row = iota((2 * ROWS, E), 0)
        core = jnp.where(row >= ROWS, 1, 0)
        rr = row - core * ROWS
        i = jnp.where(rr >= PER, 1, 0) + jnp.where(rr >= 2 * PER, 1, 0) + jnp.where(rr >= 3 * PER, 1, 0)
        r = rr - i * PER
        i = i + po[h] + 1
        i = jnp.where(i >= 4, i - 4, i)
        dev = (q * 8 + i * 2 + core) if h == 0 else (i * 8 + q * 2 + core)
        pick = (jnp.broadcast_to(dev[:, 0:1] * 8, (2 * ROWS, 256)) == iota((2 * ROWS, 256), 1))
        pick = jnp.where(pick, 1.0, 0.0).astype(BF16)
        t = [dot(pick, cc_v[k]).astype(I32) for k in range(K)]
        e_in = jnp.where(r >= t[0], 1, 0) + jnp.where(r >= t[1], 1, 0) + jnp.where(r >= t[2], 1, 0)
        base = jnp.where(r >= t[2], t[2], jnp.where(r >= t[1], t[1], jnp.where(r >= t[0], t[0], 0)))
        es = e_in * CAP + r - base
        target = (es * 8 + i * 2 + core) if h == 0 else (i * KQ + es * 8 + q * 2 + core)
        target = jnp.where((r < t[3]) & (rr < 4 * PER), target, -1)
        depth = KQ if h == 0 else 4 * KQ
        sel = jnp.broadcast_to(target[:, 0:1], (2 * ROWS, depth)) == iota((2 * ROWS, depth), 1)
        sel = jnp.where(sel, 1.0, 0.0).astype(BF16)
        rows = pl.ds(pl.multiple_of(q * KQ, KQ), KQ) if h == 0 else pl.ds(0, 4 * KQ)
        for lo, w in PIECES[h]:
            snd[h][delta, :, lo : lo + w] = dot(sel, ev[rows, h * SPLIT + lo : h * SPLIT + lo + w]).astype(BF16)

    def core_rows(cc):
        return pl.ds(pl.multiple_of(cc * ROWS, 16), ROWS)

    def piece(h, ref, row, n):
        if n == N:
            return ref.at[pl.ds(pl.multiple_of(row + MAIN, 16), LAST), :]
        return ref.at[pl.ds(pl.multiple_of(row, 16), MAIN), pl.ds(*PIECES[h][n])]

    def landing(h, slot, n):
        return exl[h].at[slot] if n == N else ex[h].at[slot, :, pl.ds(*PIECES[h][n])]

    def landed(h, pair, n):
        return last_r.at[h] if n == N else exr.at[h, pair, n]

    for h in range(2):
        gather(h, 2)
        for d in range(2):
            for n in range(N + 1):
                send(
                    piece(h, snd[h].at[2], d * ROWS, n), piece(h, tr[h].at[d], 0, n),
                    G_EX + h, ex2_r.at[h, d, n], ex_dev[h](1 - 2 * d, c),
                )

    def gather_rest(o, _):
        delta = jnp.where(o == 0, 1, jnp.where(o == 1, 3, 0))
        gather(0, delta)
        gather(1, delta)
        return 0

    lax.fori_loop(0, 3, gather_rest, 0)

    def ex1_send(far, pieces):
        cc = other if far else c
        for n in pieces:
            for h in range(2):
                for d in range(2):
                    slot = 3 - d + 4 * far
                    send(
                        piece(h, snd[h].at[1 + 2 * d], cc * ROWS, n), landing(h, slot, n),
                        G_EX + h, landed(h, 1 + 2 * far, n), ex_dev[h](1 - 2 * d, cc),
                    )

    ex1_send(0, range(N))
    for h in range(2):
        for n in range(N + 1):
            send(piece(h, snd[h].at[0], other * ROWS, n), landing(h, 1, n), G_OWN + h, landed(h, 0, n), at(cc=other))
        ex[h][0] = snd[h][0, pl.ds(pl.multiple_of(c * ROWS, 16), MAIN), :]
        exl[h][0] = snd[h][0, pl.ds(pl.multiple_of(c * ROWS + MAIN, 16), LAST), :]

    for h in range(2):
        got(metar.at[h, 0:3], rr.at[2 + h])
        metar[h, po[h]] = meta[...]
        for i in range(4):
            code = metar[h, i, 4 * h : 4 * h + 4, 0:T].astype(I32) - po[h] * 1024
            slot = code // 32
            place = code - slot * 32 + m4(i - po[h] - 1) * PER
            valid = (code >= 0) & (code < 256)
            rowsel[h, :, i * T : (i + 1) * T] = jnp.where(valid & (place < MAIN), slot * MAIN + place, -1).astype(F32)
            rowlast[h, i] = jnp.where(valid & (place >= MAIN), slot * LAST + place - MAIN, -1).astype(F32)
        got(og[h].at[0 : 2 * T, :], og_r.at[h, 2])
    acc[...] = jnp.zeros_like(acc)

    def absorb(pair, mine):
        for n in range(N):
            for h in range(2):
                if mine:
                    got(landing(h, 1, n), landed(h, 0, n))
                else:
                    got(ex[h].at[pl.ds(2 * pair, 2), :, pl.ds(*PIECES[h][n])], landed(h, pair, n))
                lo, w = PIECES[h][n]
                block = ex[h][pl.ds(2 * pair, 2), :, lo : lo + w].reshape(2 * MAIN, w)
                part = dot(block, og[h][:, lo : lo + w], ((1,), (1,)))
                if n == 0:
                    gbuf[h] = part
                else:
                    gbuf[h] += part
        rid = (iota((2 * MAIN, 128), 0) + pair * 2 * MAIN).astype(F32)
        for h in range(2):
            for lb in range(6):
                lanes = slice(lb * 128, lb * 128 + 128)
                g = gbuf[h, :, lanes]
                for k in range(K):
                    hit = jnp.where(rid == rowsel[h, k : k + 1, lanes], g, 0.0)
                    acc[h, k, :, lanes] += jnp.sum(hit.reshape(2 * MAIN // 8, 8, 128), axis=0)

    absorb(0, True)

    def forward(n):
        for h in range(2):
            for d in range(2):
                got(piece(h, tr[h].at[d], 0, n), ex2_r.at[h, d, n])
                send(
                    piece(h, tr[h].at[d], 0, n), landing(h, 4 + c, n),
                    G_EX + h, landed(h, 2, n), ex_dev[h](1 - 2 * d, d),
                )

    for n in range(N):
        forward(n)
    ex1_send(1, range(N))
    forward(N)
    for far in range(2):
        ex1_send(far, (N,))

    got(psr1.at[0:7], rr.at[5])
    psb2[...] = jnp.sum(psr1[...], axis=0)
    psr2[y] = psb2[...]
    for s in (1, 2, 3):
        send(psb2, psr2.at[y], G_P2, rr.at[6], at(dy=s))

    got(xcr.at[0:3], rr.at[7])
    cnt_row = jnp.sum(xcr[...], axis=0)[0:1, :]
    cnt_col = jnp.sum(jnp.where(diag, cnt_row, 0.0), axis=1, keepdims=True)
    loads[9].wait()
    push = bs_s[...] * E * (cnt_col / (TOTAL * K))
    prob = pt[...]
    spread = prob * (push - jnp.sum(prob * push, axis=0, keepdims=True))
    lt[...] = spread
    spb[...] = jnp.zeros_like(spb)
    for par in range(2):
        for n in range(16):
            spb[par, 4 * n : 4 * n + 4, 0:T] = spread[8 * n + 4 * par : 8 * n + 4 * par + 4, :]
        for k in range(K):
            ik = idxv[k : k + 1, :]
            spb[par, 64 + k : 65 + k, 0:T] = jnp.where((ik // 4) % 2 == par, ik // 8 * 4 + ik % 4, -1).astype(F32)
    for n, (a, k) in enumerate(xpeers):
        send(spb.at[lax.rem(c + k, 2)], spr.at[xc], G_SP, rr.at[9], xdev(a, k))
    spr[xc] = spb[c]

    def arrivals(pair, _):
        absorb(pair, False)
        return 0

    lax.fori_loop(1, 4, arrivals, 0)

    for h in range(2):
        for i in range(4):
            pds[h, i] = jnp.zeros((K, 256), F32)
            for k in range(K):
                pds[h, i, k : k + 1, 0:T] = jnp.sum(acc[h, k, :, i * T : (i + 1) * T], axis=0, keepdims=True)
        for s in (1, 2, 3):
            send(pds.at[h, m4(po[h] + s)], pdr.at[h, po[h]], G_PD + h, rr.at[10 + h], og_dev[h](s))
        pdr[h, po[h]] = pds[h, po[h]]
    got(psr2.at[0:3], rr.at[6])
    xps[...] = jnp.sum(psr2[...], axis=0)
    xpr[x] = xps[...]
    for a in (1, 2, 3):
        send(xps, xpr.at[x], G_XP, rr.at[8], at(dx=a))
    late = [jnp.zeros((1, T), F32)] * K
    rid = iota((8 * LAST, T), 0).astype(F32)
    for h in range(2):
        got(exl[h].at[1:8], last_r.at[h])
        g = dot(exl[h][...].reshape(8 * LAST, WIDTH[h]), og[h][own_og[h], :], ((1,), (1,)))
        for k in range(K):
            hit = jnp.where(rid == rowlast[h, po[h], k : k + 1, :], g, 0.0)
            late[k] += jnp.sum(hit, axis=0, keepdims=True)

    pd = jnp.zeros((K, 256), F32)
    for h in range(2):
        got(pdr.at[h, 0:3], rr.at[10 + h])
        pd += (pdr[h, 0] + pdr[h, 1]) + (pdr[h, 2] + pdr[h, 3])

    dots = [pd[k : k + 1, 0:T] + late[k] for k in range(K)]
    mix = [mixv[k : k + 1, :] for k in range(K)]
    mean = mix[0] * dots[0] + mix[1] * dots[1] + mix[2] * dots[2] + mix[3] * dots[3]
    for k in range(K):
        selb[k : k + 1, 0:T] = mix[k] * (dots[k] - mean)
    selb[:, T:256] = jnp.zeros((K, 256 - T), F32)
    for n, (a, k) in enumerate(xpeers):
        send(selb, selr.at[xc], G_LG, lg_r.at[xc], xdev(a, k))

    lg = jnp.zeros((E, T), F32)
    for k in range(K):
        lg += jnp.where(idxv[k : k + 1, :] == ie, selb[k : k + 1, 0:T], 0.0)
    lgv[...] = jnp.transpose(lt[...] + lg).astype(BF16)
    out_lg = pltpu.make_async_copy(lgv, lg_o, loc.at[10])
    out_lg.start()
    got(tokr.at[0:7], rr.at[4])
    got(spr.at[0:7], rr.at[9])

    ir = iota((64, T), 0).astype(F32)

    def weight_term(src, sel):
        named = jnp.zeros((64, T), F32)
        for k in range(K):
            named += jnp.where(spr[src, 64 + k : 65 + k, 0:T] == ir, sel[k : k + 1, 0:T], 0.0)
        return dot((spr[src, 0:64, 0:T] + named).astype(BF16), tokr[src])

    wsum = weight_term(xc, selb)
    for a, k in reversed(xpeers):
        src = m4(x + a) * 2 + lax.rem(c + k, 2)
        got(selr.at[src], lg_r.at[src])
        wsum += weight_term(src, selr.at[src])
    shift = x * 720 - (x * 720) // 128 * 128
    wsum = pltpu.roll(wsum, lax.rem(BLK - shift, BLK), 1)
    for n in range(16):
        rss[n] = wsum[4 * n : 4 * n + 4, 0:OUT]

    chip = y * 4 + z
    hops = lambda v: min(v[0], 4 - v[0]) + min(v[1], 4 - v[1])
    for n, (a, b) in enumerate(sorted([(a, b) for a in range(4) for b in range(4) if a or b], key=hops, reverse=True)):
        dest = m4(y + a) * 4 + m4(z + b)
        send(rss.at[dest], rsr.at[chip], G_RS, rr.at[12], at(dy=a, dz=b))
    rsr[chip] = rss[chip]

    got(xpr.at[0:3], rr.at[8])
    ps_row = jnp.sum(xpr[...], axis=0)[0:1, :]
    lossv[0] = E * jnp.sum((cnt_row / (TOTAL * K)) * (ps_row / TOTAL))

    out_loss = pltpu.make_async_copy(lossv, loss_o, loc.at[11])
    out_loss.start()
    for h in range(2):
        drain(snd[h], G_EX + h)
        drain(snd[h].at[0, 0:ROWS, :], G_OWN + h)
        drain(og[h].at[0 : 3 * T, :], G_OG + h)
        drain(metar.at[h, 0:3], G_ME + h)
        drain(pdr.at[h, 0:3], G_PD + h)
    for ref, group in (
        (cntr.at[0, 0:7], G_C1), (cntr.at[0:3], G_C2), (psr1.at[0:7], G_P1), (psr2.at[0:3], G_P2), (xcr.at[0:3], G_XC), (xpr.at[0:3], G_XP),
        (tokr.at[0:7], G_TK), (spr.at[0:7], G_SP), (selr.at[0:7], G_LG), (rsr.at[0:15], G_RS),
    ):
        drain(ref, group)
    out_lg.wait()
    got(rsr.at[0:15], rr.at[12])
    out = jnp.sum(rsr[...], axis=0) * (1.0 / math.sqrt(TOTAL))
    wtv[...] = out[:, 0:720]
    out_wt = pltpu.make_async_copy(wtv, wt_o, loc.at[12])
    out_wt.start()
    out_loss.wait()
    out_wt.wait()


def finish(lg_h, w_h, wt_h, loss_h, tg_o, wt_o, loss_o, lgv, wv, tgv, sem):
    lg_in = pltpu.make_async_copy(lg_h, lgv, sem.at[0])
    lg_in.start()
    w_in = pltpu.make_async_copy(w_h, wv, sem.at[5])
    w_in.start()
    moves = [pltpu.make_async_copy(wt_h, wt_o, sem.at[1]), pltpu.make_async_copy(loss_h, loss_o, sem.at[2])]
    for m in moves:
        m.start()
    lg_in.wait()
    w_in.wait()
    for n in range(2):
        rows = pl.ds(n * 96, 96)
        tgv[rows, :] = dot(lgv[rows, :], wv[...], ((1,), (1,))).astype(BF16)
        moves.append(pltpu.make_async_copy(tgv.at[rows, :], tg_o.at[rows, :], sem.at[3 + n]))
        moves[-1].start()
    for m in moves:
        m.wait()


def on_device(tokens, out_grad, indices, expert_rows, router_weight, router_bias, balance_scale):
    rows = jnp.transpose(expert_rows[0], (0, 2, 1, 3)).reshape(ES, 32, D)
    dma = pltpu.SemaphoreType.DMA
    vm = pltpu.VMEM
    scratch = [
        vm((T, D), BF16), vm((T, DPAD), BF16), vm((T, D), BF16), vm((4 * T, WIDTH[0]), BF16), vm((4 * T, WIDTH[1]), BF16),
        vm((K, T), I32), vm((4, ES, 8, D), BF16), vm((4 * KQ, DPAD), BF16), vm((D, E), BF16), vm((1, E), F32),
        vm((4, 2 * ROWS, WIDTH[0]), BF16), vm((4, 2 * ROWS, WIDTH[1]), BF16),
        vm((2, ROWS, WIDTH[0]), BF16), vm((2, ROWS, WIDTH[1]), BF16),
        vm((8, MAIN, WIDTH[0]), BF16), vm((8, MAIN, WIDTH[1]), BF16), vm((8, LAST, WIDTH[0]), BF16), vm((8, LAST, WIDTH[1]), BF16),
        vm((8, T, BLK), BF16),
        vm((8, E), F32), vm((4, 8, 8, E), F32), vm((K, 256, E), BF16), vm((8, 256), F32), vm((2, 4, 8, 256), F32),
        vm((2, K, 4 * T), F32), vm((2, 4, K, T), F32), vm((2, K, 8, 4 * T), F32), vm((2, 2 * MAIN, 4 * T), F32), vm((2, 4, K, 256), F32), vm((2, 4, K, 256), F32),
        vm((8, E), F32), vm((8, 8, E), F32), vm((4, 8, E), F32), vm((8, E), F32),
        vm((8, E), F32), vm((4, 8, E), F32), vm((8, E), F32), vm((4, 8, E), F32),
        vm((E, T), F32), vm((E, T), F32), vm((K, T), F32), vm((2, 72, 256), F32), vm((8, 72, 256), F32),
        vm((K, 256), F32), vm((8, K, 256), F32), vm((16, 4, OUT), F32), vm((16, 4, OUT), F32), vm((1, 1), F32), vm((T, E), BF16), vm((4, 720), F32), pltpu.SMEM((1,), F32),
        dma((13,)), dma((20,)), dma((13,)), dma((2, 3)), dma((2, 2, N + 1)), dma((2, 4, N)), dma((2,)), dma((8,)),
    ]
    hbm = pl.BlockSpec(memory_space=pltpu.HBM)
    logit_grad, weight_grad, loss = pl.pallas_call(
        kernel,
        out_shape=(
            jax.ShapeDtypeStruct((T, E), BF16),
            jax.ShapeDtypeStruct((4, 720), F32),
            jax.ShapeDtypeStruct((1,), F32),
        ),
        in_specs=[hbm] * 7,
        out_specs=(hbm, hbm, hbm),
        scratch_shapes=scratch,
        compiler_params=pltpu.CompilerParams(collective_id=0, has_side_effects=True, vmem_limit_bytes=64000 * 1024),
        name="router",
    )(tokens, out_grad, indices.T, rows, router_weight, router_bias.reshape(1, E), balance_scale.reshape(1, 1))
    token_grad, weight_grad, loss = pl.pallas_call(
        finish,
        out_shape=(
            jax.ShapeDtypeStruct((T, D), BF16),
            jax.ShapeDtypeStruct((4, 720), F32),
            jax.ShapeDtypeStruct((1,), F32),
        ),
        in_specs=[hbm] * 4,
        out_specs=(hbm, hbm, hbm),
        scratch_shapes=[vm((T, E), BF16), vm((D, E), BF16), vm((T, D), BF16), dma((6,))],
        name="finish",
    )(logit_grad, router_weight, weight_grad, loss)
    return token_grad, weight_grad.T, loss


def solution(mesh):
    torus = Mesh(mesh.devices.reshape(4, 4, 2, mesh.shape["dp"]), AXES)
    return jax.shard_map(
        on_device,
        mesh=torus,
        in_specs=(P(AXES, None), P(AXES, None), P(AXES, None), P("dp", EP, None, None, None), P(), P(), P()),
        out_specs=(P(AXES, None), P("dp", EP), P()),
        check_vma=False,
    )
```

```python
import math

import jax
import jax.numpy as jnp
from jax import lax
from jax.experimental import pallas as pl
from jax.experimental.pallas import tpu as pltpu
from jax.sharding import Mesh
from jax.sharding import PartitionSpec as P

AXES = ("ep_0", "ep_1", "ep_2", "dp")
EP = AXES[:3]
MESH = pl.DeviceIdType.MESH
F32, BF16, I32 = jnp.float32, jnp.bfloat16, jnp.int32

D, E, T, K, CAP = 2880, 128, 192, 4, 9
DPAD = 2944
SPLIT = 1536
WIDTH = (SPLIT, DPAD - SPLIT)
PER = 27
ROWS = 112
MAIN, LAST = 96, 16
ES = 4 * CAP
KQ = ES * 8
PIECES = (((0, 640), (640, 512), (1152, 384)), ((0, 640), (640, 512), (1152, 256)))
N = 3
BLK = 896
OUT = 768
TOTAL = 24576
G_EX, G_OWN, G_OG, G_ME, G_PD = 0, 2, 4, 6, 8
G_C1, G_C2, G_P1, G_P2, G_XC, G_XP, G_TK, G_SP, G_LG, G_RS = range(10, 20)


def dot(a, b, dims=((1,), (0,)), **kw):
    return lax.dot_general(a, b, (dims, ((), ())), preferred_element_type=F32, **kw)


def iota(shape, dim):
    return lax.broadcasted_iota(I32, shape, dim)


def kernel(
    tok_h, og_h, idx_h, ex_h, w_h, b_h, bs_s,
    tg_o, small_o,
    tokraw, tokp, ogfull, og0, og1, idxv, ev3, ev, wv, bv,
    snd0, snd1, tr0, tr1, ex0, ex1, exl0, exl1, tokr,
    cntsnd, cntr, cc_v, meta, metar, rowsel, rowlast, acc, gbuf, pds, pdr,
    psb, psr1, psr2, psb2, xcs, xcr, xps, xpr,
    lt, pt, mixv, spb, spr, selb, selr, rss, rsr, lgv,
    loc, ss, rr, og_r, ex2_r, exr, last_r, lg_r,
):
    y, z, c, x = (lax.axis_index(a) for a in AXES)
    og, snd, tr, ex, exl = (og0, og1), (snd0, snd1), (tr0, tr1), (ex0, ex1), (exl0, exl1)
    m4 = lambda v: lax.rem(v + 4, 4)
    po = (z, y)
    pe = (y, z)
    other = 1 - c

    def at(dy=0, dz=0, cc=None, dx=0):
        return (m4(y + dy), m4(z + dz), c if cc is None else cc, m4(x + dx))

    og_dev = (lambda s: at(dz=s), lambda s: at(dy=s))
    ex_dev = (lambda s, cc: at(dy=s, cc=cc), lambda s, cc: at(dz=s, cc=cc))

    def remote(src, dst, ss, rs, dev):
        return pltpu.make_async_remote_copy(src_ref=src, dst_ref=dst, send_sem=ss, recv_sem=rs, device_id=dev, device_id_type=MESH)

    def send(src, dst, group, recv, dev):
        remote(src, dst, ss.at[group], recv, dev).start()

    def got(ref, sem):
        remote(ref, ref, sem, sem, at(dx=1)).wait_recv()

    def drain(ref, group):
        remote(ref, ref, ss.at[group], ss.at[group], at(dx=1)).wait_send()

    loads = [
        pltpu.make_async_copy(idx_h, idxv, loc.at[0]),
        pltpu.make_async_copy(og_h, ogfull, loc.at[1]),
        pltpu.make_async_copy(tok_h, tokraw, loc.at[2]),
        pltpu.make_async_copy(w_h, wv, loc.at[3]),
        pltpu.make_async_copy(b_h, bv, loc.at[4]),
    ] + [pltpu.make_async_copy(ex_h.at[:, q * 8 : q * 8 + 8, :], ev3.at[q], loc.at[5 + q]) for q in range(4)]
    for l in loads:
        l.start()
    peers = [at(dy=a, dz=b) for a in range(4) for b in range(4) if a or b]
    peers += [at(dy=a, cc=other) for a in (1, 2, 3)] + [at(dz=a, cc=other) for a in (1, 2, 3)]
    peers += [at(cc=other)] + [at(dx=a, cc=k) for a in (1, 2, 3) for k in (c, other)]
    barrier = pltpu.get_barrier_semaphore()
    for p in peers:
        pl.semaphore_signal(barrier, inc=1, device_id=p, device_id_type=MESH)

    loads[0].wait()
    idx = idxv[...]
    ie = iota((E, T), 0)
    named = jnp.zeros((E, T), F32)
    for k in range(K):
        named += jnp.where(idx[k : k + 1, :] == ie, 1.0, 0.0)
    nb = named.astype(BF16)
    upper = jnp.where(iota((T, T), 0) < iota((T, T), 1), 1.0, 0.0).astype(BF16)
    ones_tt = jnp.ones((T, T), BF16)
    r_e, c_e = iota((E, E), 0), iota((E, E), 1)
    same_ep = jnp.where((r_e // 4 == c_e // 4) & (c_e < r_e), 1.0, 0.0).astype(BF16)
    ahead = dot(same_ep, nb).astype(BF16)
    rowpos = dot(nb, upper) + dot(ahead, ones_tt)
    cntsnd[...] = dot(jnp.ones((8, T), BF16), nb, ((1,), (1,)))
    meta[...] = jnp.full((8, 256), -1e6, F32)
    for k in range(K):
        ik = idx[k : k + 1, :]
        off = jnp.sum(jnp.where(ik == ie, rowpos, 0.0), axis=0, keepdims=True)
        ey, ez, ec = ik // 32, (ik // 8) % 4, (ik // 4) % 2
        for h, (ea, eb) in enumerate(((ey, ez), (ez, ey))):
            step, same = (ea - pe[h] + 4) % 4, ec == c
            near = jnp.where(step == 1, jnp.where(same, 2, 6), jnp.where(same, 3, 7))
            slot = jnp.where(step == 0, jnp.where(same, 0, 1), jnp.where(step == 2, 4 + ec, near))
            code = (eb * 1024 + slot * 32).astype(F32) + off
            meta[4 * h + k : 4 * h + k + 1, 0:T] = code

    loads[1].wait()
    own_og = [pl.ds(pl.multiple_of(po[h] * T, T), T) for h in range(2)]
    og0[own_og[0], :] = ogfull[:, 0:SPLIT]
    og1[own_og[1], WIDTH[1] - 128 : WIDTH[1]] = jnp.zeros((T, 128), BF16)
    og1[own_og[1], 0 : D - SPLIT] = ogfull[:, SPLIT:D]
    pl.semaphore_wait(barrier, len(peers))

    zc = z * 2 + c
    cntr[y, zc] = cntsnd[...]
    zpeers = [(b, k) for b in (1, 2, 3) for k in (0, 1)] + [(0, 1)]
    zdev = lambda b, k: at(dz=b, cc=lax.rem(c + k, 2))
    for n, (b, k) in enumerate(zpeers):
        send(cntsnd, cntr.at[y, zc], G_C1, rr.at[0], zdev(b, k))
    for h in range(2):
        for s in (1, 2, 3):
            send(meta, metar.at[h, po[h]], G_ME + h, rr.at[2 + h], og_dev[h](s))

    def og_rows(pos, second):
        return pl.ds(pl.multiple_of(pos * T + second * 96, 32), 96)

    def og_send(h, d, m):
        where = og_rows(po[h], d ^ m)
        send(og[h].at[where, :], og[h].at[where, :], G_OG + h, og_r.at[h, 2 if m else d], og_dev[h](1 - 2 * d))

    for h in range(2):
        for d in range(2):
            og_send(h, d, 0)

    got(cntr.at[0, 0:7], rr.at[0])
    for s in (1, 2, 3):
        send(cntr.at[y], cntr.at[y], G_C2, rr.at[1], at(dy=s))
    for h in range(2):
        for d in range(2):
            og_send(h, d, 1)

    loads[2].wait()
    tokp[:, DPAD - 128 : DPAD] = jnp.zeros((T, 128), BF16)
    tokp[:, 0:D] = tokraw[...]

    def block(pos):
        return pl.ds(pl.multiple_of((pos * 720) // 128 * 128, 128), BLK)

    xc = x * 2 + c
    xpeers = [(a, k) for a in (1, 2, 3) for k in (0, 1)] + [(0, 1)]
    xdev = lambda a, k: at(dx=a, cc=lax.rem(c + k, 2))
    tokr[xc] = tokp[:, block(x)]
    for n, (a, k) in enumerate(xpeers):
        send(tokp.at[:, block(m4(x + a))], tokr.at[xc], G_TK, rr.at[4], xdev(a, k))

    loads[3].wait()
    loads[4].wait()
    logits = jnp.transpose(dot(tokp[:, 0:D], wv[...]) + bv[...])
    lt[...] = logits
    ex_l = jnp.exp(logits - jnp.max(logits, axis=0, keepdims=True))
    prob = ex_l / jnp.sum(ex_l, axis=0, keepdims=True)
    pt[...] = prob
    picked = [jnp.sum(jnp.where(idx[k : k + 1, :] == ie, logits, 0.0), axis=0, keepdims=True) for k in range(K)]
    top = jnp.maximum(jnp.maximum(picked[0], picked[1]), jnp.maximum(picked[2], picked[3]))
    picked = [jnp.exp(p - top) for p in picked]
    total = picked[0] + picked[1] + picked[2] + picked[3]
    for k in range(K):
        mixv[k : k + 1, :] = picked[k] / total
    diag = r_e == c_e
    pcol = jnp.sum(prob, axis=1, keepdims=True)
    prow = jnp.sum(jnp.where(diag, pcol, 0.0), axis=0, keepdims=True)
    psb[...] = jnp.broadcast_to(prow, (8, E))
    for n, (b, k) in enumerate(zpeers):
        send(psb, psr1.at[zc], G_P1, rr.at[5], zdev(b, k))
    psr1[zc] = psb[...]

    for q in range(4):
        loads[5 + q].wait()
    ev[:, DPAD - 128 : DPAD] = jnp.zeros((4 * KQ, 128), BF16)

    def flatten(n, _):
        q, p = n // (ES // 2), lax.rem(n, ES // 2)
        pair = jnp.concatenate([ev3[q, 2 * p], ev3[q, 2 * p + 1]], axis=0)
        ev[pl.ds(pl.multiple_of(n * 16, 16), 16), 0:D] = pair
        return 0

    lax.fori_loop(0, 4 * ES // 2, flatten, 0)

    def og_from(d, h):
        return m4(po[h] - (1 - 2 * d))

    for h in range(2):
        for d in range(2):
            where = og_rows(og_from(d, h), d)
            got(og[h].at[where, :], og_r.at[h, d])
            send(og[h].at[where, :], og[h].at[where, :], G_OG + h, og_r.at[h, 2], og_dev[h](1 - 2 * d))

    got(cntr.at[0:3], rr.at[1])
    counts = cntr[...]
    plane = jnp.sum(counts.reshape(32, 8, E), axis=0)
    xcs[...] = plane
    xcr[x] = plane
    for a in (1, 2, 3):
        send(xcs, xcr.at[x], G_XC, rr.at[7], at(dx=a))
    first = (y * 8 + z * 2 + c) * 4
    cb = counts.reshape(256, E).astype(BF16)
    for k in range(K):
        mine = jnp.where((r_e >= first) & (r_e <= first + k), 1.0, 0.0).astype(BF16)
        cc_v[k] = dot(cb, mine).astype(BF16)

    def gather(h, delta):
        q = m4(pe[h] + delta)
        row = iota((2 * ROWS, E), 0)
        core = jnp.where(row >= ROWS, 1, 0)
        rr = row - core * ROWS
        i = jnp.where(rr >= PER, 1, 0) + jnp.where(rr >= 2 * PER, 1, 0) + jnp.where(rr >= 3 * PER, 1, 0)
        r = rr - i * PER
        i = i + po[h] + 1
        i = jnp.where(i >= 4, i - 4, i)
        dev = (q * 8 + i * 2 + core) if h == 0 else (i * 8 + q * 2 + core)
        pick = (jnp.broadcast_to(dev[:, 0:1] * 8, (2 * ROWS, 256)) == iota((2 * ROWS, 256), 1))
        pick = jnp.where(pick, 1.0, 0.0).astype(BF16)
        t = [dot(pick, cc_v[k]).astype(I32) for k in range(K)]
        e_in = jnp.where(r >= t[0], 1, 0) + jnp.where(r >= t[1], 1, 0) + jnp.where(r >= t[2], 1, 0)
        base = jnp.where(r >= t[2], t[2], jnp.where(r >= t[1], t[1], jnp.where(r >= t[0], t[0], 0)))
        es = e_in * CAP + r - base
        target = (es * 8 + i * 2 + core) if h == 0 else (i * KQ + es * 8 + q * 2 + core)
        target = jnp.where((r < t[3]) & (rr < 4 * PER), target, -1)
        depth = KQ if h == 0 else 4 * KQ
        sel = jnp.broadcast_to(target[:, 0:1], (2 * ROWS, depth)) == iota((2 * ROWS, depth), 1)
        sel = jnp.where(sel, 1.0, 0.0).astype(BF16)
        rows = pl.ds(pl.multiple_of(q * KQ, KQ), KQ) if h == 0 else pl.ds(0, 4 * KQ)
        for lo, w in PIECES[h]:
            snd[h][delta, :, lo : lo + w] = dot(sel, ev[rows, h * SPLIT + lo : h * SPLIT + lo + w]).astype(BF16)

    def core_rows(cc):
        return pl.ds(pl.multiple_of(cc * ROWS, 16), ROWS)

    def piece(h, ref, row, n):
        if n == N:
            return ref.at[pl.ds(pl.multiple_of(row + MAIN, 16), LAST), :]
        return ref.at[pl.ds(pl.multiple_of(row, 16), MAIN), pl.ds(*PIECES[h][n])]

    def landing(h, slot, n):
        return exl[h].at[slot] if n == N else ex[h].at[slot, :, pl.ds(*PIECES[h][n])]

    def landed(h, pair, n):
        return last_r.at[h] if n == N else exr.at[h, pair, n]

    for h in range(2):
        gather(h, 2)
        for d in range(2):
            for n in range(N + 1):
                send(
                    piece(h, snd[h].at[2], d * ROWS, n), piece(h, tr[h].at[d], 0, n),
                    G_EX + h, ex2_r.at[h, d, n], ex_dev[h](1 - 2 * d, c),
                )

    def gather_rest(o, _):
        delta = jnp.where(o == 0, 1, jnp.where(o == 1, 3, 0))
        gather(0, delta)
        gather(1, delta)
        return 0

    lax.fori_loop(0, 3, gather_rest, 0)

    def ex1_send(far, pieces):
        cc = other if far else c
        for n in pieces:
            for h in range(2):
                for d in range(2):
                    slot = 3 - d + 4 * far
                    send(
                        piece(h, snd[h].at[1 + 2 * d], cc * ROWS, n), landing(h, slot, n),
                        G_EX + h, landed(h, 1 + 2 * far, n), ex_dev[h](1 - 2 * d, cc),
                    )

    ex1_send(0, range(N))
    for h in range(2):
        for n in range(N + 1):
            send(piece(h, snd[h].at[0], other * ROWS, n), landing(h, 1, n), G_OWN + h, landed(h, 0, n), at(cc=other))
        ex[h][0] = snd[h][0, pl.ds(pl.multiple_of(c * ROWS, 16), MAIN), :]
        exl[h][0] = snd[h][0, pl.ds(pl.multiple_of(c * ROWS + MAIN, 16), LAST), :]

    for h in range(2):
        got(metar.at[h, 0:3], rr.at[2 + h])
        metar[h, po[h]] = meta[...]
        for i in range(4):
            code = metar[h, i, 4 * h : 4 * h + 4, 0:T].astype(I32) - po[h] * 1024
            slot = code // 32
            place = code - slot * 32 + m4(i - po[h] - 1) * PER
            valid = (code >= 0) & (code < 256)
            rowsel[h, :, i * T : (i + 1) * T] = jnp.where(valid & (place < MAIN), slot * MAIN + place, -1).astype(F32)
            rowlast[h, i] = jnp.where(valid & (place >= MAIN), slot * LAST + place - MAIN, -1).astype(F32)
        got(og[h].at[0 : 2 * T, :], og_r.at[h, 2])
    acc[...] = jnp.zeros_like(acc)

    def absorb(pair, mine):
        for n in range(N):
            for h in range(2):
                if mine:
                    got(landing(h, 1, n), landed(h, 0, n))
                else:
                    got(ex[h].at[pl.ds(2 * pair, 2), :, pl.ds(*PIECES[h][n])], landed(h, pair, n))
                lo, w = PIECES[h][n]
                block = ex[h][pl.ds(2 * pair, 2), :, lo : lo + w].reshape(2 * MAIN, w)
                part = dot(block, og[h][:, lo : lo + w], ((1,), (1,)))
                if n == 0:
                    gbuf[h] = part
                else:
                    gbuf[h] += part
        rid = (iota((2 * MAIN, 128), 0) + pair * 2 * MAIN).astype(F32)
        for h in range(2):
            for lb in range(6):
                lanes = slice(lb * 128, lb * 128 + 128)
                g = gbuf[h, :, lanes]
                for k in range(K):
                    hit = jnp.where(rid == rowsel[h, k : k + 1, lanes], g, 0.0)
                    acc[h, k, :, lanes] += jnp.sum(hit.reshape(2 * MAIN // 8, 8, 128), axis=0)

    absorb(0, True)

    def forward(n):
        for h in range(2):
            for d in range(2):
                got(piece(h, tr[h].at[d], 0, n), ex2_r.at[h, d, n])
                send(
                    piece(h, tr[h].at[d], 0, n), landing(h, 4 + c, n),
                    G_EX + h, landed(h, 2, n), ex_dev[h](1 - 2 * d, d),
                )

    for n in range(N):
        forward(n)
    ex1_send(1, range(N))
    forward(N)
    for far in range(2):
        ex1_send(far, (N,))

    got(psr1.at[0:7], rr.at[5])
    psb2[...] = jnp.sum(psr1[...], axis=0)
    psr2[y] = psb2[...]
    for s in (1, 2, 3):
        send(psb2, psr2.at[y], G_P2, rr.at[6], at(dy=s))

    got(xcr.at[0:3], rr.at[7])
    cnt_row = jnp.sum(xcr[...], axis=0)[0:1, :]
    cnt_col = jnp.sum(jnp.where(diag, cnt_row, 0.0), axis=1, keepdims=True)
    push = bs_s[0] * E * (cnt_col / (TOTAL * K))
    prob = pt[...]
    spread = prob * (push - jnp.sum(prob * push, axis=0, keepdims=True))
    lt[...] = spread
    spb[...] = jnp.zeros_like(spb)
    for par in range(2):
        for n in range(16):
            spb[par, 4 * n : 4 * n + 4, 0:T] = spread[8 * n + 4 * par : 8 * n + 4 * par + 4, :]
        for k in range(K):
            ik = idxv[k : k + 1, :]
            spb[par, 64 + k : 65 + k, 0:T] = jnp.where((ik // 4) % 2 == par, ik // 8 * 4 + ik % 4, -1).astype(F32)
    for n, (a, k) in enumerate(xpeers):
        send(spb.at[lax.rem(c + k, 2)], spr.at[xc], G_SP, rr.at[9], xdev(a, k))
    spr[xc] = spb[c]

    def arrivals(pair, _):
        absorb(pair, False)
        return 0

    lax.fori_loop(1, 4, arrivals, 0)

    for h in range(2):
        for i in range(4):
            pds[h, i] = jnp.zeros((K, 256), F32)
            for k in range(K):
                pds[h, i, k : k + 1, 0:T] = jnp.sum(acc[h, k, :, i * T : (i + 1) * T], axis=0, keepdims=True)
        for s in (1, 2, 3):
            send(pds.at[h, m4(po[h] + s)], pdr.at[h, po[h]], G_PD + h, rr.at[10 + h], og_dev[h](s))
        pdr[h, po[h]] = pds[h, po[h]]
    got(psr2.at[0:3], rr.at[6])
    xps[...] = jnp.sum(psr2[...], axis=0)
    xpr[x] = xps[...]
    for a in (1, 2, 3):
        send(xps, xpr.at[x], G_XP, rr.at[8], at(dx=a))
    late = [jnp.zeros((1, T), F32)] * K
    rid = iota((8 * LAST, T), 0).astype(F32)
    for h in range(2):
        got(exl[h].at[1:8], last_r.at[h])
    both = [dot(exl[h][...].reshape(8 * LAST, WIDTH[h]), og[h][own_og[h], :], ((1,), (1,))) for h in range(2)]
    for h in range(2):
        g = both[h]
        for k in range(K):
            hit = jnp.where(rid == rowlast[h, po[h], k : k + 1, :], g, 0.0)
            late[k] += jnp.sum(hit, axis=0, keepdims=True)

    pd = jnp.zeros((K, 256), F32)
    for h in range(2):
        got(pdr.at[h, 0:3], rr.at[10 + h])
        pd += (pdr[h, 0] + pdr[h, 1]) + (pdr[h, 2] + pdr[h, 3])

    dots = [pd[k : k + 1, 0:T] + late[k] for k in range(K)]
    mix = [mixv[k : k + 1, :] for k in range(K)]
    mean = mix[0] * dots[0] + mix[1] * dots[1] + mix[2] * dots[2] + mix[3] * dots[3]
    for k in range(K):
        selb[k : k + 1, 0:T] = mix[k] * (dots[k] - mean)
    selb[:, T:256] = jnp.zeros((K, 256 - T), F32)
    for n, (a, k) in enumerate(xpeers):
        send(selb, selr.at[xc], G_LG, lg_r.at[xc], xdev(a, k))

    lg = jnp.zeros((E, T), F32)
    for k in range(K):
        lg += jnp.where(idxv[k : k + 1, :] == ie, selb[k : k + 1, 0:T], 0.0)
    lgv[...] = jnp.transpose(lt[...] + lg).astype(BF16)
    got(tokr.at[0:7], rr.at[4])
    got(spr.at[0:7], rr.at[9])

    ir = iota((64, T), 0).astype(F32)

    def weight_term(src, sel):
        named = jnp.zeros((64, T), F32)
        for k in range(K):
            named += jnp.where(spr[src, 64 + k : 65 + k, 0:T] == ir, sel[k : k + 1, 0:T], 0.0)
        return dot((spr[src, 0:64, 0:T] + named).astype(BF16), tokr[src])

    wsum = weight_term(xc, selb)
    for a, k in reversed(xpeers):
        src = m4(x + a) * 2 + lax.rem(c + k, 2)
        got(selr.at[src], lg_r.at[src])
        wsum += weight_term(src, selr.at[src])
    shift = x * 720 - (x * 720) // 128 * 128
    wsum = pltpu.roll(wsum, lax.rem(BLK - shift, BLK), 1)
    for n in range(16):
        rss[n] = wsum[4 * n : 4 * n + 4, 0:OUT]

    chip = y * 4 + z
    hops = lambda v: min(v[0], 4 - v[0]) + min(v[1], 4 - v[1])
    for n, (a, b) in enumerate(sorted([(a, b) for a in range(4) for b in range(4) if a or b], key=hops, reverse=True)):
        dest = m4(y + a) * 4 + m4(z + b)
        send(rss.at[dest], rsr.at[chip], G_RS, rr.at[12], at(dy=a, dz=b))
    rsr[chip] = rss[chip]
    tg_o[...] = dot(lgv[...], wv[...], ((1,), (1,))).astype(BF16)

    got(xpr.at[0:3], rr.at[8])
    ps_row = jnp.sum(xpr[...], axis=0)[0:1, :]
    loss = E * jnp.sum((cnt_row / (TOTAL * K)) * (ps_row / TOTAL), axis=1, keepdims=True)
    small_o[4:8, :] = jnp.broadcast_to(loss, (4, OUT))

    for h in range(2):
        drain(snd[h], G_EX + h)
        drain(snd[h].at[0, 0:ROWS, :], G_OWN + h)
        drain(og[h].at[0 : 3 * T, :], G_OG + h)
        drain(metar.at[h, 0:3], G_ME + h)
        drain(pdr.at[h, 0:3], G_PD + h)
    for ref, group in (
        (cntr.at[0, 0:7], G_C1), (cntr.at[0:3], G_C2), (psr1.at[0:7], G_P1), (psr2.at[0:3], G_P2), (xcr.at[0:3], G_XC), (xpr.at[0:3], G_XP),
        (tokr.at[0:7], G_TK), (spr.at[0:7], G_SP), (selr.at[0:7], G_LG), (rsr.at[0:15], G_RS),
    ):
        drain(ref, group)
    got(rsr.at[0:15], rr.at[12])
    out = jnp.sum(rsr[...], axis=0) * (1.0 / math.sqrt(TOTAL))
    small_o[0:4, :] = out[:, 0:OUT]


def finish(tg_ref, small_ref, tg_o, wt_o, loss_o, wtv, lossv, sem):
    tg_out = pltpu.make_async_copy(tg_ref, tg_o, sem.at[0])
    tg_out.start()
    wtv[...] = small_ref[0:4, 0:720]
    wt_out = pltpu.make_async_copy(wtv, wt_o, sem.at[1])
    wt_out.start()
    lossv[0] = jnp.sum(small_ref[4:5, 0:1])
    loss_out = pltpu.make_async_copy(lossv, loss_o, sem.at[2])
    loss_out.start()
    loss_out.wait()
    tg_out.wait()
    wt_out.wait()


def on_device(tokens, out_grad, indices, expert_rows, router_weight, router_bias, balance_scale):
    rows = jnp.transpose(expert_rows[0], (0, 2, 1, 3)).reshape(ES, 32, D)
    dma = pltpu.SemaphoreType.DMA
    vm = pltpu.VMEM
    scratch = [
        vm((T, D), BF16), vm((T, DPAD), BF16), vm((T, D), BF16), vm((4 * T, WIDTH[0]), BF16), vm((4 * T, WIDTH[1]), BF16),
        vm((K, T), I32), vm((4, ES, 8, D), BF16), vm((4 * KQ, DPAD), BF16), vm((D, E), BF16), vm((1, E), F32),
        vm((4, 2 * ROWS, WIDTH[0]), BF16), vm((4, 2 * ROWS, WIDTH[1]), BF16),
        vm((2, ROWS, WIDTH[0]), BF16), vm((2, ROWS, WIDTH[1]), BF16),
        vm((8, MAIN, WIDTH[0]), BF16), vm((8, MAIN, WIDTH[1]), BF16), vm((8, LAST, WIDTH[0]), BF16), vm((8, LAST, WIDTH[1]), BF16),
        vm((8, T, BLK), BF16),
        vm((8, E), F32), vm((4, 8, 8, E), F32), vm((K, 256, E), BF16), vm((8, 256), F32), vm((2, 4, 8, 256), F32),
        vm((2, K, 4 * T), F32), vm((2, 4, K, T), F32), vm((2, K, 8, 4 * T), F32), vm((2, 2 * MAIN, 4 * T), F32), vm((2, 4, K, 256), F32), vm((2, 4, K, 256), F32),
        vm((8, E), F32), vm((8, 8, E), F32), vm((4, 8, E), F32), vm((8, E), F32),
        vm((8, E), F32), vm((4, 8, E), F32), vm((8, E), F32), vm((4, 8, E), F32),
        vm((E, T), F32), vm((E, T), F32), vm((K, T), F32), vm((2, 72, 256), F32), vm((8, 72, 256), F32),
        vm((K, 256), F32), vm((8, K, 256), F32), vm((16, 4, OUT), F32), vm((16, 4, OUT), F32), vm((T, E), BF16),
        dma((9,)), dma((20,)), dma((13,)), dma((2, 3)), dma((2, 2, N + 1)), dma((2, 4, N)), dma((2,)), dma((8,)),
    ]
    hbm = pl.BlockSpec(memory_space=pltpu.HBM)
    in_vmem = pl.BlockSpec(memory_space=vm)
    token_grad, small = pl.pallas_call(
        kernel,
        out_shape=(vm((T, D), BF16), vm((8, OUT), F32)),
        in_specs=[hbm] * 6 + [pl.BlockSpec(memory_space=pltpu.SMEM)],
        out_specs=(in_vmem, in_vmem),
        scratch_shapes=scratch,
        compiler_params=pltpu.CompilerParams(collective_id=0, has_side_effects=True, vmem_limit_bytes=54000 * 1024),
        name="router",
    )(
        *(
            pltpu.with_memory_space_constraint(a, pltpu.HBM)
            for a in (tokens, out_grad, indices.T, rows, router_weight, router_bias.reshape(1, E))
        ),
        balance_scale,
    )
    token_grad, weight_grad, loss = pl.pallas_call(
        finish,
        out_shape=(
            jax.ShapeDtypeStruct((T, D), BF16),
            jax.ShapeDtypeStruct((4, 720), F32),
            jax.ShapeDtypeStruct((1,), F32),
        ),
        in_specs=[in_vmem] * 2,
        out_specs=(hbm, hbm, hbm),
        scratch_shapes=[vm((4, 720), F32), pltpu.SMEM((1,), F32), dma((3,))],
        name="finish",
    )(*(pltpu.with_memory_space_constraint(a, vm) for a in (token_grad, small)))
    return token_grad, weight_grad.T, loss


def solution(mesh):
    torus = Mesh(mesh.devices.reshape(4, 4, 2, mesh.shape["dp"]), AXES)
    return jax.shard_map(
        on_device,
        mesh=torus,
        in_specs=(P(AXES, None), P(AXES, None), P(AXES, None), P("dp", EP, None, None, None), P(), P(), P()),
        out_specs=(P(AXES, None), P("dp", EP), P()),
        check_vma=False,
    )
```

```python
import math

import jax
import jax.numpy as jnp
from jax import lax
from jax.experimental import pallas as pl
from jax.experimental.pallas import tpu as pltpu
from jax.sharding import Mesh
from jax.sharding import PartitionSpec as P

AXES = ("ep_0", "ep_1", "ep_2", "dp")
EP = AXES[:3]
MESH = pl.DeviceIdType.MESH
F32, BF16, I32 = jnp.float32, jnp.bfloat16, jnp.int32

D, E, T, K, CAP = 2880, 128, 192, 4, 9
DPAD = 2944
SPLIT = 1408
FIRST, WIDTH = (SPLIT, 0), (DPAD - SPLIT, SPLIT)
PER = 27
ROWS = 112
MAIN, LAST = 96, 16
ES = 4 * CAP
KQ = ES * 8
PIECES = ((0, 640), (640, 512), (1152, 256))
N = 3
HALF = MAIN // 2
BLK = 896
OUT = 768
TOTAL = 24576
G_EX, G_OWN, G_OG, G_ME, G_PD = 0, 2, 4, 6, 8
G_C1, G_C2, G_P1, G_P2, G_XC, G_XP, G_TK, G_SP, G_LG, G_RS = range(10, 20)
G_TL, G_TO, G_LS, G_OL = 20, 21, 22, 24


def dot(a, b, dims=((1,), (0,)), **kw):
    return lax.dot_general(a, b, (dims, ((), ())), preferred_element_type=F32, **kw)


def iota(shape, dim):
    return lax.broadcasted_iota(I32, shape, dim)


def kernel(
    tok_h, og_h, idx_h, ex_h, w_h, b_h, bs_s,
    tg_o, small_o,
    tokraw, tokp, ogfull, og0, og1, idxv, ev3, ev, wv, bv,
    snd0, snd1, tr0, tr1, ex0, ex1, exl0, exl1, tls, trt, ext, ogr, tokr,
    cntsnd, cntr, cc_v, meta, metar, rowsel, rowlast, acc, gbuf, pds, pdr,
    psb, psr1, psr2, psb2, xcs, xcr, xps, xpr,
    lt, pt, mixv, spb, spr, selb, selr, rss, rsr, lgv,
    loc, ss, rr, og_r, ex2_r, exr, last_r, tr_r, tail_r, lg_r,
):
    y, z, c, x = (lax.axis_index(a) for a in AXES)
    og, snd, tr, ex, exl = (og0, og1), (snd0, snd1), (tr0, tr1), (ex0, ex1), (exl0, exl1)
    m4 = lambda v: lax.rem(v + 4, 4)
    po = (z, y)
    pe = (y, z)
    other = 1 - c

    def at(dy=0, dz=0, cc=None, dx=0):
        return (m4(y + dy), m4(z + dz), c if cc is None else cc, m4(x + dx))

    og_dev = (lambda s: at(dz=s), lambda s: at(dy=s))
    ex_dev = (lambda s, cc: at(dy=s, cc=cc), lambda s, cc: at(dz=s, cc=cc))

    def remote(src, dst, ss, rs, dev):
        return pltpu.make_async_remote_copy(src_ref=src, dst_ref=dst, send_sem=ss, recv_sem=rs, device_id=dev, device_id_type=MESH)

    def send(src, dst, group, recv, dev):
        remote(src, dst, ss.at[group], recv, dev).start()

    def got(ref, sem):
        remote(ref, ref, sem, sem, at(dx=1)).wait_recv()

    def drain(ref, group):
        remote(ref, ref, ss.at[group], ss.at[group], at(dx=1)).wait_send()

    loads = [
        pltpu.make_async_copy(idx_h, idxv, loc.at[0]),
        pltpu.make_async_copy(og_h, ogfull, loc.at[1]),
        pltpu.make_async_copy(tok_h, tokraw, loc.at[2]),
        pltpu.make_async_copy(w_h, wv, loc.at[3]),
        pltpu.make_async_copy(b_h, bv, loc.at[4]),
    ] + [pltpu.make_async_copy(ex_h.at[:, q * 8 : q * 8 + 8, :], ev3.at[q], loc.at[5 + q]) for q in range(4)]
    for l in loads:
        l.start()
    peers = [at(dy=a, dz=b) for a in range(4) for b in range(4) if a or b]
    peers += [at(dy=a, cc=other) for a in (1, 2, 3)] + [at(dz=a, cc=other) for a in (1, 2, 3)]
    peers += [at(cc=other)] + [at(dx=a, cc=k) for a in (1, 2, 3) for k in (c, other)]
    barrier = pltpu.get_barrier_semaphore()
    for p in peers:
        pl.semaphore_signal(barrier, inc=1, device_id=p, device_id_type=MESH)

    loads[0].wait()
    idx = idxv[...]
    ie = iota((E, T), 0)
    named = jnp.zeros((E, T), F32)
    for k in range(K):
        named += jnp.where(idx[k : k + 1, :] == ie, 1.0, 0.0)
    nb = named.astype(BF16)
    upper = jnp.where(iota((T, T), 0) < iota((T, T), 1), 1.0, 0.0).astype(BF16)
    ones_tt = jnp.ones((T, T), BF16)
    r_e, c_e = iota((E, E), 0), iota((E, E), 1)
    same_ep = jnp.where((r_e // 4 == c_e // 4) & (c_e < r_e), 1.0, 0.0).astype(BF16)
    ahead = dot(same_ep, nb).astype(BF16)
    rowpos = dot(nb, upper) + dot(ahead, ones_tt)
    cntsnd[...] = dot(jnp.ones((8, T), BF16), nb, ((1,), (1,)))
    meta[...] = jnp.full((8, 256), -1e6, F32)
    for k in range(K):
        ik = idx[k : k + 1, :]
        off = jnp.sum(jnp.where(ik == ie, rowpos, 0.0), axis=0, keepdims=True)
        ey, ez, ec = ik // 32, (ik // 8) % 4, (ik // 4) % 2
        for h, (ea, eb) in enumerate(((ey, ez), (ez, ey))):
            step, same = (ea - pe[h] + 4) % 4, ec == c
            near = jnp.where(step == 1, jnp.where(same, 2, 6), jnp.where(same, 3, 7))
            slot = jnp.where(step == 0, jnp.where(same, 0, 1), jnp.where(step == 2, 4 + ec, near))
            code = (eb * 1024 + slot * 32).astype(F32) + off
            meta[4 * h + k : 4 * h + k + 1, 0:T] = code

    loads[1].wait()
    own_og = [pl.ds(pl.multiple_of(po[h] * T, T), T) for h in range(2)]
    og0[own_og[0], WIDTH[0] - 128 : WIDTH[0]] = jnp.zeros((T, 128), BF16)
    og0[own_og[0], 0 : D - SPLIT] = ogfull[:, SPLIT:D]
    og1[own_og[1], :] = ogfull[:, 0:SPLIT]
    pl.semaphore_wait(barrier, len(peers))

    zc = z * 2 + c
    cntr[y, zc] = cntsnd[...]
    zpeers = [(b, k) for b in (1, 2, 3) for k in (0, 1)] + [(0, 1)]
    zdev = lambda b, k: at(dz=b, cc=lax.rem(c + k, 2))
    for n, (b, k) in enumerate(zpeers):
        send(cntsnd, cntr.at[y, zc], G_C1, rr.at[0], zdev(b, k))
    for h in range(2):
        for s in (1, 2, 3):
            send(meta, metar.at[h, po[h]], G_ME + h, rr.at[2 + h], og_dev[h](s))

    def og_rows(pos, second):
        return pl.ds(pl.multiple_of(pos * T + second * 96, 32), 96)

    def og_send(h, d, m):
        where = og_rows(po[h], d ^ m)
        send(og[h].at[where, :], og[h].at[where, :], G_OG + h, og_r.at[h, 2 if m else d], og_dev[h](1 - 2 * d))

    for h in range(2):
        for d in range(2):
            og_send(h, d, 0)

    got(cntr.at[0, 0:7], rr.at[0])
    for s in (1, 2, 3):
        send(cntr.at[y], cntr.at[y], G_C2, rr.at[1], at(dy=s))
    for h in range(2):
        for d in range(2):
            og_send(h, d, 1)

    loads[2].wait()
    tokp[:, DPAD - 128 : DPAD] = jnp.zeros((T, 128), BF16)
    tokp[:, 0:D] = tokraw[...]

    def block(pos):
        return pl.ds(pl.multiple_of((pos * 720) // 128 * 128, 128), BLK)

    xc = x * 2 + c
    xpeers = [(a, k) for a in (1, 2, 3) for k in (0, 1)] + [(0, 1)]
    xdev = lambda a, k: at(dx=a, cc=lax.rem(c + k, 2))
    tokr[xc] = tokp[:, block(x)]
    for n, (a, k) in enumerate(xpeers):
        send(tokp.at[:, block(m4(x + a))], tokr.at[xc], G_TK, rr.at[4], xdev(a, k))

    loads[3].wait()
    loads[4].wait()
    logits = jnp.transpose(dot(tokp[:, 0:D], wv[...]) + bv[...])
    lt[...] = logits
    ex_l = jnp.exp(logits - jnp.max(logits, axis=0, keepdims=True))
    prob = ex_l / jnp.sum(ex_l, axis=0, keepdims=True)
    pt[...] = prob
    picked = [jnp.sum(jnp.where(idx[k : k + 1, :] == ie, logits, 0.0), axis=0, keepdims=True) for k in range(K)]
    top = jnp.maximum(jnp.maximum(picked[0], picked[1]), jnp.maximum(picked[2], picked[3]))
    picked = [jnp.exp(p - top) for p in picked]
    total = picked[0] + picked[1] + picked[2] + picked[3]
    for k in range(K):
        mixv[k : k + 1, :] = picked[k] / total
    diag = r_e == c_e
    pcol = jnp.sum(prob, axis=1, keepdims=True)
    prow = jnp.sum(jnp.where(diag, pcol, 0.0), axis=0, keepdims=True)
    psb[...] = jnp.broadcast_to(prow, (8, E))
    for n, (b, k) in enumerate(zpeers):
        send(psb, psr1.at[zc], G_P1, rr.at[5], zdev(b, k))
    psr1[zc] = psb[...]

    for q in range(4):
        loads[5 + q].wait()
    ev[:, DPAD - 128 : DPAD] = jnp.zeros((4 * KQ, 128), BF16)

    def flatten(n, _):
        q, p = n // (ES // 2), lax.rem(n, ES // 2)
        pair = jnp.concatenate([ev3[q, 2 * p], ev3[q, 2 * p + 1]], axis=0)
        ev[pl.ds(pl.multiple_of(n * 16, 16), 16), 0:D] = pair
        return 0

    lax.fori_loop(0, 4 * ES // 2, flatten, 0)

    def og_from(d, h):
        return m4(po[h] - (1 - 2 * d))

    for h in range(2):
        for d in range(2):
            where = og_rows(og_from(d, h), d)
            got(og[h].at[where, :], og_r.at[h, d])
            send(og[h].at[where, :], og[h].at[where, :], G_OG + h, og_r.at[h, 2], og_dev[h](1 - 2 * d))

    got(cntr.at[0:3], rr.at[1])
    counts = cntr[...]
    plane = jnp.sum(counts.reshape(32, 8, E), axis=0)
    xcs[...] = plane
    xcr[x] = plane
    for a in (1, 2, 3):
        send(xcs, xcr.at[x], G_XC, rr.at[7], at(dx=a))
    first = (y * 8 + z * 2 + c) * 4
    cb = counts.reshape(256, E).astype(BF16)
    for k in range(K):
        mine = jnp.where((r_e >= first) & (r_e <= first + k), 1.0, 0.0).astype(BF16)
        cc_v[k] = dot(cb, mine).astype(BF16)

    def gather(h, delta):
        q = m4(pe[h] + delta)
        row = iota((2 * ROWS, E), 0)
        core = jnp.where(row >= ROWS, 1, 0)
        rr = row - core * ROWS
        i = jnp.where(rr >= PER, 1, 0) + jnp.where(rr >= 2 * PER, 1, 0) + jnp.where(rr >= 3 * PER, 1, 0)
        r = rr - i * PER
        i = i + po[h] + 1
        i = jnp.where(i >= 4, i - 4, i)
        dev = (q * 8 + i * 2 + core) if h == 0 else (i * 8 + q * 2 + core)
        pick = (jnp.broadcast_to(dev[:, 0:1] * 8, (2 * ROWS, 256)) == iota((2 * ROWS, 256), 1))
        pick = jnp.where(pick, 1.0, 0.0).astype(BF16)
        t = [dot(pick, cc_v[k]).astype(I32) for k in range(K)]
        e_in = jnp.where(r >= t[0], 1, 0) + jnp.where(r >= t[1], 1, 0) + jnp.where(r >= t[2], 1, 0)
        base = jnp.where(r >= t[2], t[2], jnp.where(r >= t[1], t[1], jnp.where(r >= t[0], t[0], 0)))
        es = e_in * CAP + r - base
        target = (es * 8 + i * 2 + core) if h == 0 else (i * KQ + es * 8 + q * 2 + core)
        target = jnp.where((r < t[3]) & (rr < 4 * PER), target, -1)
        depth = KQ if h == 0 else 4 * KQ
        sel = jnp.broadcast_to(target[:, 0:1], (2 * ROWS, depth)) == iota((2 * ROWS, depth), 1)
        sel = jnp.where(sel, 1.0, 0.0).astype(BF16)
        rows = pl.ds(pl.multiple_of(q * KQ, KQ), KQ) if h == 0 else pl.ds(0, 4 * KQ)
        for lo, w in PIECES:
            snd[h][delta, :, lo : lo + w] = dot(sel, ev[rows, FIRST[h] + lo : FIRST[h] + lo + w]).astype(BF16)
        if h == 0:
            tail = dot(sel, ev[rows, DPAD - 128 : DPAD])
            snd[h][delta, :, SPLIT : SPLIT + 128] = tail.astype(BF16)
            for k in range(2):
                upper, lower = (tail[k * ROWS + j * HALF : k * ROWS + j * HALF + HALF] for j in range(2))
                tls[delta, k] = (upper + pltpu.roll(lower, 64, 1)).astype(BF16)

    def core_rows(cc):
        return pl.ds(pl.multiple_of(cc * ROWS, 16), ROWS)

    def piece(h, ref, row, n):
        if n == N:
            return ref.at[pl.ds(pl.multiple_of(row + MAIN, 16), LAST), :]
        return ref.at[pl.ds(pl.multiple_of(row, 16), MAIN), pl.ds(*PIECES[n])]

    def landing(h, slot, n):
        return exl[h].at[slot] if n == N else ex[h].at[slot, :, pl.ds(*PIECES[n])]

    def landed(h, pair, n):
        return last_r.at[h] if n == N else exr.at[h, pair, n]

    def leaving(h, n):
        return (G_LS if n == N else G_EX) + h

    for h in range(2):
        gather(h, 2)
        for d in range(2):
            if h == 0:
                send(tls.at[2, d], trt.at[d], G_TL, tr_r.at[d], ex_dev[0](1 - 2 * d, c))
            for n in range(N + 1):
                send(
                    piece(h, snd[h].at[2], d * ROWS, n), piece(h, tr[h].at[d], 0, n),
                    leaving(h, n), ex2_r.at[h, d, n], ex_dev[h](1 - 2 * d, c),
                )

    def gather_rest(o, _):
        delta = jnp.where(o == 0, 1, jnp.where(o == 1, 3, 0))
        gather(0, delta)
        gather(1, delta)
        return 0

    lax.fori_loop(0, 3, gather_rest, 0)

    def ex1_send(far, pieces):
        cc = other if far else c
        for n in pieces:
            for h in range(2):
                for d in range(2):
                    slot = 3 - d + 4 * far
                    send(
                        piece(h, snd[h].at[1 + 2 * d], cc * ROWS, n), landing(h, slot, n),
                        leaving(h, n), landed(h, 1 + 2 * far, n), ex_dev[h](1 - 2 * d, cc),
                    )
                    if h == 0 and n == 0:
                        send(tls.at[1 + 2 * d, cc], ext.at[slot], G_TL, tail_r.at[1 + 2 * far], ex_dev[0](1 - 2 * d, cc))

    ex1_send(0, range(N))
    send(tls.at[0, other], ext.at[1], G_TO, tail_r.at[0], at(cc=other))
    ext[0] = tls[0, c]
    for h in range(2):
        for n in range(N + 1):
            send(piece(h, snd[h].at[0], other * ROWS, n), landing(h, 1, n), (G_OL if n == N else G_OWN) + h, landed(h, 0, n), at(cc=other))
        ex[h][0] = snd[h][0, pl.ds(pl.multiple_of(c * ROWS, 16), MAIN), 0:SPLIT]
        exl[h][0] = snd[h][0, pl.ds(pl.multiple_of(c * ROWS + MAIN, 16), LAST), :]

    for h in range(2):
        got(metar.at[h, 0:3], rr.at[2 + h])
        metar[h, po[h]] = meta[...]
        for i in range(4):
            code = metar[h, i, 4 * h : 4 * h + 4, 0:T].astype(I32) - po[h] * 1024
            slot = code // 32
            place = code - slot * 32 + m4(i - po[h] - 1) * PER
            valid = (code >= 0) & (code < 256)
            rowsel[h, :, i * T : (i + 1) * T] = jnp.where(valid & (place < MAIN), slot * MAIN + place, -1).astype(F32)
            rowlast[h, i] = jnp.where(valid & (place >= MAIN), slot * LAST + place - MAIN, -1).astype(F32)
        got(og[h].at[0 : 2 * T, :], og_r.at[h, 2])
    ogr[...] = pltpu.roll(og0[:, SPLIT : SPLIT + 128].astype(F32), 64, 1).astype(BF16)
    acc[...] = jnp.zeros_like(acc)

    def absorb(pair, mine):
        for n in range(N):
            for h in range(2):
                if mine:
                    got(landing(h, 1, n), landed(h, 0, n))
                else:
                    got(ex[h].at[pl.ds(2 * pair, 2), :, pl.ds(*PIECES[n])], landed(h, pair, n))
                lo, w = PIECES[n]
                block = ex[h][pl.ds(2 * pair, 2), :, lo : lo + w].reshape(2 * MAIN, w)
                part = dot(block, og[h][:, lo : lo + w], ((1,), (1,)))
                if n == 0:
                    gbuf[h] = part
                else:
                    gbuf[h] += part
        if mine:
            got(ext.at[1], tail_r.at[0])
        else:
            got(ext.at[pl.ds(2 * pair, 2)], tail_r.at[pair])
        tail = ext[pl.ds(2 * pair, 2)].reshape(MAIN, 128)
        for j, other_side in enumerate((og0[:, SPLIT : SPLIT + 128], ogr[...])):
            part = dot(tail, other_side, ((1,), (1,)))
            for slot in range(2):
                where = slice(slot * MAIN + j * HALF, slot * MAIN + j * HALF + HALF)
                gbuf[0, where, :] += part[slot * HALF : slot * HALF + HALF]
        rid = (iota((2 * MAIN, 128), 0) + pair * 2 * MAIN).astype(F32)
        for h in range(2):
            for lb in range(6):
                lanes = slice(lb * 128, lb * 128 + 128)
                g = gbuf[h, :, lanes]
                for k in range(K):
                    hit = jnp.where(rid == rowsel[h, k : k + 1, lanes], g, 0.0)
                    acc[h, k, :, lanes] += jnp.sum(hit.reshape(2 * MAIN // 8, 8, 128), axis=0)

    absorb(0, True)

    def forward(n):
        for h in range(2):
            for d in range(2):
                got(piece(h, tr[h].at[d], 0, n), ex2_r.at[h, d, n])
                send(
                    piece(h, tr[h].at[d], 0, n), landing(h, 4 + c, n),
                    leaving(h, n), landed(h, 2, n), ex_dev[h](1 - 2 * d, d),
                )

    for d in range(2):
        got(trt.at[d], tr_r.at[d])
        send(trt.at[d], ext.at[4 + c], G_TL, tail_r.at[2], ex_dev[0](1 - 2 * d, d))
    for n in range(N):
        forward(n)
    ex1_send(1, range(N))
    forward(N)
    for far in range(2):
        ex1_send(far, (N,))

    got(psr1.at[0:7], rr.at[5])
    psb2[...] = jnp.sum(psr1[...], axis=0)
    psr2[y] = psb2[...]
    for s in (1, 2, 3):
        send(psb2, psr2.at[y], G_P2, rr.at[6], at(dy=s))

    got(xcr.at[0:3], rr.at[7])
    cnt_row = jnp.sum(xcr[...], axis=0)[0:1, :]
    cnt_col = jnp.sum(jnp.where(diag, cnt_row, 0.0), axis=1, keepdims=True)
    push = bs_s[0] * E * (cnt_col / (TOTAL * K))
    prob = pt[...]
    spread = prob * (push - jnp.sum(prob * push, axis=0, keepdims=True))
    lt[...] = spread
    spb[...] = jnp.zeros_like(spb)
    for par in range(2):
        for n in range(16):
            spb[par, 4 * n : 4 * n + 4, 0:T] = spread[8 * n + 4 * par : 8 * n + 4 * par + 4, :]
        for k in range(K):
            ik = idxv[k : k + 1, :]
            spb[par, 64 + k : 65 + k, 0:T] = jnp.where((ik // 4) % 2 == par, ik // 8 * 4 + ik % 4, -1).astype(F32)
    for n, (a, k) in enumerate(xpeers):
        send(spb.at[lax.rem(c + k, 2)], spr.at[xc], G_SP, rr.at[9], xdev(a, k))
    spr[xc] = spb[c]

    def arrivals(pair, _):
        absorb(pair, False)
        return 0

    lax.fori_loop(1, 4, arrivals, 0)

    for h in range(2):
        for i in range(4):
            pds[h, i] = jnp.zeros((K, 256), F32)
            for k in range(K):
                pds[h, i, k : k + 1, 0:T] = jnp.sum(acc[h, k, :, i * T : (i + 1) * T], axis=0, keepdims=True)
        for s in (1, 2, 3):
            send(pds.at[h, m4(po[h] + s)], pdr.at[h, po[h]], G_PD + h, rr.at[10 + h], og_dev[h](s))
        pdr[h, po[h]] = pds[h, po[h]]
    got(psr2.at[0:3], rr.at[6])
    xps[...] = jnp.sum(psr2[...], axis=0)
    xpr[x] = xps[...]
    for a in (1, 2, 3):
        send(xps, xpr.at[x], G_XP, rr.at[8], at(dx=a))
    late = [jnp.zeros((1, T), F32)] * K
    rid = iota((8 * LAST, T), 0).astype(F32)
    for h in range(2):
        got(exl[h].at[1:8], last_r.at[h])
    both = [dot(exl[h][...].reshape(8 * LAST, WIDTH[h]), og[h][own_og[h], :], ((1,), (1,))) for h in range(2)]
    for h in range(2):
        g = both[h]
        for k in range(K):
            hit = jnp.where(rid == rowlast[h, po[h], k : k + 1, :], g, 0.0)
            late[k] += jnp.sum(hit, axis=0, keepdims=True)

    pd = jnp.zeros((K, 256), F32)
    for h in range(2):
        got(pdr.at[h, 0:3], rr.at[10 + h])
        pd += (pdr[h, 0] + pdr[h, 1]) + (pdr[h, 2] + pdr[h, 3])

    dots = [pd[k : k + 1, 0:T] + late[k] for k in range(K)]
    mix = [mixv[k : k + 1, :] for k in range(K)]
    mean = mix[0] * dots[0] + mix[1] * dots[1] + mix[2] * dots[2] + mix[3] * dots[3]
    for k in range(K):
        selb[k : k + 1, 0:T] = mix[k] * (dots[k] - mean)
    selb[:, T:256] = jnp.zeros((K, 256 - T), F32)
    for n, (a, k) in enumerate(xpeers):
        send(selb, selr.at[xc], G_LG, lg_r.at[xc], xdev(a, k))

    lg = jnp.zeros((E, T), F32)
    for k in range(K):
        lg += jnp.where(idxv[k : k + 1, :] == ie, selb[k : k + 1, 0:T], 0.0)
    lgv[...] = jnp.transpose(lt[...] + lg).astype(BF16)
    got(tokr.at[0:7], rr.at[4])
    got(spr.at[0:7], rr.at[9])

    ir = iota((64, T), 0).astype(F32)

    def weight_term(src, sel):
        named = jnp.zeros((64, T), F32)
        for k in range(K):
            named += jnp.where(spr[src, 64 + k : 65 + k, 0:T] == ir, sel[k : k + 1, 0:T], 0.0)
        return dot((spr[src, 0:64, 0:T] + named).astype(BF16), tokr[src])

    wsum = weight_term(xc, selb)
    for a, k in reversed(xpeers):
        src = m4(x + a) * 2 + lax.rem(c + k, 2)
        got(selr.at[src], lg_r.at[src])
        wsum += weight_term(src, selr.at[src])
    shift = x * 720 - (x * 720) // 128 * 128
    wsum = pltpu.roll(wsum, lax.rem(BLK - shift, BLK), 1)
    for n in range(16):
        rss[n] = wsum[4 * n : 4 * n + 4, 0:OUT]

    chip = y * 4 + z
    hops = lambda v: min(v[0], 4 - v[0]) + min(v[1], 4 - v[1])
    for n, (a, b) in enumerate(sorted([(a, b) for a in range(4) for b in range(4) if a or b], key=hops, reverse=True)):
        dest = m4(y + a) * 4 + m4(z + b)
        send(rss.at[dest], rsr.at[chip], G_RS, rr.at[12], at(dy=a, dz=b))
    rsr[chip] = rss[chip]
    tg_o[...] = dot(lgv[...], wv[...], ((1,), (1,))).astype(BF16)

    got(xpr.at[0:3], rr.at[8])
    ps_row = jnp.sum(xpr[...], axis=0)[0:1, :]
    loss = E * jnp.sum((cnt_row / (TOTAL * K)) * (ps_row / TOTAL), axis=1, keepdims=True)
    small_o[4:8, :] = jnp.broadcast_to(loss, (4, OUT))

    for h in range(2):
        drain(ex[h], G_EX + h)
        drain(exl[h], G_LS + h)
        drain(ex[h].at[0], G_OWN + h)
        drain(exl[h].at[0], G_OL + h)
        drain(og[h].at[0 : 3 * T, :], G_OG + h)
        drain(metar.at[h, 0:3], G_ME + h)
        drain(pdr.at[h, 0:3], G_PD + h)
    for ref, group in (
        (cntr.at[0, 0:7], G_C1), (cntr.at[0:3], G_C2), (psr1.at[0:7], G_P1), (psr2.at[0:3], G_P2), (xcr.at[0:3], G_XC), (xpr.at[0:3], G_XP),
        (tokr.at[0:7], G_TK), (spr.at[0:7], G_SP), (tls, G_TL), (tls.at[0, 0], G_TO), (selr.at[0:7], G_LG), (rsr.at[0:15], G_RS),
    ):
        drain(ref, group)
    got(rsr.at[0:15], rr.at[12])
    out = jnp.sum(rsr[...], axis=0) * (1.0 / math.sqrt(TOTAL))
    small_o[0:4, :] = out[:, 0:OUT]


def finish(tg_ref, small_ref, tg_o, wt_o, loss_o, wtv, lossv, sem):
    tg_out = pltpu.make_async_copy(tg_ref, tg_o, sem.at[0])
    tg_out.start()
    wtv[...] = small_ref[0:4, 0:720]
    wt_out = pltpu.make_async_copy(wtv, wt_o, sem.at[1])
    wt_out.start()
    lossv[0] = jnp.sum(small_ref[4:5, 0:1])
    loss_out = pltpu.make_async_copy(lossv, loss_o, sem.at[2])
    loss_out.start()
    loss_out.wait()
    tg_out.wait()
    wt_out.wait()


def on_device(tokens, out_grad, indices, expert_rows, router_weight, router_bias, balance_scale):
    rows = jnp.transpose(expert_rows[0], (0, 2, 1, 3)).reshape(ES, 32, D)
    dma = pltpu.SemaphoreType.DMA
    vm = pltpu.VMEM
    scratch = [
        vm((T, D), BF16), vm((T, DPAD), BF16), vm((T, D), BF16), vm((4 * T, WIDTH[0]), BF16), vm((4 * T, WIDTH[1]), BF16),
        vm((K, T), I32), vm((4, ES, 8, D), BF16), vm((4 * KQ, DPAD), BF16), vm((D, E), BF16), vm((1, E), F32),
        vm((4, 2 * ROWS, WIDTH[0]), BF16), vm((4, 2 * ROWS, WIDTH[1]), BF16),
        vm((2, ROWS, WIDTH[0]), BF16), vm((2, ROWS, WIDTH[1]), BF16),
        vm((8, MAIN, SPLIT), BF16), vm((8, MAIN, SPLIT), BF16), vm((8, LAST, WIDTH[0]), BF16), vm((8, LAST, WIDTH[1]), BF16),
        vm((4, 2, HALF, 128), BF16), vm((2, HALF, 128), BF16), vm((8, HALF, 128), BF16), vm((4 * T, 128), BF16),
        vm((8, T, BLK), BF16),
        vm((8, E), F32), vm((4, 8, 8, E), F32), vm((K, 256, E), BF16), vm((8, 256), F32), vm((2, 4, 8, 256), F32),
        vm((2, K, 4 * T), F32), vm((2, 4, K, T), F32), vm((2, K, 8, 4 * T), F32), vm((2, 2 * MAIN, 4 * T), F32), vm((2, 4, K, 256), F32), vm((2, 4, K, 256), F32),
        vm((8, E), F32), vm((8, 8, E), F32), vm((4, 8, E), F32), vm((8, E), F32),
        vm((8, E), F32), vm((4, 8, E), F32), vm((8, E), F32), vm((4, 8, E), F32),
        vm((E, T), F32), vm((E, T), F32), vm((K, T), F32), vm((2, 72, 256), F32), vm((8, 72, 256), F32),
        vm((K, 256), F32), vm((8, K, 256), F32), vm((16, 4, OUT), F32), vm((16, 4, OUT), F32), vm((T, E), BF16),
        dma((9,)), dma((26,)), dma((13,)), dma((2, 3)), dma((2, 2, N + 1)), dma((2, 4, N)), dma((2,)), dma((2,)), dma((4,)), dma((8,)),
    ]
    hbm = pl.BlockSpec(memory_space=pltpu.HBM)
    in_vmem = pl.BlockSpec(memory_space=vm)
    token_grad, small = pl.pallas_call(
        kernel,
        out_shape=(vm((T, D), BF16), vm((8, OUT), F32)),
        in_specs=[hbm] * 6 + [pl.BlockSpec(memory_space=pltpu.SMEM)],
        out_specs=(in_vmem, in_vmem),
        scratch_shapes=scratch,
        compiler_params=pltpu.CompilerParams(collective_id=0, has_side_effects=True, vmem_limit_bytes=54000 * 1024),
        name="router",
    )(
        *(
            pltpu.with_memory_space_constraint(a, pltpu.HBM)
            for a in (tokens, out_grad, indices.T, rows, router_weight, router_bias.reshape(1, E))
        ),
        balance_scale,
    )
    token_grad, weight_grad, loss = pl.pallas_call(
        finish,
        out_shape=(
            jax.ShapeDtypeStruct((T, D), BF16),
            jax.ShapeDtypeStruct((4, 720), F32),
            jax.ShapeDtypeStruct((1,), F32),
        ),
        in_specs=[in_vmem] * 2,
        out_specs=(hbm, hbm, hbm),
        scratch_shapes=[vm((4, 720), F32), pltpu.SMEM((1,), F32), dma((3,))],
        name="finish",
    )(*(pltpu.with_memory_space_constraint(a, vm) for a in (token_grad, small)))
    return token_grad, weight_grad.T, loss


def solution(mesh):
    torus = Mesh(mesh.devices.reshape(4, 4, 2, mesh.shape["dp"]), AXES)
    return jax.shard_map(
        on_device,
        mesh=torus,
        in_specs=(P(AXES, None), P(AXES, None), P(AXES, None), P("dp", EP, None, None, None), P(), P(), P()),
        out_specs=(P(AXES, None), P("dp", EP), P()),
        check_vma=False,
    )
```

```python
import math

import jax
import jax.numpy as jnp
from jax import lax
from jax.experimental import pallas as pl
from jax.experimental.pallas import tpu as pltpu
from jax.sharding import Mesh
from jax.sharding import PartitionSpec as P

AXES = ("ep_0", "ep_1", "ep_2", "dp")
EP = AXES[:3]
MESH = pl.DeviceIdType.MESH
F32, BF16, I32 = jnp.float32, jnp.bfloat16, jnp.int32

D, E, T, K, CAP = 2880, 128, 192, 4, 9
DPAD = 2944
SPLIT = 1408
FIRST, WIDTH = (SPLIT, 0), (DPAD - SPLIT, SPLIT)
PER = 27
ROWS = 112
MAIN, LAST = 96, 16
ES = 4 * CAP
KQ = ES * 8
PIECES = ((0, 640), (640, 640), (1280, 128))
N = 3
HALF = MAIN // 2
BLK = 896
OUT = 768
TOTAL = 24576
G_EX, G_OWN, G_OG, G_LS, G_OL = 0, 2, 4, 6, 8
G_SMALL, G_TK, G_SP, G_RS, G_TL, G_TO = range(10, 16)


def dot(a, b, dims=((1,), (0,)), **kw):
    return lax.dot_general(a, b, (dims, ((), ())), preferred_element_type=F32, **kw)


def iota(shape, dim):
    return lax.broadcasted_iota(I32, shape, dim)


def kernel(
    tok_h, og_h, idx_h, ex_h, w_h, b_h, bs_s,
    tg_o, small_o,
    tokraw, tokp, ogfull, og0, og1, idxv, ev3, ev, wv, bv,
    snd0, snd1, tr0, tr1, ex0, ex1, exl0, exl1, tls, trt, ext, ogr, tokr,
    cntsnd, cntr, cc_v, meta, metar, rowsel, rowlast, acc, gbuf, pds, pdr,
    psb, psr1, psr2, psb2, xcs, xcr, xps, xpr,
    lt, pt, mixv, spb, spr, selb, selr, rss, rsr, lgv,
    loc, ss, rr, og_r, ex2_r, exr, last_r, tr_r, tail_r, lg_r,
):
    y, z, c, x = (lax.axis_index(a) for a in AXES)
    og, snd, tr, ex, exl = (og0, og1), (snd0, snd1), (tr0, tr1), (ex0, ex1), (exl0, exl1)
    m4 = lambda v: lax.rem(v + 4, 4)
    po = (z, y)
    pe = (y, z)
    other = 1 - c

    def at(dy=0, dz=0, cc=None, dx=0):
        return (m4(y + dy), m4(z + dz), c if cc is None else cc, m4(x + dx))

    og_dev = (lambda s: at(dz=s), lambda s: at(dy=s))
    ex_dev = (lambda s, cc: at(dy=s, cc=cc), lambda s, cc: at(dz=s, cc=cc))

    def remote(src, dst, ss, rs, dev):
        return pltpu.make_async_remote_copy(src_ref=src, dst_ref=dst, send_sem=ss, recv_sem=rs, device_id=dev, device_id_type=MESH)

    def send(src, dst, group, recv, dev):
        remote(src, dst, ss.at[group], recv, dev).start()

    def got(ref, sem):
        remote(ref, ref, sem, sem, at(dx=1)).wait_recv()

    def drain(ref, group):
        remote(ref, ref, ss.at[group], ss.at[group], at(dx=1)).wait_send()

    loads = [
        pltpu.make_async_copy(idx_h, idxv, loc.at[0]),
        pltpu.make_async_copy(og_h, ogfull, loc.at[1]),
        pltpu.make_async_copy(tok_h, tokraw, loc.at[2]),
        pltpu.make_async_copy(w_h, wv, loc.at[3]),
        pltpu.make_async_copy(b_h, bv, loc.at[4]),
    ] + [pltpu.make_async_copy(ex_h.at[:, q * 8 : q * 8 + 8, :], ev3.at[q], loc.at[5]) for q in range(4)]
    loads[0].start()
    for n in range(4):
        rows = pl.ds(48 * n, 48)
        pltpu.make_async_copy(og_h.at[rows, :], ogfull.at[rows, :], loc.at[1]).start()
    for l in loads[2:]:
        l.start()
    peers = [at(dy=a, dz=b) for a in range(4) for b in range(4) if a or b]
    peers += [at(dy=a, cc=other) for a in (1, 2, 3)] + [at(dz=a, cc=other) for a in (1, 2, 3)]
    peers += [at(cc=other)] + [at(dx=a, cc=k) for a in (1, 2, 3) for k in (c, other)]
    barrier = pltpu.get_barrier_semaphore()
    for p in peers:
        pl.semaphore_signal(barrier, inc=1, device_id=p, device_id_type=MESH)

    loads[0].wait()
    idx = idxv[...]
    ie = iota((E, T), 0)
    named = jnp.zeros((E, T), F32)
    for k in range(K):
        named += jnp.where(idx[k : k + 1, :] == ie, 1.0, 0.0)
    nb = named.astype(BF16)
    upper = jnp.where(iota((T, T), 0) < iota((T, T), 1), 1.0, 0.0).astype(BF16)
    ones_tt = jnp.ones((T, T), BF16)
    r_e, c_e = iota((E, E), 0), iota((E, E), 1)
    same_ep = jnp.where((r_e // 4 == c_e // 4) & (c_e < r_e), 1.0, 0.0).astype(BF16)
    ahead = dot(same_ep, nb).astype(BF16)
    rowpos = dot(nb, upper) + dot(ahead, ones_tt)
    cntsnd[...] = dot(jnp.ones((8, T), BF16), nb, ((1,), (1,)))
    meta[...] = jnp.full((8, 256), -1e6, F32)
    for k in range(K):
        ik = idx[k : k + 1, :]
        off = jnp.sum(jnp.where(ik == ie, rowpos, 0.0), axis=0, keepdims=True)
        ey, ez, ec = ik // 32, (ik // 8) % 4, (ik // 4) % 2
        for h, (ea, eb) in enumerate(((ey, ez), (ez, ey))):
            step, same = (ea - pe[h] + 4) % 4, ec == c
            near = jnp.where(step == 1, jnp.where(same, 2, 6), jnp.where(same, 3, 7))
            slot = jnp.where(step == 0, jnp.where(same, 0, 1), jnp.where(step == 2, 4 + ec, near))
            code = (eb * 1024 + slot * 32).astype(F32) + off
            meta[4 * h + k : 4 * h + k + 1, 0:T] = code

    loads[1].wait()
    own_og = [pl.ds(pl.multiple_of(po[h] * T, T), T) for h in range(2)]
    og0[own_og[0], WIDTH[0] - 128 : WIDTH[0]] = jnp.zeros((T, 128), BF16)
    og0[own_og[0], 0 : D - SPLIT] = ogfull[:, SPLIT:D]
    og1[own_og[1], :] = ogfull[:, 0:SPLIT]
    pl.semaphore_wait(barrier, len(peers))

    zc = z * 2 + c
    cntr[y, zc] = cntsnd[...]
    zpeers = [(b, k) for b in (1, 2, 3) for k in (0, 1)] + [(0, 1)]
    zdev = lambda b, k: at(dz=b, cc=lax.rem(c + k, 2))
    for n, (b, k) in enumerate(zpeers):
        send(cntsnd, cntr.at[y, zc], G_SMALL, rr.at[0], zdev(b, k))
    for h in range(2):
        for s in (1, 2, 3):
            send(meta, metar.at[h, po[h]], G_SMALL, rr.at[2 + h], og_dev[h](s))

    def og_rows(pos, second):
        return pl.ds(pl.multiple_of(pos * T + second * 96, 32), 96)

    def og_send(h, d, m):
        where = og_rows(po[h], d ^ m)
        send(og[h].at[where, :], og[h].at[where, :], G_OG + h, og_r.at[h, 2 if m else d], og_dev[h](1 - 2 * d))

    for h in range(2):
        for d in range(2):
            og_send(h, d, 0)

    got(cntr.at[0, 0:7], rr.at[0])
    for s in (1, 2, 3):
        send(cntr.at[y], cntr.at[y], G_SMALL, rr.at[1], at(dy=s))
    for h in range(2):
        for d in range(2):
            og_send(h, d, 1)

    loads[2].wait()
    tokp[:, DPAD - 128 : DPAD] = jnp.zeros((T, 128), BF16)
    tokp[:, 0:D] = tokraw[...]

    def block(pos):
        return pl.ds(pl.multiple_of((pos * 720) // 128 * 128, 128), BLK)

    xc = x * 2 + c
    xpeers = [(a, k) for a in (1, 2, 3) for k in (0, 1)] + [(0, 1)]
    xdev = lambda a, k: at(dx=a, cc=lax.rem(c + k, 2))
    tokr[xc] = tokp[:, block(x)]
    for n, (a, k) in enumerate(xpeers):
        send(tokp.at[:, block(m4(x + a))], tokr.at[xc], G_TK, rr.at[4], xdev(a, k))

    loads[3].wait()
    loads[4].wait()
    logits = jnp.transpose(dot(tokp[:, 0:D], wv[...]) + bv[...])
    lt[...] = logits
    ex_l = jnp.exp(logits - jnp.max(logits, axis=0, keepdims=True))
    prob = ex_l / jnp.sum(ex_l, axis=0, keepdims=True)
    pt[...] = prob
    picked = [jnp.sum(jnp.where(idx[k : k + 1, :] == ie, logits, 0.0), axis=0, keepdims=True) for k in range(K)]
    top = jnp.maximum(jnp.maximum(picked[0], picked[1]), jnp.maximum(picked[2], picked[3]))
    picked = [jnp.exp(p - top) for p in picked]
    total = picked[0] + picked[1] + picked[2] + picked[3]
    for k in range(K):
        mixv[k : k + 1, :] = picked[k] / total
    diag = r_e == c_e
    pcol = jnp.sum(prob, axis=1, keepdims=True)
    prow = jnp.sum(jnp.where(diag, pcol, 0.0), axis=0, keepdims=True)
    psb[...] = jnp.broadcast_to(prow, (8, E))
    for n, (b, k) in enumerate(zpeers):
        send(psb, psr1.at[zc], G_SMALL, rr.at[5], zdev(b, k))
    psr1[zc] = psb[...]

    pltpu.make_async_copy(ev3, ev3, loc.at[5]).wait()
    ev[:, DPAD - 128 : DPAD] = jnp.zeros((4 * KQ, 128), BF16)

    def flatten(n, _):
        q, p = n // (ES // 2), lax.rem(n, ES // 2)
        pair = jnp.concatenate([ev3[q, 2 * p], ev3[q, 2 * p + 1]], axis=0)
        ev[pl.ds(pl.multiple_of(n * 16, 16), 16), 0:D] = pair
        return 0

    lax.fori_loop(0, 4 * ES // 2, flatten, 0)

    def og_from(d, h):
        return m4(po[h] - (1 - 2 * d))

    for h in range(2):
        for d in range(2):
            where = og_rows(og_from(d, h), d)
            got(og[h].at[where, :], og_r.at[h, d])
            send(og[h].at[where, :], og[h].at[where, :], G_OG + h, og_r.at[h, 2], og_dev[h](1 - 2 * d))

    got(cntr.at[0:3], rr.at[1])
    counts = cntr[...]
    plane = jnp.sum(counts.reshape(32, 8, E), axis=0)
    xcs[...] = plane
    xcr[x] = plane
    for a in (1, 2, 3):
        send(xcs, xcr.at[x], G_SMALL, rr.at[7], at(dx=a))
    first = (y * 8 + z * 2 + c) * 4
    cb = counts.reshape(256, E).astype(BF16)
    for k in range(K):
        mine = jnp.where((r_e >= first) & (r_e <= first + k), 1.0, 0.0).astype(BF16)
        cc_v[k] = dot(cb, mine).astype(BF16)

    def gather(h, delta):
        q = m4(pe[h] + delta)
        row = iota((2 * ROWS, E), 0)
        core = jnp.where(row >= ROWS, 1, 0)
        rr = row - core * ROWS
        i = jnp.where(rr >= PER, 1, 0) + jnp.where(rr >= 2 * PER, 1, 0) + jnp.where(rr >= 3 * PER, 1, 0)
        r = rr - i * PER
        i = i + po[h] + 1
        i = jnp.where(i >= 4, i - 4, i)
        dev = (q * 8 + i * 2 + core) if h == 0 else (i * 8 + q * 2 + core)
        pick = (jnp.broadcast_to(dev[:, 0:1] * 8, (2 * ROWS, 256)) == iota((2 * ROWS, 256), 1))
        pick = jnp.where(pick, 1.0, 0.0).astype(BF16)
        t = [dot(pick, cc_v[k]).astype(I32) for k in range(K)]
        e_in = jnp.where(r >= t[0], 1, 0) + jnp.where(r >= t[1], 1, 0) + jnp.where(r >= t[2], 1, 0)
        base = jnp.where(r >= t[2], t[2], jnp.where(r >= t[1], t[1], jnp.where(r >= t[0], t[0], 0)))
        es = e_in * CAP + r - base
        target = (es * 8 + i * 2 + core) if h == 0 else (i * KQ + es * 8 + q * 2 + core)
        target = jnp.where((r < t[3]) & (rr < 4 * PER), target, -1)
        depth = KQ if h == 0 else 4 * KQ
        sel = jnp.broadcast_to(target[:, 0:1], (2 * ROWS, depth)) == iota((2 * ROWS, depth), 1)
        sel = jnp.where(sel, 1.0, 0.0).astype(BF16)
        rows = pl.ds(pl.multiple_of(q * KQ, KQ), KQ) if h == 0 else pl.ds(0, 4 * KQ)
        for lo, w in PIECES:
            snd[h][delta, :, lo : lo + w] = dot(sel, ev[rows, FIRST[h] + lo : FIRST[h] + lo + w]).astype(BF16)
        if h == 0:
            tail = dot(sel, ev[rows, DPAD - 128 : DPAD])
            snd[h][delta, :, SPLIT : SPLIT + 128] = tail.astype(BF16)
            for k in range(2):
                upper, lower = (tail[k * ROWS + j * HALF : k * ROWS + j * HALF + HALF] for j in range(2))
                tls[delta, k] = (upper + pltpu.roll(lower, 64, 1)).astype(BF16)

    def core_rows(cc):
        return pl.ds(pl.multiple_of(cc * ROWS, 16), ROWS)

    def piece(h, ref, row, n):
        if n == N:
            return ref.at[pl.ds(pl.multiple_of(row + MAIN, 16), LAST), :]
        return ref.at[pl.ds(pl.multiple_of(row, 16), MAIN), pl.ds(*PIECES[n])]

    def landing(h, slot, n):
        return exl[h].at[slot] if n == N else ex[h].at[slot, :, pl.ds(*PIECES[n])]

    def landed(h, pair, n):
        return last_r.at[h] if n == N else exr.at[pair, n]

    def leaving(h, n):
        return (G_LS if n == N else G_EX) + h

    for h in range(2):
        gather(h, 2)
        for d in range(2):
            if h == 0:
                send(tls.at[2, d], trt.at[d], G_TL, tr_r.at[d], ex_dev[0](1 - 2 * d, c))
            for n in range(N + 1):
                send(
                    piece(h, snd[h].at[2], d * ROWS, n), piece(h, tr[h].at[d], 0, n),
                    leaving(h, n), ex2_r.at[h, d, n], ex_dev[h](1 - 2 * d, c),
                )

    def gather_rest(o, _):
        delta = jnp.where(o == 0, 1, jnp.where(o == 1, 3, 0))
        gather(0, delta)
        gather(1, delta)
        return 0

    lax.fori_loop(0, 3, gather_rest, 0)

    def ex1_send(far, pieces):
        cc = other if far else c
        for n in pieces:
            for h in range(2):
                for d in range(2):
                    slot = 3 - d + 4 * far
                    send(
                        piece(h, snd[h].at[1 + 2 * d], cc * ROWS, n), landing(h, slot, n),
                        leaving(h, n), landed(h, 1 + 2 * far, n), ex_dev[h](1 - 2 * d, cc),
                    )
                    if h == 0 and n == 0:
                        send(tls.at[1 + 2 * d, cc], ext.at[slot], G_TL, tail_r.at[1 + 2 * far], ex_dev[0](1 - 2 * d, cc))

    ex1_send(0, range(N))
    send(tls.at[0, other], ext.at[1], G_TO, tail_r.at[0], at(cc=other))
    ext[0] = tls[0, c]
    for h in range(2):
        for n in range(N + 1):
            send(piece(h, snd[h].at[0], other * ROWS, n), landing(h, 1, n), (G_OL if n == N else G_OWN) + h, landed(h, 0, n), at(cc=other))
        ex[h][0] = snd[h][0, pl.ds(pl.multiple_of(c * ROWS, 16), MAIN), 0:SPLIT]
        exl[h][0] = snd[h][0, pl.ds(pl.multiple_of(c * ROWS + MAIN, 16), LAST), :]

    for h in range(2):
        got(metar.at[h, 0:3], rr.at[2 + h])
        metar[h, po[h]] = meta[...]
        for i in range(4):
            code = metar[h, i, 4 * h : 4 * h + 4, 0:T].astype(I32) - po[h] * 1024
            slot = code // 32
            place = code - slot * 32 + m4(i - po[h] - 1) * PER
            valid = (code >= 0) & (code < 256)
            rowsel[h, :, i * T : (i + 1) * T] = jnp.where(valid & (place < MAIN), slot * MAIN + place, -1).astype(F32)
            rowlast[h, i] = jnp.where(valid & (place >= MAIN), slot * LAST + place - MAIN, -1).astype(F32)
        got(og[h].at[0 : 2 * T, :], og_r.at[h, 2])
    ogr[...] = pltpu.roll(og0[:, SPLIT : SPLIT + 128].astype(F32), 64, 1).astype(BF16)
    acc[...] = jnp.zeros_like(acc)

    def absorb(pair, mine):
        for n in range(N):
            if mine:
                got(ex[0].at[0:2, :, pl.ds(*PIECES[n])], exr.at[0, n])
            else:
                got(ex[0].at[0:4, :, pl.ds(*PIECES[n])], exr.at[pair, n])
            for h in range(2):
                lo, w = PIECES[n]
                block = ex[h][pl.ds(2 * pair, 2), :, lo : lo + w].reshape(2 * MAIN, w)
                part = dot(block, og[h][:, lo : lo + w], ((1,), (1,)))
                if n == 0:
                    gbuf[h] = part
                else:
                    gbuf[h] += part
            if n == 0:
                if mine:
                    got(ext.at[1], tail_r.at[0])
                else:
                    got(ext.at[pl.ds(2 * pair, 2)], tail_r.at[pair])
                tail = ext[pl.ds(2 * pair, 2)].reshape(MAIN, 128)
                for j, other_side in enumerate((og0[:, SPLIT : SPLIT + 128], ogr[...])):
                    part = dot(tail, other_side, ((1,), (1,)))
                    for slot in range(2):
                        where = slice(slot * MAIN + j * HALF, slot * MAIN + j * HALF + HALF)
                        gbuf[0, where, :] += part[slot * HALF : slot * HALF + HALF]
        rid = (iota((2 * MAIN, 128), 0) + pair * 2 * MAIN).astype(F32)
        for h in range(2):
            for lb in range(6):
                lanes = slice(lb * 128, lb * 128 + 128)
                g = gbuf[h, :, lanes]
                for k in range(K):
                    hit = jnp.where(rid == rowsel[h, k : k + 1, lanes], g, 0.0)
                    acc[h, k, :, lanes] += jnp.sum(hit.reshape(2 * MAIN // 8, 8, 128), axis=0)

    absorb(0, True)

    def forward(n):
        for h in range(2):
            for d in range(2):
                got(piece(h, tr[h].at[d], 0, n), ex2_r.at[h, d, n])
                send(
                    piece(h, tr[h].at[d], 0, n), landing(h, 4 + c, n),
                    leaving(h, n), landed(h, 2, n), ex_dev[h](1 - 2 * d, d),
                )

    for d in range(2):
        got(trt.at[d], tr_r.at[d])
        send(trt.at[d], ext.at[4 + c], G_TL, tail_r.at[2], ex_dev[0](1 - 2 * d, d))
    for n in range(N):
        forward(n)
    ex1_send(1, range(N))
    forward(N)
    for far in range(2):
        ex1_send(far, (N,))

    got(psr1.at[0:7], rr.at[5])
    psb2[...] = jnp.sum(psr1[...], axis=0)
    psr2[y] = psb2[...]
    for s in (1, 2, 3):
        send(psb2, psr2.at[y], G_SMALL, rr.at[6], at(dy=s))

    got(xcr.at[0:3], rr.at[7])
    cnt_row = jnp.sum(xcr[...], axis=0)[0:1, :]
    cnt_col = jnp.sum(jnp.where(diag, cnt_row, 0.0), axis=1, keepdims=True)
    push = bs_s[0] * E * (cnt_col / (TOTAL * K))
    prob = pt[...]
    spread = prob * (push - jnp.sum(prob * push, axis=0, keepdims=True))
    lt[...] = spread
    spb[...] = jnp.zeros_like(spb)
    for par in range(2):
        for n in range(16):
            spb[par, 4 * n : 4 * n + 4, 0:T] = spread[8 * n + 4 * par : 8 * n + 4 * par + 4, :]
        for k in range(K):
            ik = idxv[k : k + 1, :]
            spb[par, 64 + k : 65 + k, 0:T] = jnp.where((ik // 4) % 2 == par, ik // 8 * 4 + ik % 4, -1).astype(F32)
    for n, (a, k) in enumerate(xpeers):
        send(spb.at[lax.rem(c + k, 2)], spr.at[xc], G_SP, rr.at[9], xdev(a, k))
    spr[xc] = spb[c]

    def arrivals(pair, _):
        absorb(pair, False)
        return 0

    lax.fori_loop(1, 4, arrivals, 0)

    for h in range(2):
        for i in range(4):
            pds[h, i] = jnp.zeros((K, 256), F32)
            for k in range(K):
                pds[h, i, k : k + 1, 0:T] = jnp.sum(acc[h, k, :, i * T : (i + 1) * T], axis=0, keepdims=True)
        for s in (1, 2, 3):
            send(pds.at[h, m4(po[h] + s)], pdr.at[h, po[h]], G_SMALL, rr.at[10 + h], og_dev[h](s))
        pdr[h, po[h]] = pds[h, po[h]]
    late = [jnp.zeros((1, T), F32)] * K
    rid = iota((8 * LAST, T), 0).astype(F32)
    for h in range(2):
        got(exl[h].at[1:8], last_r.at[h])
    both = [dot(exl[h][...].reshape(8 * LAST, WIDTH[h]), og[h][own_og[h], :], ((1,), (1,))) for h in range(2)]
    for h in range(2):
        g = both[h]
        for k in range(K):
            hit = jnp.where(rid == rowlast[h, po[h], k : k + 1, :], g, 0.0)
            late[k] += jnp.sum(hit, axis=0, keepdims=True)

    pd = jnp.zeros((K, 256), F32)
    for h in range(2):
        got(pdr.at[h, 0:3], rr.at[10 + h])
        pd += (pdr[h, 0] + pdr[h, 1]) + (pdr[h, 2] + pdr[h, 3])

    dots = [pd[k : k + 1, 0:T] + late[k] for k in range(K)]
    mix = [mixv[k : k + 1, :] for k in range(K)]
    mean = mix[0] * dots[0] + mix[1] * dots[1] + mix[2] * dots[2] + mix[3] * dots[3]
    for k in range(K):
        selb[k : k + 1, 0:T] = mix[k] * (dots[k] - mean)
    selb[:, T:256] = jnp.zeros((K, 256 - T), F32)
    for n, (a, k) in enumerate(xpeers):
        send(selb, selr.at[xc], G_SMALL, lg_r.at[xc], xdev(a, k))

    lg = jnp.zeros((E, T), F32)
    for k in range(K):
        lg += jnp.where(idxv[k : k + 1, :] == ie, selb[k : k + 1, 0:T], 0.0)
    lgv[...] = jnp.transpose(lt[...] + lg).astype(BF16)
    got(psr2.at[0:3], rr.at[6])
    xps[...] = jnp.sum(psr2[...], axis=0)
    xpr[x] = xps[...]
    for a in (1, 2, 3):
        send(xps, xpr.at[x], G_SMALL, rr.at[8], at(dx=a))
    got(tokr.at[0:7], rr.at[4])
    got(spr.at[0:7], rr.at[9])

    ir = iota((64, T), 0).astype(F32)

    def weight_term(src, sel):
        named = jnp.zeros((64, T), F32)
        for k in range(K):
            named += jnp.where(spr[src, 64 + k : 65 + k, 0:T] == ir, sel[k : k + 1, 0:T], 0.0)
        return dot((spr[src, 0:64, 0:T] + named).astype(BF16), tokr[src])

    wsum = weight_term(xc, selb)
    for a, k in reversed(xpeers):
        src = m4(x + a) * 2 + lax.rem(c + k, 2)
        got(selr.at[src], lg_r.at[src])
        wsum += weight_term(src, selr.at[src])
    shift = x * 720 - (x * 720) // 128 * 128
    wsum = pltpu.roll(wsum, lax.rem(BLK - shift, BLK), 1)
    for n in range(16):
        rss[n] = wsum[4 * n : 4 * n + 4, 0:OUT]

    chip = y * 4 + z
    hops = lambda v: min(v[0], 4 - v[0]) + min(v[1], 4 - v[1])
    for n, (a, b) in enumerate(sorted([(a, b) for a in range(4) for b in range(4) if a or b], key=hops, reverse=True)):
        dest = m4(y + a) * 4 + m4(z + b)
        send(rss.at[dest], rsr.at[chip], G_RS, rr.at[12], at(dy=a, dz=b))
    rsr[chip] = rss[chip]
    tg_o[...] = dot(lgv[...], wv[...], ((1,), (1,))).astype(BF16)

    got(xpr.at[0:3], rr.at[8])
    ps_row = jnp.sum(xpr[...], axis=0)[0:1, :]
    loss = E * jnp.sum((cnt_row / (TOTAL * K)) * (ps_row / TOTAL), axis=1, keepdims=True)
    small_o[4:8, :] = jnp.broadcast_to(loss, (4, OUT))

    for h in range(2):
        drain(ex[h], G_EX + h)
        drain(exl[h], G_LS + h)
        drain(ex[h].at[0], G_OWN + h)
        drain(exl[h].at[0], G_OL + h)
        drain(og[h].at[0 : 3 * T, :], G_OG + h)
    for ref, group in (
        (spr.at[0:4], G_SMALL),
        (tokr.at[0:7], G_TK), (spr.at[0:7], G_SP), (tls, G_TL), (tls.at[0, 0], G_TO), (rsr.at[0:15], G_RS),
    ):
        drain(ref, group)
    got(rsr.at[0:15], rr.at[12])
    out = jnp.sum(rsr[...], axis=0) * (1.0 / math.sqrt(TOTAL))
    small_o[0:4, :] = out[:, 0:OUT]


def finish(tg_ref, small_ref, tg_o, wt_o, loss_o, wtv, lossv, sem):
    tg_out = [pltpu.make_async_copy(tg_ref.at[48 * n : 48 * n + 48], tg_o.at[48 * n : 48 * n + 48], sem.at[3 + n]) for n in range(4)]
    for t in tg_out:
        t.start()
    wtv[...] = small_ref[0:4, 0:720]
    wt_out = pltpu.make_async_copy(wtv, wt_o, sem.at[1])
    wt_out.start()
    lossv[0] = jnp.sum(small_ref[4:5, 0:1])
    loss_out = pltpu.make_async_copy(lossv, loss_o, sem.at[2])
    loss_out.start()
    loss_out.wait()
    for t in tg_out:
        t.wait()
    wt_out.wait()


def on_device(tokens, out_grad, indices, expert_rows, router_weight, router_bias, balance_scale):
    rows = jnp.transpose(expert_rows[0], (0, 2, 1, 3)).reshape(ES, 32, D)
    dma = pltpu.SemaphoreType.DMA
    vm = pltpu.VMEM
    scratch = [
        vm((T, D), BF16), vm((T, DPAD), BF16), vm((T, D), BF16), vm((4 * T, WIDTH[0]), BF16), vm((4 * T, WIDTH[1]), BF16),
        vm((K, T), I32), vm((4, ES, 8, D), BF16), vm((4 * KQ, DPAD), BF16), vm((D, E), BF16), vm((1, E), F32),
        vm((4, 2 * ROWS, WIDTH[0]), BF16), vm((4, 2 * ROWS, WIDTH[1]), BF16),
        vm((2, ROWS, WIDTH[0]), BF16), vm((2, ROWS, WIDTH[1]), BF16),
        vm((8, MAIN, SPLIT), BF16), vm((8, MAIN, SPLIT), BF16), vm((8, LAST, WIDTH[0]), BF16), vm((8, LAST, WIDTH[1]), BF16),
        vm((4, 2, HALF, 128), BF16), vm((2, HALF, 128), BF16), vm((8, HALF, 128), BF16), vm((4 * T, 128), BF16),
        vm((8, T, BLK), BF16),
        vm((8, E), F32), vm((4, 8, 8, E), F32), vm((K, 256, E), BF16), vm((8, 256), F32), vm((2, 4, 8, 256), F32),
        vm((2, K, 4 * T), F32), vm((2, 4, K, T), F32), vm((2, K, 8, 4 * T), F32), vm((2, 2 * MAIN, 4 * T), F32), vm((2, 4, K, 256), F32), vm((2, 4, K, 256), F32),
        vm((8, E), F32), vm((8, 8, E), F32), vm((4, 8, E), F32), vm((8, E), F32),
        vm((8, E), F32), vm((4, 8, E), F32), vm((8, E), F32), vm((4, 8, E), F32),
        vm((E, T), F32), vm((E, T), F32), vm((K, T), F32), vm((2, 72, 256), F32), vm((8, 72, 256), F32),
        vm((K, 256), F32), vm((8, K, 256), F32), vm((16, 4, OUT), F32), vm((16, 4, OUT), F32), vm((T, E), BF16),
        dma((6,)), dma((16,)), dma((13,)), dma((2, 3)), dma((2, 2, N + 1)), dma((4, N)), dma((2,)), dma((2,)), dma((4,)), dma((8,)),
    ]
    hbm = pl.BlockSpec(memory_space=pltpu.HBM)
    in_vmem = pl.BlockSpec(memory_space=vm)
    token_grad, small = pl.pallas_call(
        kernel,
        out_shape=(vm((T, D), BF16), vm((8, OUT), F32)),
        in_specs=[hbm] * 6 + [pl.BlockSpec(memory_space=pltpu.SMEM)],
        out_specs=(in_vmem, in_vmem),
        scratch_shapes=scratch,
        compiler_params=pltpu.CompilerParams(collective_id=0, has_side_effects=True, vmem_limit_bytes=54000 * 1024),
        name="router",
    )(
        *(
            pltpu.with_memory_space_constraint(a, pltpu.HBM)
            for a in (tokens, out_grad, indices.T, rows, router_weight, router_bias.reshape(1, E))
        ),
        balance_scale,
    )
    token_grad, weight_grad, loss = pl.pallas_call(
        finish,
        out_shape=(
            jax.ShapeDtypeStruct((T, D), BF16),
            jax.ShapeDtypeStruct((4, 720), F32),
            jax.ShapeDtypeStruct((1,), F32),
        ),
        in_specs=[in_vmem] * 2,
        out_specs=(hbm, hbm, hbm),
        scratch_shapes=[vm((4, 720), F32), pltpu.SMEM((1,), F32), dma((7,))],
        name="finish",
    )(*(pltpu.with_memory_space_constraint(a, vm) for a in (token_grad, small)))
    return token_grad, weight_grad.T, loss


def solution(mesh):
    torus = Mesh(mesh.devices.reshape(4, 4, 2, mesh.shape["dp"]), AXES)
    return jax.shard_map(
        on_device,
        mesh=torus,
        in_specs=(P(AXES, None), P(AXES, None), P(AXES, None), P("dp", EP, None, None, None), P(), P(), P()),
        out_specs=(P(AXES, None), P("dp", EP), P()),
        check_vma=False,
    )
```

```python
import math

import jax
import jax.numpy as jnp
from jax import lax
from jax.experimental import pallas as pl
from jax.experimental.pallas import tpu as pltpu
from jax.sharding import Mesh
from jax.sharding import PartitionSpec as P

AXES = ("ep_0", "ep_1", "ep_2", "dp")
EP = AXES[:3]
MESH = pl.DeviceIdType.MESH
F32, BF16, I32 = jnp.float32, jnp.bfloat16, jnp.int32

D, E, T, K, CAP = 2880, 128, 192, 4, 9
DPAD = 2944
SPLIT = 1408
FIRST, WIDTH = (SPLIT, 0), (DPAD - SPLIT, SPLIT)
PER = 27
ROWS = 112
MAIN, LAST = 96, 16
ES = 4 * CAP
KQ = ES * 8
PIECES = ((0, 640), (640, 640), (1280, 128))
N = 3
HALF = MAIN // 2
BLK = 896
OUT = 768
TOTAL = 24576
G_EX, G_OWN, G_OG, G_LS, G_OL = 0, 2, 4, 6, 8
G_SMALL, G_TK, G_SP, G_RS, G_TL, G_TO = range(10, 16)


def dot(a, b, dims=((1,), (0,)), **kw):
    return lax.dot_general(a, b, (dims, ((), ())), preferred_element_type=F32, **kw)


def iota(shape, dim):
    return lax.broadcasted_iota(I32, shape, dim)


def kernel(
    tok_h, og_h, idx_h, ex_h, w_h, b_h, bs_s,
    tg_o, small_o,
    tokraw, tokp, ogfull, og0, og1, idxv, ev3, ev, wv, bv,
    snd0, snd1, tr0, tr1, ex0, ex1, exl0, exl1, tls, trt, ext, ogr, tokr,
    cntsnd, cntr, cc_v, meta, metar, rowsel, rowlast, acc, gbuf, pds, pdr,
    psb, psr1, psr2, psb2, xcs, xcr, xps, xpr,
    lt, pt, mixv, spb, spr, selb, selr, rss, rsr, lgv,
    loc, ss, rr, og_r, ex2_r, exr, last_r, tr_r, tail_r, lg_r,
):
    y, z, c, x = (lax.axis_index(a) for a in AXES)
    og, snd, tr, ex, exl = (og0, og1), (snd0, snd1), (tr0, tr1), (ex0, ex1), (exl0, exl1)
    m4 = lambda v: lax.rem(v + 4, 4)
    po = (z, y)
    pe = (y, z)
    other = 1 - c

    def at(dy=0, dz=0, cc=None, dx=0):
        return (m4(y + dy), m4(z + dz), c if cc is None else cc, m4(x + dx))

    og_dev = (lambda s: at(dz=s), lambda s: at(dy=s))
    ex_dev = (lambda s, cc: at(dy=s, cc=cc), lambda s, cc: at(dz=s, cc=cc))

    def remote(src, dst, ss, rs, dev):
        return pltpu.make_async_remote_copy(src_ref=src, dst_ref=dst, send_sem=ss, recv_sem=rs, device_id=dev, device_id_type=MESH)

    def send(src, dst, group, recv, dev):
        remote(src, dst, ss.at[group], recv, dev).start()

    def got(ref, sem):
        remote(ref, ref, sem, sem, at(dx=1)).wait_recv()

    def drain(ref, group):
        remote(ref, ref, ss.at[group], ss.at[group], at(dx=1)).wait_send()

    loads = [
        pltpu.make_async_copy(idx_h, idxv, loc.at[0]),
        pltpu.make_async_copy(og_h, ogfull, loc.at[1]),
        pltpu.make_async_copy(tok_h, tokraw, loc.at[2]),
        pltpu.make_async_copy(w_h, wv, loc.at[3]),
        pltpu.make_async_copy(b_h, bv, loc.at[4]),
    ] + [pltpu.make_async_copy(ex_h.at[:, q * 8 : q * 8 + 8, :], ev3.at[q], loc.at[5]) for q in range(4)]
    loads[0].start()
    for n in range(4):
        rows = pl.ds(48 * n, 48)
        pltpu.make_async_copy(og_h.at[rows, :], ogfull.at[rows, :], loc.at[1]).start()
    for l in loads[2:]:
        l.start()
    peers = [at(dy=a) for a in (1, 2, 3)] + [at(dz=a, cc=k) for a in (1, 2, 3) for k in (c, other)]
    peers += [at(cc=other)] + [at(dx=a, cc=k) for a in (1, 2, 3) for k in (c, other)]
    barrier = pltpu.get_barrier_semaphore()
    for p in peers:
        pl.semaphore_signal(barrier, inc=1, device_id=p, device_id_type=MESH)

    loads[0].wait()
    idx = idxv[...]
    ie = iota((E, T), 0)
    named = jnp.zeros((E, T), F32)
    for k in range(K):
        named += jnp.where(idx[k : k + 1, :] == ie, 1.0, 0.0)
    nb = named.astype(BF16)
    upper = jnp.where(iota((T, T), 0) < iota((T, T), 1), 1.0, 0.0).astype(BF16)
    ones_tt = jnp.ones((T, T), BF16)
    r_e, c_e = iota((E, E), 0), iota((E, E), 1)
    same_ep = jnp.where((r_e // 4 == c_e // 4) & (c_e < r_e), 1.0, 0.0).astype(BF16)
    ahead = dot(same_ep, nb).astype(BF16)
    rowpos = dot(nb, upper) + dot(ahead, ones_tt)
    cntsnd[...] = dot(jnp.ones((8, T), BF16), nb, ((1,), (1,)))
    meta[...] = jnp.full((8, 256), -1e6, F32)
    for k in range(K):
        ik = idx[k : k + 1, :]
        off = jnp.sum(jnp.where(ik == ie, rowpos, 0.0), axis=0, keepdims=True)
        ey, ez, ec = ik // 32, (ik // 8) % 4, (ik // 4) % 2
        for h, (ea, eb) in enumerate(((ey, ez), (ez, ey))):
            step, same = (ea - pe[h] + 4) % 4, ec == c
            near = jnp.where(step == 1, jnp.where(same, 2, 6), jnp.where(same, 3, 7))
            slot = jnp.where(step == 0, jnp.where(same, 0, 1), jnp.where(step == 2, 4 + ec, near))
            code = (eb * 1024 + slot * 32).astype(F32) + off
            meta[4 * h + k : 4 * h + k + 1, 0:T] = code

    loads[1].wait()
    own_og = [pl.ds(pl.multiple_of(po[h] * T, T), T) for h in range(2)]
    og0[own_og[0], WIDTH[0] - 128 : WIDTH[0]] = jnp.zeros((T, 128), BF16)
    og0[own_og[0], 0 : D - SPLIT] = ogfull[:, SPLIT:D]
    og1[own_og[1], :] = ogfull[:, 0:SPLIT]
    pl.semaphore_wait(barrier, len(peers))

    zc = z * 2 + c
    cntr[y, zc] = cntsnd[...]
    zpeers = [(b, k) for b in (1, 2, 3) for k in (0, 1)] + [(0, 1)]
    zdev = lambda b, k: at(dz=b, cc=lax.rem(c + k, 2))
    for n, (b, k) in enumerate(zpeers):
        send(cntsnd, cntr.at[y, zc], G_SMALL, rr.at[0], zdev(b, k))
    for h in range(2):
        for s in (1, 2, 3):
            send(meta, metar.at[h, po[h]], G_SMALL, rr.at[2 + h], og_dev[h](s))

    def og_rows(pos, second):
        return pl.ds(pl.multiple_of(pos * T + second * 96, 32), 96)

    def og_send(h, d, m):
        where = og_rows(po[h], d ^ m)
        send(og[h].at[where, :], og[h].at[where, :], G_OG + h, og_r.at[h, 2 if m else d], og_dev[h](1 - 2 * d))

    for h in range(2):
        for d in range(2):
            og_send(h, d, 0)

    got(cntr.at[0, 0:7], rr.at[0])
    for s in (1, 2, 3):
        send(cntr.at[y], cntr.at[y], G_SMALL, rr.at[1], at(dy=s))
    for h in range(2):
        for d in range(2):
            og_send(h, d, 1)

    loads[2].wait()
    tokp[:, DPAD - 128 : DPAD] = jnp.zeros((T, 128), BF16)
    tokp[:, 0:D] = tokraw[...]

    def block(pos):
        return pl.ds(pl.multiple_of((pos * 720) // 128 * 128, 128), BLK)

    xc = x * 2 + c
    xpeers = [(a, k) for a in (1, 2, 3) for k in (0, 1)] + [(0, 1)]
    xdev = lambda a, k: at(dx=a, cc=lax.rem(c + k, 2))
    tokr[xc] = tokp[:, block(x)]
    for n, (a, k) in enumerate(xpeers):
        send(tokp.at[:, block(m4(x + a))], tokr.at[xc], G_TK, rr.at[4], xdev(a, k))

    loads[3].wait()
    loads[4].wait()
    logits = jnp.transpose(dot(tokp[:, 0:D], wv[...]) + bv[...])
    lt[...] = logits
    ex_l = jnp.exp(logits - jnp.max(logits, axis=0, keepdims=True))
    prob = ex_l / jnp.sum(ex_l, axis=0, keepdims=True)
    pt[...] = prob
    picked = [jnp.sum(jnp.where(idx[k : k + 1, :] == ie, logits, 0.0), axis=0, keepdims=True) for k in range(K)]
    top = jnp.maximum(jnp.maximum(picked[0], picked[1]), jnp.maximum(picked[2], picked[3]))
    picked = [jnp.exp(p - top) for p in picked]
    total = picked[0] + picked[1] + picked[2] + picked[3]
    for k in range(K):
        mixv[k : k + 1, :] = picked[k] / total
    diag = r_e == c_e
    pcol = jnp.sum(prob, axis=1, keepdims=True)
    prow = jnp.sum(jnp.where(diag, pcol, 0.0), axis=0, keepdims=True)
    psb[...] = jnp.broadcast_to(prow, (8, E))
    for n, (b, k) in enumerate(zpeers):
        send(psb, psr1.at[zc], G_SMALL, rr.at[5], zdev(b, k))
    psr1[zc] = psb[...]

    pltpu.make_async_copy(ev3, ev3, loc.at[5]).wait()
    ev[:, DPAD - 128 : DPAD] = jnp.zeros((4 * KQ, 128), BF16)

    def flatten(n, _):
        q, p = n // (ES // 2), lax.rem(n, ES // 2)
        pair = jnp.concatenate([ev3[q, 2 * p], ev3[q, 2 * p + 1]], axis=0)
        ev[pl.ds(pl.multiple_of(n * 16, 16), 16), 0:D] = pair
        return 0

    lax.fori_loop(0, 4 * ES // 2, flatten, 0)

    def og_from(d, h):
        return m4(po[h] - (1 - 2 * d))

    for h in range(2):
        for d in range(2):
            where = og_rows(og_from(d, h), d)
            got(og[h].at[where, :], og_r.at[h, d])
            send(og[h].at[where, :], og[h].at[where, :], G_OG + h, og_r.at[h, 2], og_dev[h](1 - 2 * d))

    got(cntr.at[0:3], rr.at[1])
    counts = cntr[...]
    plane = jnp.sum(counts.reshape(32, 8, E), axis=0)
    xcs[...] = plane
    xcr[x] = plane
    for a in (1, 2, 3):
        send(xcs, xcr.at[x], G_SMALL, rr.at[7], at(dx=a))
    first = (y * 8 + z * 2 + c) * 4
    cb = counts.reshape(256, E).astype(BF16)
    for k in range(K):
        mine = jnp.where((r_e >= first) & (r_e <= first + k), 1.0, 0.0).astype(BF16)
        cc_v[k] = dot(cb, mine).astype(BF16)

    def gather(h, delta):
        q = m4(pe[h] + delta)
        row = iota((2 * ROWS, E), 0)
        core = jnp.where(row >= ROWS, 1, 0)
        rr = row - core * ROWS
        i = jnp.where(rr >= PER, 1, 0) + jnp.where(rr >= 2 * PER, 1, 0) + jnp.where(rr >= 3 * PER, 1, 0)
        r = rr - i * PER
        i = i + po[h] + 1
        i = jnp.where(i >= 4, i - 4, i)
        dev = (q * 8 + i * 2 + core) if h == 0 else (i * 8 + q * 2 + core)
        pick = (jnp.broadcast_to(dev[:, 0:1] * 8, (2 * ROWS, 256)) == iota((2 * ROWS, 256), 1))
        pick = jnp.where(pick, 1.0, 0.0).astype(BF16)
        t = [dot(pick, cc_v[k]).astype(I32) for k in range(K)]
        e_in = jnp.where(r >= t[0], 1, 0) + jnp.where(r >= t[1], 1, 0) + jnp.where(r >= t[2], 1, 0)
        base = jnp.where(r >= t[2], t[2], jnp.where(r >= t[1], t[1], jnp.where(r >= t[0], t[0], 0)))
        es = e_in * CAP + r - base
        target = (es * 8 + i * 2 + core) if h == 0 else (i * KQ + es * 8 + q * 2 + core)
        target = jnp.where((r < t[3]) & (rr < 4 * PER), target, -1)
        depth = KQ if h == 0 else 4 * KQ
        sel = jnp.broadcast_to(target[:, 0:1], (2 * ROWS, depth)) == iota((2 * ROWS, depth), 1)
        sel = jnp.where(sel, 1.0, 0.0).astype(BF16)
        rows = pl.ds(pl.multiple_of(q * KQ, KQ), KQ) if h == 0 else pl.ds(0, 4 * KQ)
        for lo, w in PIECES:
            snd[h][delta, :, lo : lo + w] = dot(sel, ev[rows, FIRST[h] + lo : FIRST[h] + lo + w]).astype(BF16)
        if h == 0:
            tail = dot(sel, ev[rows, DPAD - 128 : DPAD])
            snd[h][delta, :, SPLIT : SPLIT + 128] = tail.astype(BF16)
            for k in range(2):
                upper, lower = (tail[k * ROWS + j * HALF : k * ROWS + j * HALF + HALF] for j in range(2))
                tls[delta, k] = (upper + pltpu.roll(lower, 64, 1)).astype(BF16)

    def core_rows(cc):
        return pl.ds(pl.multiple_of(cc * ROWS, 16), ROWS)

    def piece(h, ref, row, n):
        if n == N:
            return ref.at[pl.ds(pl.multiple_of(row + MAIN, 16), LAST), :]
        return ref.at[pl.ds(pl.multiple_of(row, 16), MAIN), pl.ds(*PIECES[n])]

    def landing(h, slot, n):
        return exl[h].at[slot] if n == N else ex[h].at[slot, :, pl.ds(*PIECES[n])]

    def landed(h, pair, n):
        return last_r.at[h] if n == N else exr.at[pair, n]

    def leaving(h, n):
        return (G_LS if n == N else G_EX) + h

    for h in range(2):
        gather(h, 2)
        for d in range(2):
            if h == 0:
                send(tls.at[2, d], trt.at[d], G_TL, tr_r.at[d], ex_dev[0](1 - 2 * d, c))
            for n in range(N + 1):
                send(
                    piece(h, snd[h].at[2], d * ROWS, n), piece(h, tr[h].at[d], 0, n),
                    leaving(h, n), ex2_r.at[h, d, n], ex_dev[h](1 - 2 * d, c),
                )

    def gather_rest(o, _):
        delta = jnp.where(o == 0, 1, jnp.where(o == 1, 3, 0))
        gather(0, delta)
        gather(1, delta)
        return 0

    lax.fori_loop(0, 3, gather_rest, 0)

    def ex1_send(far, pieces):
        cc = other if far else c
        for n in pieces:
            for h in range(2):
                for d in range(2):
                    slot = 3 - d + 4 * far
                    send(
                        piece(h, snd[h].at[1 + 2 * d], cc * ROWS, n), landing(h, slot, n),
                        leaving(h, n), landed(h, 1 + 2 * far, n), ex_dev[h](1 - 2 * d, cc),
                    )
                    if h == 0 and n == 0:
                        send(tls.at[1 + 2 * d, cc], ext.at[slot], G_TL, tail_r.at[1 + 2 * far], ex_dev[0](1 - 2 * d, cc))

    ex1_send(0, range(N))
    send(tls.at[0, other], ext.at[1], G_TO, tail_r.at[0], at(cc=other))
    ext[0] = tls[0, c]
    for h in range(2):
        for n in range(N + 1):
            send(piece(h, snd[h].at[0], other * ROWS, n), landing(h, 1, n), (G_OL if n == N else G_OWN) + h, landed(h, 0, n), at(cc=other))
        ex[h][0] = snd[h][0, pl.ds(pl.multiple_of(c * ROWS, 16), MAIN), 0:SPLIT]
        exl[h][0] = snd[h][0, pl.ds(pl.multiple_of(c * ROWS + MAIN, 16), LAST), :]

    for h in range(2):
        got(metar.at[h, 0:3], rr.at[2 + h])
        metar[h, po[h]] = meta[...]
        for i in range(4):
            code = metar[h, i, 4 * h : 4 * h + 4, 0:T].astype(I32) - po[h] * 1024
            slot = code // 32
            place = code - slot * 32 + m4(i - po[h] - 1) * PER
            valid = (code >= 0) & (code < 256)
            rowsel[h, :, i * T : (i + 1) * T] = jnp.where(valid & (place < MAIN), slot * MAIN + place, -1).astype(F32)
            rowlast[h, i] = jnp.where(valid & (place >= MAIN), slot * LAST + place - MAIN, -1).astype(F32)
        got(og[h].at[0 : 2 * T, :], og_r.at[h, 2])
    ogr[...] = pltpu.roll(og0[:, SPLIT : SPLIT + 128].astype(F32), 64, 1).astype(BF16)
    acc[...] = jnp.zeros_like(acc)

    def absorb(pair, mine):
        for n in range(N):
            if mine:
                got(ex[0].at[0:2, :, pl.ds(*PIECES[n])], exr.at[0, n])
            else:
                got(ex[0].at[0:4, :, pl.ds(*PIECES[n])], exr.at[pair, n])
            for h in range(2):
                lo, w = PIECES[n]
                block = ex[h][pl.ds(2 * pair, 2), :, lo : lo + w].reshape(2 * MAIN, w)
                part = dot(block, og[h][:, lo : lo + w], ((1,), (1,)))
                if n == 0:
                    gbuf[h] = part
                else:
                    gbuf[h] += part
            if n == 0:
                if mine:
                    got(ext.at[1], tail_r.at[0])
                else:
                    got(ext.at[pl.ds(2 * pair, 2)], tail_r.at[pair])
                tail = ext[pl.ds(2 * pair, 2)].reshape(MAIN, 128)
                for j, other_side in enumerate((og0[:, SPLIT : SPLIT + 128], ogr[...])):
                    part = dot(tail, other_side, ((1,), (1,)))
                    for slot in range(2):
                        where = slice(slot * MAIN + j * HALF, slot * MAIN + j * HALF + HALF)
                        gbuf[0, where, :] += part[slot * HALF : slot * HALF + HALF]
        rid = (iota((2 * MAIN, 128), 0) + pair * 2 * MAIN).astype(F32)
        for h in range(2):
            for lb in range(6):
                lanes = slice(lb * 128, lb * 128 + 128)
                g = gbuf[h, :, lanes]
                for k in range(K):
                    hit = jnp.where(rid == rowsel[h, k : k + 1, lanes], g, 0.0)
                    acc[h, k, :, lanes] += jnp.sum(hit.reshape(2 * MAIN // 8, 8, 128), axis=0)

    absorb(0, True)

    def forward(n):
        for h in range(2):
            for d in range(2):
                got(piece(h, tr[h].at[d], 0, n), ex2_r.at[h, d, n])
                send(
                    piece(h, tr[h].at[d], 0, n), landing(h, 4 + c, n),
                    leaving(h, n), landed(h, 2, n), ex_dev[h](1 - 2 * d, d),
                )

    for d in range(2):
        got(trt.at[d], tr_r.at[d])
        send(trt.at[d], ext.at[4 + c], G_TL, tail_r.at[2], ex_dev[0](1 - 2 * d, d))
    for n in range(N):
        forward(n)
    ex1_send(1, range(N))
    forward(N)
    for far in range(2):
        ex1_send(far, (N,))

    got(psr1.at[0:7], rr.at[5])
    psb2[...] = jnp.sum(psr1[...], axis=0)
    psr2[y] = psb2[...]
    for s in (1, 2, 3):
        send(psb2, psr2.at[y], G_SMALL, rr.at[6], at(dy=s))

    got(xcr.at[0:3], rr.at[7])
    cnt_row = jnp.sum(xcr[...], axis=0)[0:1, :]
    cnt_col = jnp.sum(jnp.where(diag, cnt_row, 0.0), axis=1, keepdims=True)
    push = bs_s[0] * E * (cnt_col / (TOTAL * K))
    prob = pt[...]
    spread = prob * (push - jnp.sum(prob * push, axis=0, keepdims=True))
    lt[...] = spread
    spb[...] = jnp.zeros_like(spb)
    for par in range(2):
        for n in range(16):
            spb[par, 4 * n : 4 * n + 4, 0:T] = spread[8 * n + 4 * par : 8 * n + 4 * par + 4, :]
        for k in range(K):
            ik = idxv[k : k + 1, :]
            spb[par, 64 + k : 65 + k, 0:T] = jnp.where((ik // 4) % 2 == par, ik // 8 * 4 + ik % 4, -1).astype(F32)
    for n, (a, k) in enumerate(xpeers):
        send(spb.at[lax.rem(c + k, 2)], spr.at[xc], G_SP, rr.at[9], xdev(a, k))
    spr[xc] = spb[c]

    def arrivals(pair, _):
        absorb(pair, False)
        return 0

    lax.fori_loop(1, 4, arrivals, 0)

    for h in range(2):
        for i in range(4):
            pds[h, i] = jnp.zeros((K, 256), F32)
            for k in range(K):
                pds[h, i, k : k + 1, 0:T] = jnp.sum(acc[h, k, :, i * T : (i + 1) * T], axis=0, keepdims=True)
        for s in (1, 2, 3):
            send(pds.at[h, m4(po[h] + s)], pdr.at[h, po[h]], G_SMALL, rr.at[10 + h], og_dev[h](s))
        pdr[h, po[h]] = pds[h, po[h]]
    late = [jnp.zeros((1, T), F32)] * K
    rid = iota((8 * LAST, T), 0).astype(F32)
    for h in range(2):
        got(exl[h].at[1:8], last_r.at[h])
    both = [dot(exl[h][...].reshape(8 * LAST, WIDTH[h]), og[h][own_og[h], :], ((1,), (1,))) for h in range(2)]
    for h in range(2):
        g = both[h]
        for k in range(K):
            hit = jnp.where(rid == rowlast[h, po[h], k : k + 1, :], g, 0.0)
            late[k] += jnp.sum(hit, axis=0, keepdims=True)

    pd = jnp.zeros((K, 256), F32)
    for h in range(2):
        got(pdr.at[h, 0:3], rr.at[10 + h])
        pd += (pdr[h, 0] + pdr[h, 1]) + (pdr[h, 2] + pdr[h, 3])

    dots = [pd[k : k + 1, 0:T] + late[k] for k in range(K)]
    mix = [mixv[k : k + 1, :] for k in range(K)]
    mean = mix[0] * dots[0] + mix[1] * dots[1] + mix[2] * dots[2] + mix[3] * dots[3]
    for k in range(K):
        selb[k : k + 1, 0:T] = mix[k] * (dots[k] - mean)
    selb[:, T:256] = jnp.zeros((K, 256 - T), F32)
    for n, (a, k) in enumerate(xpeers):
        send(selb, selr.at[xc], G_SMALL, lg_r.at[xc], xdev(a, k))

    lg = jnp.zeros((E, T), F32)
    for k in range(K):
        lg += jnp.where(idxv[k : k + 1, :] == ie, selb[k : k + 1, 0:T], 0.0)
    lgv[...] = jnp.transpose(lt[...] + lg).astype(BF16)
    got(psr2.at[0:3], rr.at[6])
    xps[...] = jnp.sum(psr2[...], axis=0)
    xpr[x] = xps[...]
    for a in (1, 2, 3):
        send(xps, xpr.at[x], G_SMALL, rr.at[8], at(dx=a))
    got(tokr.at[0:7], rr.at[4])
    got(spr.at[0:7], rr.at[9])

    ir = iota((64, T), 0).astype(F32)

    def weight_term(src, sel):
        named = jnp.zeros((64, T), F32)
        for k in range(K):
            named += jnp.where(spr[src, 64 + k : 65 + k, 0:T] == ir, sel[k : k + 1, 0:T], 0.0)
        return dot((spr[src, 0:64, 0:T] + named).astype(BF16), tokr[src])

    wsum = weight_term(xc, selb)
    for a, k in reversed(xpeers):
        src = m4(x + a) * 2 + lax.rem(c + k, 2)
        got(selr.at[src], lg_r.at[src])
        wsum += weight_term(src, selr.at[src])
    shift = x * 720 - (x * 720) // 128 * 128
    wsum = pltpu.roll(wsum, lax.rem(BLK - shift, BLK), 1)
    for n in range(16):
        rss[n] = wsum[4 * n : 4 * n + 4, 0:OUT]

    chip = y * 4 + z
    hops = lambda v: min(v[0], 4 - v[0]) + min(v[1], 4 - v[1])
    for n, (a, b) in enumerate(sorted([(a, b) for a in range(4) for b in range(4) if a or b], key=hops, reverse=True)):
        dest = m4(y + a) * 4 + m4(z + b)
        send(rss.at[dest], rsr.at[chip], G_RS, rr.at[12], at(dy=a, dz=b))
    rsr[chip] = rss[chip]
    tg_o[...] = dot(lgv[...], wv[...], ((1,), (1,))).astype(BF16)

    got(xpr.at[0:3], rr.at[8])
    ps_row = jnp.sum(xpr[...], axis=0)[0:1, :]
    loss = E * jnp.sum((cnt_row / (TOTAL * K)) * (ps_row / TOTAL), axis=1, keepdims=True)
    small_o[4:8, :] = jnp.broadcast_to(loss, (4, OUT))

    for h in range(2):
        drain(ex[h], G_EX + h)
        drain(exl[h], G_LS + h)
        drain(ex[h].at[0], G_OWN + h)
        drain(exl[h].at[0], G_OL + h)
        drain(og[h].at[0 : 3 * T, :], G_OG + h)
    for ref, group in (
        (spr.at[0:4], G_SMALL),
        (tokr.at[0:7], G_TK), (spr.at[0:7], G_SP), (tls, G_TL), (tls.at[0, 0], G_TO), (rsr.at[0:15], G_RS),
    ):
        drain(ref, group)
    got(rsr.at[0:15], rr.at[12])
    out = jnp.sum(rsr[...], axis=0) * (1.0 / math.sqrt(TOTAL))
    small_o[0:4, :] = out[:, 0:OUT]


def finish(tg_ref, small_ref, tg_o, wt_o, loss_o, wtv, lossv, sem):
    tg_out = [pltpu.make_async_copy(tg_ref.at[48 * n : 48 * n + 48], tg_o.at[48 * n : 48 * n + 48], sem.at[3 + n]) for n in range(4)]
    for t in tg_out:
        t.start()
    wtv[...] = small_ref[0:4, 0:720]
    wt_out = pltpu.make_async_copy(wtv, wt_o, sem.at[1])
    wt_out.start()
    lossv[0] = jnp.sum(small_ref[4:5, 0:1])
    loss_out = pltpu.make_async_copy(lossv, loss_o, sem.at[2])
    loss_out.start()
    loss_out.wait()
    for t in tg_out:
        t.wait()
    wt_out.wait()


def on_device(tokens, out_grad, indices, expert_rows, router_weight, router_bias, balance_scale):
    rows = jnp.transpose(expert_rows[0], (0, 2, 1, 3)).reshape(ES, 32, D)
    dma = pltpu.SemaphoreType.DMA
    vm = pltpu.VMEM
    scratch = [
        vm((T, D), BF16), vm((T, DPAD), BF16), vm((T, D), BF16), vm((4 * T, WIDTH[0]), BF16), vm((4 * T, WIDTH[1]), BF16),
        vm((K, T), I32), vm((4, ES, 8, D), BF16), vm((4 * KQ, DPAD), BF16), vm((D, E), BF16), vm((1, E), F32),
        vm((4, 2 * ROWS, WIDTH[0]), BF16), vm((4, 2 * ROWS, WIDTH[1]), BF16),
        vm((2, ROWS, WIDTH[0]), BF16), vm((2, ROWS, WIDTH[1]), BF16),
        vm((8, MAIN, SPLIT), BF16), vm((8, MAIN, SPLIT), BF16), vm((8, LAST, WIDTH[0]), BF16), vm((8, LAST, WIDTH[1]), BF16),
        vm((4, 2, HALF, 128), BF16), vm((2, HALF, 128), BF16), vm((8, HALF, 128), BF16), vm((4 * T, 128), BF16),
        vm((8, T, BLK), BF16),
        vm((8, E), F32), vm((4, 8, 8, E), F32), vm((K, 256, E), BF16), vm((8, 256), F32), vm((2, 4, 8, 256), F32),
        vm((2, K, 4 * T), F32), vm((2, 4, K, T), F32), vm((2, K, 8, 4 * T), F32), vm((2, 2 * MAIN, 4 * T), F32), vm((2, 4, K, 256), F32), vm((2, 4, K, 256), F32),
        vm((8, E), F32), vm((8, 8, E), F32), vm((4, 8, E), F32), vm((8, E), F32),
        vm((8, E), F32), vm((4, 8, E), F32), vm((8, E), F32), vm((4, 8, E), F32),
        vm((E, T), F32), vm((E, T), F32), vm((K, T), F32), vm((2, 72, 256), F32), vm((8, 72, 256), F32),
        vm((K, 256), F32), vm((8, K, 256), F32), vm((16, 4, OUT), F32), vm((16, 4, OUT), F32), vm((T, E), BF16),
        dma((6,)), dma((16,)), dma((13,)), dma((2, 3)), dma((2, 2, N + 1)), dma((4, N)), dma((2,)), dma((2,)), dma((4,)), dma((8,)),
    ]
    hbm = pl.BlockSpec(memory_space=pltpu.HBM)
    in_vmem = pl.BlockSpec(memory_space=vm)
    token_grad, small = pl.pallas_call(
        kernel,
        out_shape=(vm((T, D), BF16), vm((8, OUT), F32)),
        in_specs=[hbm] * 6 + [pl.BlockSpec(memory_space=pltpu.SMEM)],
        out_specs=(in_vmem, in_vmem),
        scratch_shapes=scratch,
        compiler_params=pltpu.CompilerParams(collective_id=0, has_side_effects=True, vmem_limit_bytes=54000 * 1024),
        name="router",
    )(
        *(
            pltpu.with_memory_space_constraint(a, pltpu.HBM)
            for a in (tokens, out_grad, indices.T, rows, router_weight, router_bias.reshape(1, E))
        ),
        balance_scale,
    )
    token_grad, weight_grad, loss = pl.pallas_call(
        finish,
        out_shape=(
            jax.ShapeDtypeStruct((T, D), BF16),
            jax.ShapeDtypeStruct((4, 720), F32),
            jax.ShapeDtypeStruct((1,), F32),
        ),
        in_specs=[in_vmem] * 2,
        out_specs=(hbm, hbm, hbm),
        scratch_shapes=[vm((4, 720), F32), pltpu.SMEM((1,), F32), dma((7,))],
        name="finish",
    )(*(pltpu.with_memory_space_constraint(a, vm) for a in (token_grad, small)))
    return token_grad, weight_grad.T, loss


def solution(mesh):
    torus = Mesh(mesh.devices.reshape(4, 4, 2, mesh.shape["dp"]), AXES)
    return jax.shard_map(
        on_device,
        mesh=torus,
        in_specs=(P(AXES, None), P(AXES, None), P(AXES, None), P("dp", EP, None, None, None), P(), P(), P()),
        out_specs=(P(AXES, None), P("dp", EP), P()),
        check_vma=False,
    )
```
